256 devices in a mesh: row: 128 (over y, z, x), grp: 2 (over core).
Axes of the slice: x: 4, y: 4, z: 8, core: 2. Of those that a mesh axis runs over, the one named last changes fastest.
Arguments:
- features: float32 [1048576, 256], P(('row', 'grp')), may hold values from -6 to 6
- session: int32 [1048576], P(('row', 'grp')), may hold values from 0 to 8191, never falling along the last dimension, each value on 1 to 163840 neighbouring positions
- owner_map: int32 [256, 64], P(('row', 'grp')), may hold values from 0 to 127, as said below
Outputs:
- received: bfloat16 [32768, 64, 256], P(('row', 'grp'))
The draws below stay inside these ranges and needn't reach their ends.
Inputs may be any that keep to these rules, and one draw needn't show every extreme that they name: session numbers never fall along the rows; each session covers 1 to 163840 consecutive rows. `owner_map`: no owner is named by more than 1 of the blocks of one group of 64.
All inputs are finite; a program needn't handle non-finite values.
Results may differ from the reference program's by a relative error of at most 0.001.
Values may be sent and summed in bfloat16 or wider, within the bound.
A program may use at most 128 MiB of HBM per device.

```python
import math
import jax
import jax.numpy as jnp
import numpy as np
from jax import lax

F = 256
BLOCK = 64
BLOCKS = 64
ROWS_DEV = 4096
ROWS = 1048576
CAP = 1
SESSIONS = 8192
MOST = 163840
N_ROW = 128
N_GRP = 2
DEVICES = 256


def draw_owner_map(key, part):
    base = jax.random.fold_in(key, 11)
    key_pop, key_hot, key_noise, key_order = jax.random.split(base, 4)
    slot_capacity_total = N_ROW * CAP
    favored_devices = jax.random.randint(key_pop, (N_ROW,), 0, 96)
    busiest_device = jax.random.randint(key_hot, (), 0, N_ROW)
    candidate_owner = jnp.arange(slot_capacity_total) // CAP
    extra_reward = favored_devices[candidate_owner] + jnp.where(candidate_owner == busiest_device, 4096, 0)
    random_jitter = jax.random.randint(key_noise, (DEVICES, slot_capacity_total), 0, 64)
    owner_rating = (random_jitter + extra_reward[None, :]) * slot_capacity_total + jnp.arange(slot_capacity_total)[None, :]
    unused, picked = lax.top_k(owner_rating, BLOCKS)
    owners = candidate_owner[picked]
    shuffle = jax.random.randint(key_order, (DEVICES, BLOCKS), 0, 65536) * BLOCKS + jnp.arange(BLOCKS)[None, :]
    arrange = jnp.argsort(shuffle, axis=1)
    return jnp.take_along_axis(owners, arrange, axis=1).astype(jnp.int32)


def shard_levels(rng, dims, shards, low, largest):
    def one(position, parts):
        heights = jax.random.uniform(jax.random.fold_in(jax.random.fold_in(rng, 6), position), (parts,), jnp.float32, low / len(shards), largest / len(shards))
        return jnp.repeat(jnp.exp(heights), dims[position] // parts).reshape((-1,) + (1,) * (len(dims) - position - 1))

    gain = one(*shards[0])
    for cut in shards[1:]:
        gain = gain * one(*cut)
    return gain


def split_up(number_of, total, limit, lean):
    loads = [(1 << 20) // math.isqrt(rank ** lean) + 1 for rank in range(2, number_of + 1)]
    rest, counts = total - limit - (number_of - 1), [1] * (number_of - 1)
    while rest > 0:
        free = [i for i in range(number_of - 1) if counts[i] < limit]
        pool, remaining = sum([loads[i] for i in free]), rest
        for i in free:
            more = min(limit - counts[i], max(1, remaining * loads[i] // pool), rest)
            counts[i] = counts[i] + more
            rest = rest - more
    return np.array([limit] + counts)


def ragged_sizes(stream_key, number_of, total, limit, slope):
    if number_of == 2:
        one = jax.random.randint(stream_key, (), max(1, total - limit), min(limit, total - 1) + 1)
        return jnp.stack([one, total - one])
    lengths = jnp.asarray(split_up(number_of, total, limit, slope), jnp.int32)
    couples = (number_of - 1) // 2
    donor, receiver = lengths[1:1 + 2 * couples:2], lengths[2:2 + 2 * couples:2]
    slack = jnp.minimum(donor - 1, limit - receiver)
    shifted = jax.random.randint(jax.random.fold_in(stream_key, 1), (couples,), 0, 1 << 20) % (slack + 1)
    lengths = lengths.at[1:1 + 2 * couples:2].set(donor - shifted).at[2:2 + 2 * couples:2].set(receiver + shifted)
    return lengths[jax.random.permutation(jax.random.fold_in(stream_key, 2), number_of)]


def noise(key, shape, scale, most, pieces=(), dtype=jnp.bfloat16):
    values = jax.random.normal(key, shape, jnp.float32) * scale
    if len(pieces) > 0:
        values = shard_levels(key, shape, pieces, -0.22, 0.18) * values
    return jnp.clip(values, min=-most, max=most).astype(dtype)


def setup_inputs(seed: int = 0) -> dict:
    seeds = jax.random.split(jax.random.key(seed), 4)
    return {
        "features": noise(seeds[0], (ROWS, F), 1.0, 6.0, ((0, 256),), jnp.float32),
        "session": jnp.searchsorted(jnp.cumsum(ragged_sizes(seeds[1], SESSIONS, ROWS, MOST, 2)), jnp.arange(ROWS), side="right").astype(jnp.int32),
        "owner_map": draw_owner_map(jax.random.fold_in(seeds[3], 71), 0),
    }


def combine(earlier, latter):
    same_ids = earlier[0] == latter[0]
    return (latter[0], latter[1] + jnp.where(same_ids[..., None], earlier[1], 0.0), latter[2] + jnp.where(same_ids, earlier[2], 0.0))

def shard_step(carry, inputs):
    group_rows, group_ids = inputs
    all_ids = jnp.concatenate([carry[0][None], group_ids.astype(jnp.int32)])
    all_rows = jnp.concatenate([carry[1][None], group_rows])
    all_counts = jnp.concatenate([carry[2][None], jnp.ones((ROWS_DEV,), jnp.float32)])
    out_ids, out_rows, out_counts = lax.associative_scan(combine, (all_ids, all_rows, all_counts))
    normalized = (out_rows[1:] / jnp.sqrt(out_counts[1:])[:, None]).astype(jnp.bfloat16)
    return ((out_ids[-1], out_rows[-1], out_counts[-1]), normalized)

def reference(features, session, owner_map):
    grouped = features.reshape(DEVICES, ROWS_DEV, F)
    grouped_ids = session.reshape(DEVICES, ROWS_DEV)
    start = (jnp.array(-1, jnp.int32), jnp.zeros((F,), jnp.float32), jnp.array(0.0, jnp.float32))
    unused, normalized = lax.scan(shard_step, start, (grouped, grouped_ids))
    block_rows = normalized.reshape(DEVICES * BLOCKS, BLOCK, F)
    order = jnp.arange(BLOCKS).astype(jnp.int32)
    lower = order[None, :] < order[:, None]
    same_owner = owner_map[:, :, None] == owner_map[:, None, :]
    rank = lax.optimization_barrier(jnp.sum((same_owner & lower[None]).astype(jnp.int32), axis=2))
    device = jnp.arange(DEVICES).astype(jnp.int32)
    row_pos = device // N_GRP
    grp_pos = device % N_GRP
    target = (owner_map * N_GRP + grp_pos[:, None]) * (N_ROW * CAP) + row_pos[:, None] * CAP + rank
    received = jnp.zeros((DEVICES * N_ROW * CAP, BLOCK, F), jnp.bfloat16)
    received = received.at[target.reshape(-1).astype(jnp.int32)].set(block_rows)
    return received
```

```python
import jax
import jax.numpy as jnp
from jax import lax
from jax.experimental import pallas as pl
from jax.experimental.pallas import tpu as pltpu
from jax.sharding import Mesh
from jax.sharding import PartitionSpec as P

ROW = ("row_0", "row_1", "row_2")
ROW_GRP = ("row_0", "row_1", "row_2", "grp")
MOST = 163840
TILE = 128
MESH = pl.DeviceIdType.MESH


def coords(d, sizes):
    out = []
    for n in reversed(sizes):
        out.append(lax.rem(d, n))
        d = lax.div(d, n)
    return tuple(reversed(out))


def prelude_kernel(
    sizes, reach, block_rows,
    src_ref, ids_ref, feat_hbm, out_ref,
    feat, idcol, cnt, norm, tail, got, load_sem, send_sem, recv_sem,
):
    total_devices = 1
    for n in sizes:
        total_devices *= n
    me = lax.axis_index(ROW_GRP)
    rows_dev, width = feat.shape
    tiles = rows_dev // TILE
    chunks = load_sem.shape[0]
    per = rows_dev // chunks

    def load(c):
        at = pl.ds(c * per, per)
        return pltpu.make_async_copy(feat_hbm.at[at], feat.at[at], load_sem.at[c])

    for c in range(chunks):
        load(c).start()

    barrier = pltpu.get_barrier_semaphore()

    @pl.loop(1, reach + 1)
    def _(k):
        peer = lax.rem(me + total_devices - k, total_devices)
        pl.semaphore_signal(barrier, 1, device_id=coords(peer, sizes), device_id_type=MESH)

    last = ids_ref[tiles - 1 : tiles, TILE - 1 : TILE]
    last_wide = jnp.broadcast_to(last, (TILE, TILE))

    sums = jnp.zeros((8, width), jnp.float32)
    count = jnp.zeros((8, TILE), jnp.float32)
    for c in range(chunks):
        load(c).wait()

        @pl.loop(c * (tiles // chunks), (c + 1) * (tiles // chunks), init_carry=(sums, count))
        def tail_step(t, carry):
            acc, num = carry
            wide = jnp.broadcast_to(ids_ref[pl.ds(t, 1), :], (TILE, TILE))
            col = wide.T
            at = pl.ds(pl.multiple_of(t * TILE, TILE), TILE)
            idcol[at, :] = col
            open_rows = col == last_wide
            both = jnp.concatenate([open_rows, open_rows], axis=1)
            rows = jnp.where(both, feat[at, :], 0.0)
            acc = acc + jnp.sum(rows.reshape(TILE // 8, 8, width), axis=0)
            num = num + jnp.sum(
                jnp.where(open_rows, 1.0, 0.0).reshape(TILE // 8, 8, TILE), axis=0
            )
            return acc, num

        sums, count = tail_step
    sums = jnp.sum(sums, axis=0, keepdims=True)
    count = jnp.sum(count, axis=0, keepdims=True)
    tail[0:1, :] = sums[:, :TILE]
    tail[1:2, :] = sums[:, TILE:]
    tail[2:3, :] = jnp.broadcast_to(last, (1, TILE))
    tail[3:4, :] = count

    pl.semaphore_wait(barrier, reach)

    @pl.loop(1, reach + 1)
    def _(k):
        peer = lax.rem(me + k, total_devices)
        pltpu.make_async_remote_copy(
            src_ref=tail,
            dst_ref=got.at[k - 1],
            send_sem=send_sem,
            recv_sem=recv_sem,
            device_id=coords(peer, sizes),
            device_id_type=MESH,
        ).start()

    above = lax.broadcasted_iota(jnp.int32, (TILE, TILE), 0)
    left = lax.broadcasted_iota(jnp.int32, (TILE, TILE), 1)
    causal = left <= above
    ones = jnp.ones((TILE, TILE), jnp.bfloat16)

    @pl.loop(
        0, tiles,
        init_carry=(
            jnp.full((1, TILE), -1.0, jnp.float32),
            jnp.zeros((1, width), jnp.float32),
            jnp.zeros((1, TILE), jnp.float32),
        ),
        unroll=2,
    )
    def _(t, carry):
        open_id, open_sum, open_count = carry
        at = pl.ds(pl.multiple_of(t * TILE, TILE), TILE)
        col = idcol[at, :]
        wide = jnp.broadcast_to(ids_ref[pl.ds(t, 1), :], (TILE, TILE))
        mask = jnp.where((col == wide) & causal, 1.0, 0.0).astype(jnp.bfloat16)
        rows = feat[at, :]
        high = rows.astype(jnp.bfloat16)
        rest = rows - high.astype(jnp.float32)
        mid = rest.astype(jnp.bfloat16)
        low = (rest - mid.astype(jnp.float32)).astype(jnp.bfloat16)
        inside = (
            jnp.dot(mask, high, preferred_element_type=jnp.float32)
            + jnp.dot(mask, mid, preferred_element_type=jnp.float32)
            + jnp.dot(mask, low, preferred_element_type=jnp.float32)
        )
        number = jnp.dot(mask, ones, preferred_element_type=jnp.float32)
        joined = col == jnp.broadcast_to(open_id, (TILE, TILE))
        both = jnp.concatenate([joined, joined], axis=1)
        inside = inside + jnp.where(both, jnp.broadcast_to(open_sum, (TILE, width)), 0.0)
        number = number + jnp.where(joined, jnp.broadcast_to(open_count, (TILE, TILE)), 0.0)
        feat[at, :] = inside
        cnt[at, :] = number
        return col[TILE - 1 :, :], inside[TILE - 1 :, :], number[TILE - 1 :, :]

    pltpu.make_async_copy(got, got, recv_sem).wait()
    arrived = got[...]
    open_id = arrived[0, 2:3, :]
    age = lax.broadcasted_iota(jnp.int32, arrived.shape, 0) + 1
    same = jnp.broadcast_to(arrived[:, 2:3, :], arrived.shape) == jnp.broadcast_to(
        open_id[None], arrived.shape
    )
    merged = jnp.sum(jnp.where(same & (age <= me), arrived, 0.0), axis=0)
    open_sum = jnp.concatenate([merged[0:1, :], merged[1:2, :]], axis=1)
    open_count = merged[3:4, :]

    @pl.loop(0, rows_dev // block_rows, unroll=2)
    def _(b):
        at = pl.ds(pl.multiple_of(b * block_rows, block_rows), block_rows)
        joined = idcol[at, :] == jnp.broadcast_to(open_id, (block_rows, TILE))
        number = cnt[at, :] + jnp.where(
            joined, jnp.broadcast_to(open_count, (block_rows, TILE)), 0.0
        )
        scale = 1.0 / jnp.sqrt(number)
        both = jnp.concatenate([joined, joined], axis=1)
        rows = feat[at, :] + jnp.where(
            both, jnp.broadcast_to(open_sum, (block_rows, width)), 0.0
        )
        norm[b] = (rows * jnp.concatenate([scale, scale], axis=1)).astype(jnp.bfloat16)

    @pl.loop(0, out_ref.shape[0], unroll=4)
    def _(slot):
        b = src_ref[slot]
        block = norm[jnp.maximum(b, 0)]
        out_ref[slot] = jnp.where(b >= 0, block, jnp.zeros_like(block))

    pltpu.make_async_copy(got, got, send_sem).wait()


def body(features, session, owner_map):
    rows_dev, width = features.shape
    owners = owner_map[0]
    block_count = owners.shape[0]
    block_rows = rows_dev // block_count
    row_count = lax.axis_size(ROW)
    sizes = tuple(lax.axis_size(name) for name in ROW_GRP)
    slot_cap = max(1, 2 * block_count // row_count)
    slots = row_count * slot_cap
    order = jnp.arange(block_count)
    rank = jnp.sum(
        ((owners[:, None] == owners[None, :]) & (order[None, :] < order[:, None])).astype(
            jnp.int32
        ),
        axis=1,
    )
    target = owners * slot_cap + rank
    hit = jnp.arange(slots)[:, None] == target[None, :]
    source = jnp.sum(jnp.where(hit, order[None, :] + 1, 0), axis=1).astype(jnp.int32) - 1
    reach = (MOST - 2) // rows_dev + 1
    ids = session.astype(jnp.float32).reshape(rows_dev // TILE, TILE)
    outgoing = pl.pallas_call(
        lambda *refs: prelude_kernel(sizes, reach, block_rows, *refs),
        out_shape=jax.ShapeDtypeStruct((slots, block_rows, width), jnp.bfloat16),
        in_specs=[
            pl.BlockSpec(memory_space=pltpu.SMEM),
            pl.BlockSpec(memory_space=pltpu.VMEM),
            pl.BlockSpec(memory_space=pl.ANY),
        ],
        out_specs=pl.BlockSpec(memory_space=pltpu.VMEM),
        scratch_shapes=[
            pltpu.VMEM((rows_dev, width), jnp.float32),
            pltpu.VMEM((rows_dev, TILE), jnp.float32),
            pltpu.VMEM((rows_dev, TILE), jnp.float32),
            pltpu.VMEM((block_count, block_rows, width), jnp.bfloat16),
            pltpu.VMEM((4, TILE), jnp.float32),
            pltpu.VMEM((reach, 4, TILE), jnp.float32),
            pltpu.SemaphoreType.DMA((4,)),
            pltpu.SemaphoreType.DMA,
            pltpu.SemaphoreType.DMA,
        ],
        compiler_params=pltpu.CompilerParams(collective_id=0, has_side_effects=True),
        name="prelude",
    )(source, ids, features)
    return lax.all_to_all(outgoing, ROW, split_axis=0, concat_axis=0, tiled=True)


def solution(mesh):
    split = Mesh(
        mesh.devices.reshape(4, 8, 4, mesh.shape["grp"]), ("row_0", "row_1", "row_2", "grp")
    )
    return jax.shard_map(
        body,
        mesh=split,
        in_specs=(P(ROW_GRP, None), P(ROW_GRP), P(ROW_GRP, None)),
        out_specs=P(ROW_GRP, None, None),
        check_vma=False,
    )
```

```python
import jax
import jax.numpy as jnp
from jax import lax
from jax.experimental import pallas as pl
from jax.experimental.pallas import tpu as pltpu
from jax.sharding import Mesh
from jax.sharding import PartitionSpec as P

ROW = ("row_0", "row_1", "row_2")
ROW_GRP = ("row_0", "row_1", "row_2", "grp")
MOST = 163840
TILE = 128
MESH = pl.DeviceIdType.MESH


def coords(d, sizes):
    out = []
    for n in reversed(sizes):
        out.append(lax.rem(d, n))
        d = lax.div(d, n)
    return tuple(reversed(out))


def prelude_kernel(
    sizes, reach, block_rows, slot_cap,
    owners_hbm, ids_hbm, feat_hbm, out_ref,
    owners_ref, ids_ref, feat, sums, cnt, norm, ends, joins, table, slot_of, tail, got,
    load_sem, table_sem, send_sem, recv_sem,
):
    total_devices = 1
    for n in sizes:
        total_devices *= n
    me = lax.axis_index(ROW_GRP)
    rows_dev, width = feat.shape
    tiles = rows_dev // TILE
    blocks = rows_dev // block_rows
    slots = out_ref.shape[0]
    loads = [
        pltpu.make_async_copy(src, dst, load_sem.at[n])
        for n, (src, dst) in enumerate(
            ((ids_hbm, ids_ref), (owners_hbm, owners_ref), (feat_hbm, feat))
        )
    ]
    for load in loads:
        load.start()

    barrier = pltpu.get_barrier_semaphore()

    @pl.loop(1, reach + 1)
    def _(k):
        peer = lax.rem(me + total_devices - k, total_devices)
        pl.semaphore_signal(barrier, 1, device_id=coords(peer, sizes), device_id_type=MESH)

    loads[0].wait()
    ids = ids_ref[...]
    last = jnp.broadcast_to(ids[tiles - 1 :, TILE - 1 :], (1, TILE))
    in_last = jnp.where(ids == jnp.broadcast_to(last, ids.shape), 1.0, 0.0)
    count = jnp.sum(jnp.sum(in_last, axis=0, keepdims=True), axis=1, keepdims=True)
    first = jnp.broadcast_to(rows_dev - count.astype(jnp.int32), (8, width))
    step = 64
    loads[2].wait()
    sub = lax.broadcasted_iota(jnp.int32, (step, width), 0)

    @pl.loop(0, rows_dev // step, init_carry=jnp.zeros((step, width), jnp.float32), unroll=4)
    def open_rows(t, acc):
        at = pl.ds(pl.multiple_of(t * step, step), step)
        inside = sub + t * step >= jnp.broadcast_to(first[0:1], (step, width))
        return acc + jnp.where(inside, feat[at, :], 0.0)

    total = jnp.sum(open_rows, axis=0, keepdims=True)
    tail[0:1, :] = total[:, :TILE]
    tail[1:2, :] = total[:, TILE:]
    tail[2:3, :] = last.astype(jnp.float32)
    tail[3:4, :] = jnp.broadcast_to(count, (1, TILE))

    lane = lax.broadcasted_iota(jnp.int32, ids.shape, 1)
    after = pltpu.roll(ids, TILE - 1, 1)
    end = jnp.where((after != ids) | (lane == TILE - 1), lane, TILE)
    hop = 1
    while hop < TILE:
        ahead = jnp.where(lane + hop < TILE, pltpu.roll(end, TILE - hop, 1), TILE)
        end = jnp.minimum(end, ahead)
        hop *= 2
    ends[...] = end
    before = jnp.concatenate([jnp.full((1, TILE), -1, jnp.int32), ids[:-1]], axis=0)
    before = jnp.broadcast_to(before[:, TILE - 1 :], ids.shape)
    goes_on = jnp.sum(jnp.where(ids == before, 1.0, 0.0), axis=1, keepdims=True)
    joins[...] = jnp.broadcast_to(goes_on.astype(jnp.int32), ids.shape)

    pl.semaphore_wait(barrier, reach)

    @pl.loop(1, reach + 1)
    def _(k):
        peer = lax.rem(me + k, total_devices)
        pltpu.make_async_remote_copy(
            src_ref=tail,
            dst_ref=got.at[k - 1],
            send_sem=send_sem,
            recv_sem=recv_sem,
            device_id=coords(peer, sizes),
            device_id_type=MESH,
        ).start()

    loads[1].wait()
    owners = owners_ref[...]
    across = jnp.broadcast_to(owners, (blocks, blocks))
    down = jnp.broadcast_to(across.T[:, 0:1], (blocks, blocks))
    earlier = lax.broadcasted_iota(jnp.int32, (blocks, blocks), 1) < (
        lax.broadcasted_iota(jnp.int32, (blocks, blocks), 0)
    )
    rank = jnp.sum(jnp.where((across == down) & earlier, 1.0, 0.0), axis=1, keepdims=True)
    target = down[:, 0:1] * slot_cap + rank.astype(jnp.int32)
    hit = jnp.broadcast_to(target, (blocks, slots)) == (
        lax.broadcasted_iota(jnp.int32, (blocks, slots), 1)
    )
    order = lax.broadcasted_iota(jnp.int32, (blocks, slots), 0) + 1
    table[...] = jnp.sum(jnp.where(hit, order, 0), axis=0, keepdims=True)
    to_scalars = pltpu.make_async_copy(table, slot_of, table_sem)
    to_scalars.start()

    row = lax.broadcasted_iota(jnp.int32, (TILE, TILE), 0)
    col = lax.broadcasted_iota(jnp.int32, (TILE, TILE), 1)
    causal = col <= row
    ones = jnp.ones((TILE, TILE), jnp.bfloat16)

    @pl.loop(
        0, tiles,
        init_carry=(jnp.zeros((1, width), jnp.float32), jnp.zeros((1, TILE), jnp.float32)),
        unroll=4,
    )
    def _(t, carry):
        open_sum, open_count = carry
        at = pl.ds(pl.multiple_of(t * TILE, TILE), TILE)
        alive = row <= jnp.broadcast_to(ends[pl.ds(t, 1), :], (TILE, TILE))
        mask = jnp.where(alive & causal, 1.0, 0.0).astype(jnp.bfloat16)
        rows = feat[at, :]
        high = rows.astype(jnp.bfloat16)
        rest = rows - high.astype(jnp.float32)
        mid = rest.astype(jnp.bfloat16)
        low = (rest - mid.astype(jnp.float32)).astype(jnp.bfloat16)
        inside = (
            jnp.dot(mask, high, preferred_element_type=jnp.float32)
            + jnp.dot(mask, mid, preferred_element_type=jnp.float32)
            + jnp.dot(mask, low, preferred_element_type=jnp.float32)
        )
        number = jnp.dot(mask, ones, preferred_element_type=jnp.float32)
        joined = row < jnp.broadcast_to(joins[pl.ds(t, 1), :], (TILE, TILE))
        both = jnp.concatenate([joined, joined], axis=1)
        inside = inside + jnp.where(both, jnp.broadcast_to(open_sum, (TILE, width)), 0.0)
        number = number + jnp.where(joined, jnp.broadcast_to(open_count, (TILE, TILE)), 0.0)
        sums[at, :] = inside
        cnt[at, :] = number
        return inside[TILE - 1 :, :], number[TILE - 1 :, :]

    pltpu.make_async_copy(got, got, recv_sem).wait()
    arrived = got[...]
    open_id = arrived[0, 2:3, :]
    age = lax.broadcasted_iota(jnp.int32, arrived.shape, 0) + 1
    same = jnp.broadcast_to(arrived[:, 2:3, :], arrived.shape) == jnp.broadcast_to(
        open_id[None], arrived.shape
    )
    merged = jnp.sum(jnp.where(same & (age <= me), arrived, 0.0), axis=0)
    open_sum = jnp.concatenate([merged[0:1, :], merged[1:2, :]], axis=1)
    open_count = merged[3:4, :]
    in_open = jnp.where(
        ids.astype(jnp.float32) == jnp.broadcast_to(open_id, ids.shape), 1.0, 0.0
    )
    reached = jnp.sum(jnp.sum(in_open, axis=0, keepdims=True), axis=1, keepdims=True)
    reached = jnp.broadcast_to(reached.astype(jnp.int32), (1, TILE))
    sub = lax.broadcasted_iota(jnp.int32, (block_rows, TILE), 0)

    @pl.loop(0, blocks, unroll=4)
    def _(b):
        at = pl.ds(pl.multiple_of(b * block_rows, block_rows), block_rows)
        joined = sub + b * block_rows < jnp.broadcast_to(reached, (block_rows, TILE))
        number = cnt[at, :] + jnp.where(
            joined, jnp.broadcast_to(open_count, (block_rows, TILE)), 0.0
        )
        scale = 1.0 / jnp.sqrt(number)
        both = jnp.concatenate([joined, joined], axis=1)
        rows = sums[at, :] + jnp.where(
            both, jnp.broadcast_to(open_sum, (block_rows, width)), 0.0
        )
        norm[b] = (rows * jnp.concatenate([scale, scale], axis=1)).astype(jnp.bfloat16)

    to_scalars.wait()

    @pl.loop(0, slots, unroll=8)
    def _(slot):
        b = slot_of[0, slot]
        block = norm[jnp.maximum(b, 1) - 1]
        out_ref[slot] = jnp.where(b > 0, block, jnp.zeros_like(block))

    pltpu.make_async_copy(got, got, send_sem).wait()


def body(features, session, owner_map):
    rows_dev, width = features.shape
    blocks = owner_map.shape[1]
    block_rows = rows_dev // blocks
    row_count = lax.axis_size(ROW)
    sizes = tuple(lax.axis_size(name) for name in ROW_GRP)
    slot_cap = max(1, 2 * blocks // row_count)
    slots = row_count * slot_cap
    tiles = rows_dev // TILE
    reach = (MOST - 2) // rows_dev + 1
    outgoing = pl.pallas_call(
        lambda *refs: prelude_kernel(sizes, reach, block_rows, slot_cap, *refs),
        out_shape=jax.ShapeDtypeStruct((slots, block_rows, width), jnp.bfloat16),
        in_specs=[pl.BlockSpec(memory_space=pltpu.HBM)] * 3,
        out_specs=pl.BlockSpec(memory_space=pltpu.VMEM),
        scratch_shapes=[
            pltpu.VMEM(owner_map.shape, jnp.int32),
            pltpu.VMEM((tiles, TILE), jnp.int32),
            pltpu.VMEM((rows_dev, width), jnp.float32),
            pltpu.VMEM((rows_dev, width), jnp.float32),
            pltpu.VMEM((rows_dev, TILE), jnp.float32),
            pltpu.VMEM((blocks, block_rows, width), jnp.bfloat16),
            pltpu.VMEM((tiles, TILE), jnp.int32),
            pltpu.VMEM((tiles, TILE), jnp.int32),
            pltpu.VMEM((1, slots), jnp.int32),
            pltpu.SMEM((1, slots), jnp.int32),
            pltpu.VMEM((4, TILE), jnp.float32),
            pltpu.VMEM((reach, 4, TILE), jnp.float32),
            pltpu.SemaphoreType.DMA((3,)),
            pltpu.SemaphoreType.DMA,
            pltpu.SemaphoreType.DMA,
            pltpu.SemaphoreType.DMA,
        ],
        compiler_params=pltpu.CompilerParams(
            collective_id=0, has_side_effects=True, vmem_limit_bytes=24 << 20
        ),
        name="prelude",
    )(owner_map, session.reshape(tiles, TILE), features)
    return lax.all_to_all(outgoing, ROW, split_axis=0, concat_axis=0, tiled=True)


def solution(mesh):
    split = Mesh(
        mesh.devices.reshape(4, 8, 4, mesh.shape["grp"]), ("row_0", "row_1", "row_2", "grp")
    )
    return jax.shard_map(
        body,
        mesh=split,
        in_specs=(P(ROW_GRP, None), P(ROW_GRP), P(ROW_GRP, None)),
        out_specs=P(ROW_GRP, None, None),
        check_vma=False,
    )
```

```python
import jax
import jax.numpy as jnp
from jax import lax
from jax.experimental import pallas as pl
from jax.experimental.pallas import tpu as pltpu
from jax.sharding import Mesh
from jax.sharding import PartitionSpec as P

ROW = ("row_0", "row_1", "row_2")
ROW_GRP = ("row_0", "row_1", "row_2", "grp")
MOST = 163840
TILE = 128
ROOMS = (12, 13, 14, 15, 16)
MESH = pl.DeviceIdType.MESH


def coords(d, sizes):
    out = []
    for n in reversed(sizes):
        out.append(lax.rem(d, n))
        d = lax.div(d, n)
    return tuple(reversed(out))


def place():
    return tuple(lax.axis_index(name) for name in ROW_GRP)


def plane_order(y, x, nx):
    return lax.rem(x + y, nx) * nx + y


def prelude_kernel(
    sizes, reach, block_rows, slot_cap,
    owners_hbm, ids_hbm, feat_hbm,
    norm, unpack_out, pack_out, most_out,
    owners_ref, ids_ref, feat, sums, cnt, ends, joins, tail, got, mine, got_line, top, got_plane,
    load_sem, send_sem, recv_sem, line_send, line_recv, plane_send, plane_recv,
):
    ny, nz, nx, ng = sizes
    devices = ny * nz * nx * ng
    me = lax.axis_index(ROW_GRP)
    y, z, x, g = place()
    rows_dev, width = feat.shape
    tiles = rows_dev // TILE
    blocks = rows_dev // block_rows
    line = nz * ng
    plane = ny * nx
    loads = [
        pltpu.make_async_copy(src, dst, load_sem.at[n])
        for n, (src, dst) in enumerate(
            ((ids_hbm, ids_ref), (owners_hbm, owners_ref), (feat_hbm, feat))
        )
    ]
    for load in loads:
        load.start()

    def line_peer(j):
        return (y, lax.rem(z + j // ng, nz), x, lax.rem(g + j % ng, ng))

    def plane_peer(j):
        return (lax.rem(y + j // nx, ny), z, lax.rem(x + j % nx, nx), g)

    barrier = pltpu.get_barrier_semaphore()

    @pl.loop(1, reach + 1)
    def _(k):
        peer = lax.rem(me + devices - k, devices)
        pl.semaphore_signal(barrier, 1, device_id=coords(peer, sizes), device_id_type=MESH)

    for j in range(1, line):
        pl.semaphore_signal(barrier, 1, device_id=line_peer(j), device_id_type=MESH)
    for j in range(1, plane):
        pl.semaphore_signal(barrier, 1, device_id=plane_peer(j), device_id_type=MESH)

    loads[0].wait()
    ids = ids_ref[...]
    last = jnp.broadcast_to(ids[tiles - 1 :, TILE - 1 :], (1, TILE))
    in_last = jnp.where(ids == jnp.broadcast_to(last, ids.shape), 1.0, 0.0)
    count = jnp.sum(jnp.sum(in_last, axis=0, keepdims=True), axis=1, keepdims=True)
    first = jnp.broadcast_to(rows_dev - count.astype(jnp.int32), (8, width))
    step = 64
    sub = lax.broadcasted_iota(jnp.int32, (step, width), 0)
    loads[2].wait()

    @pl.loop(0, rows_dev // step, init_carry=jnp.zeros((step, width), jnp.float32), unroll=4)
    def open_rows(t, acc):
        at = pl.ds(pl.multiple_of(t * step, step), step)
        inside = sub + t * step >= jnp.broadcast_to(first[0:1], (step, width))
        return acc + jnp.where(inside, feat[at, :], 0.0)

    total = jnp.sum(open_rows, axis=0, keepdims=True)
    tail[0:1, :] = total[:, :TILE]
    tail[1:2, :] = total[:, TILE:]
    tail[2:3, :] = last.astype(jnp.float32)
    tail[3:4, :] = jnp.broadcast_to(count, (1, TILE))

    loads[1].wait()
    slots = ny * nz * nx * slot_cap
    owners = owners_ref[...]
    across = jnp.broadcast_to(owners, (blocks, blocks))
    down = jnp.broadcast_to(across.T[:, 0:1], (blocks, blocks))
    earlier = lax.broadcasted_iota(jnp.int32, (blocks, blocks), 1) < (
        lax.broadcasted_iota(jnp.int32, (blocks, blocks), 0)
    )
    rank = jnp.sum(jnp.where((across == down) & earlier, 1.0, 0.0), axis=1, keepdims=True)
    target = down[:, 0:1] * slot_cap + rank.astype(jnp.int32)
    hit = jnp.broadcast_to(target, (blocks, slots)) == (
        lax.broadcasted_iota(jnp.int32, (blocks, slots), 1)
    )
    used = jnp.sum(jnp.where(hit, 1.0, 0.0), axis=0, keepdims=True)
    o_from = lax.broadcasted_iota(jnp.int32, (slots, slots), 0)
    o_to = lax.broadcasted_iota(jnp.int32, (slots, slots), 1)

    def plane_of(o):
        return lax.rem(lax.div(o, nx), nz)

    def order_of(o):
        return plane_order(lax.div(o, nx * nz), lax.rem(o, nx), nx)

    ahead = (plane_of(o_from) == plane_of(o_to)) & (order_of(o_from) < order_of(o_to))
    before = jnp.dot(
        jnp.broadcast_to(used, (8, slots)).astype(jnp.bfloat16),
        jnp.where(ahead, 1.0, 0.0).astype(jnp.bfloat16),
        preferred_element_type=jnp.float32,
    )[0:1]
    spot = jnp.where(used > 0.0, before + 1.0, 0.0)
    mine[...] = spot.astype(jnp.int32)
    key = plane_of(o_to[0:1]).astype(jnp.float32) * plane + before
    block_key = jnp.sum(
        jnp.where(hit, jnp.broadcast_to(key, (blocks, slots)), 0.0), axis=1, keepdims=True
    )
    entry = lax.broadcasted_iota(jnp.int32, (blocks, slots), 1).astype(jnp.float32)
    order = lax.broadcasted_iota(jnp.int32, (blocks, slots), 0)
    pack_out[...] = jnp.sum(
        jnp.where(jnp.broadcast_to(block_key, (blocks, slots)) == entry, order, 0),
        axis=0, keepdims=True,
    )

    lane = lax.broadcasted_iota(jnp.int32, ids.shape, 1)
    after = pltpu.roll(ids, TILE - 1, 1)
    end = jnp.where((after != ids) | (lane == TILE - 1), lane, TILE)
    hop = 1
    while hop < TILE:
        nxt = jnp.where(lane + hop < TILE, pltpu.roll(end, TILE - hop, 1), TILE)
        end = jnp.minimum(end, nxt)
        hop *= 2
    ends[...] = end
    prior = jnp.concatenate([jnp.full((1, TILE), -1, jnp.int32), ids[:-1]], axis=0)
    prior = jnp.broadcast_to(prior[:, TILE - 1 :], ids.shape)
    goes_on = jnp.sum(jnp.where(ids == prior, 1.0, 0.0), axis=1, keepdims=True)
    joins[...] = jnp.broadcast_to(goes_on.astype(jnp.int32), ids.shape)

    pl.semaphore_wait(barrier, reach + line - 1 + plane - 1)

    @pl.loop(1, reach + 1)
    def _(k):
        peer = lax.rem(me + k, devices)
        pltpu.make_async_remote_copy(
            src_ref=tail, dst_ref=got.at[k - 1], send_sem=send_sem, recv_sem=recv_sem,
            device_id=coords(peer, sizes), device_id_type=MESH,
        ).start()

    for j in range(1, line):
        pltpu.make_async_remote_copy(
            src_ref=mine, dst_ref=got_line.at[j - 1], send_sem=line_send, recv_sem=line_recv,
            device_id=line_peer(j), device_id_type=MESH,
        ).start()

    row = lax.broadcasted_iota(jnp.int32, (TILE, TILE), 0)
    col = lax.broadcasted_iota(jnp.int32, (TILE, TILE), 1)
    causal = col <= row
    ones = jnp.ones((TILE, TILE), jnp.bfloat16)

    @pl.loop(
        0, tiles,
        init_carry=(jnp.zeros((1, width), jnp.float32), jnp.zeros((1, TILE), jnp.float32)),
        unroll=4,
    )
    def _(t, carry):
        open_sum, open_count = carry
        at = pl.ds(pl.multiple_of(t * TILE, TILE), TILE)
        alive = row <= jnp.broadcast_to(ends[pl.ds(t, 1), :], (TILE, TILE))
        mask = jnp.where(alive & causal, 1.0, 0.0).astype(jnp.bfloat16)
        rows = feat[at, :]
        high = rows.astype(jnp.bfloat16)
        rest = rows - high.astype(jnp.float32)
        mid = rest.astype(jnp.bfloat16)
        low = (rest - mid.astype(jnp.float32)).astype(jnp.bfloat16)
        inside = (
            jnp.dot(mask, high, preferred_element_type=jnp.float32)
            + jnp.dot(mask, mid, preferred_element_type=jnp.float32)
            + jnp.dot(mask, low, preferred_element_type=jnp.float32)
        )
        number = jnp.dot(mask, ones, preferred_element_type=jnp.float32)
        joined = row < jnp.broadcast_to(joins[pl.ds(t, 1), :], (TILE, TILE))
        both = jnp.concatenate([joined, joined], axis=1)
        inside = inside + jnp.where(both, jnp.broadcast_to(open_sum, (TILE, width)), 0.0)
        number = number + jnp.where(joined, jnp.broadcast_to(open_count, (TILE, TILE)), 0.0)
        sums[at, :] = inside
        cnt[at, :] = number
        return inside[TILE - 1 :, :], number[TILE - 1 :, :]

    pltpu.make_async_copy(got_line, got_line, line_recv).wait()
    spots = mine[...]
    unpack_out[0:1, :] = spots
    largest = spots
    for j in range(1, line):
        spots = got_line[j - 1]
        largest = jnp.maximum(largest, spots)
        if j % ng == 0:
            unpack_out[j // ng : j // ng + 1, :] = spots
    top[...] = largest

    pltpu.make_async_copy(got, got, recv_sem).wait()

    for j in range(1, plane):
        pltpu.make_async_remote_copy(
            src_ref=top, dst_ref=got_plane.at[j - 1], send_sem=plane_send,
            recv_sem=plane_recv, device_id=plane_peer(j), device_id_type=MESH,
        ).start()

    arrived = got[...]
    open_id = arrived[0, 2:3, :]
    age = lax.broadcasted_iota(jnp.int32, arrived.shape, 0) + 1
    same = jnp.broadcast_to(arrived[:, 2:3, :], arrived.shape) == jnp.broadcast_to(
        open_id[None], arrived.shape
    )
    merged = jnp.sum(jnp.where(same & (age <= me), arrived, 0.0), axis=0)
    open_sum = jnp.concatenate([merged[0:1, :], merged[1:2, :]], axis=1)
    open_count = merged[3:4, :]
    in_open = jnp.where(
        ids.astype(jnp.float32) == jnp.broadcast_to(open_id, ids.shape), 1.0, 0.0
    )
    reached = jnp.sum(jnp.sum(in_open, axis=0, keepdims=True), axis=1, keepdims=True)
    reached = jnp.broadcast_to(reached.astype(jnp.int32), (1, TILE))
    sub = lax.broadcasted_iota(jnp.int32, (block_rows, TILE), 0)

    @pl.loop(0, blocks, unroll=4)
    def _(b):
        at = pl.ds(pl.multiple_of(b * block_rows, block_rows), block_rows)
        joined = sub + b * block_rows < jnp.broadcast_to(reached, (block_rows, TILE))
        number = cnt[at, :] + jnp.where(
            joined, jnp.broadcast_to(open_count, (block_rows, TILE)), 0.0
        )
        scale = 1.0 / jnp.sqrt(number)
        both = jnp.concatenate([joined, joined], axis=1)
        rows = sums[at, :] + jnp.where(
            both, jnp.broadcast_to(open_sum, (block_rows, width)), 0.0
        )
        norm[b] = (rows * jnp.concatenate([scale, scale], axis=1)).astype(jnp.bfloat16)

    pltpu.make_async_copy(got_plane, got_plane, plane_recv).wait()
    for j in range(1, plane):
        largest = jnp.maximum(largest, got_plane[j - 1])
    most = jnp.max(largest.astype(jnp.float32), axis=1, keepdims=True).astype(jnp.int32)
    most_out[...] = jnp.broadcast_to(most, most_out.shape)
    pltpu.make_async_copy(got, got, send_sem).wait()
    pltpu.make_async_copy(got_line, got_line, line_send).wait()
    pltpu.make_async_copy(got_plane, got_plane, plane_send).wait()


def arrivals(sizes, room):
    ny, nz, nx, ng = sizes
    steps = []
    for d in range(1, nz // 2):
        steps += [(d, 0, room), (nz - d, 0, room)]
    cuts = list(range(0, room, nx))[:ny] + [room]
    return steps, [(nz // 2, a, b) for a, b in zip(cuts[:-1], cuts[1:])]


def exchange_kernel(
    sizes, room,
    pack, unpack, norm, out,
    send, stage, z_send, z_recv, p_send, p_recv, *recv,
):
    ny, nz, nx, ng = sizes
    plane = ny * nx
    y, z, x, g = place()
    steps, parts = arrivals(sizes, room)
    far = nz // 2
    barrier = pltpu.get_barrier_semaphore()

    def z_peer(d):
        return (y, lax.rem(z + d, nz), x, g)

    for d in range(1, nz):
        pl.semaphore_signal(barrier, 1, device_id=z_peer(d), device_id_type=MESH)
    for j in range(1, plane):
        pl.semaphore_signal(
            barrier, 1, device_id_type=MESH,
            device_id=(lax.rem(y + j // nx, ny), z, lax.rem(x + j % nx, nx), g),
        )

    for d in [d for d, _, _ in steps] + [far]:
        first = lax.rem(z + d, nz) * plane

        @pl.loop(0, room)
        def _(k):
            send[d - 1, k] = norm[pack[0, first + k]]

    pl.semaphore_wait(barrier, nz - 1 + plane - 1)

    for n, (d, a, b) in enumerate(steps + parts):
        pltpu.make_async_remote_copy(
            src_ref=send.at[d - 1, pl.ds(a, b - a)], dst_ref=recv[n],
            send_sem=z_send, recv_sem=z_recv.at[n],
            device_id=z_peer(d), device_id_type=MESH,
        ).start()

    def wanted(d, ty, tx, pieces):
        spot = unpack[d, (ty * nz + z) * nx + tx]
        block = None
        for ref, a, b in pieces:
            one = ref[jnp.clip(spot - 1 - a, 0, b - a - 1)]
            block = one if block is None else jnp.where(spot > a, one, block)
        return jnp.where(spot > 0, block, jnp.zeros_like(block))

    def own(ty, tx):
        spot = unpack[0, (ty * nz + z) * nx + tx]
        block = norm[pack[0, z * plane + jnp.maximum(spot, 1) - 1]]
        return jnp.where(spot > 0, block, jnp.zeros_like(block))

    def slot_from(d):
        return (y * nz + lax.rem(z + nz - d, nz)) * nx + x

    def p_copy(d, j, ty, tx):
        return pltpu.make_async_remote_copy(
            src_ref=stage.at[d, j], dst_ref=out.at[slot_from(d)],
            send_sem=p_send, recv_sem=p_recv,
            device_id=(ty, z, tx, g), device_id_type=MESH,
        )

    def deliver(d, block_for):
        def target(j):
            return lax.rem(y + lax.div(j, nx), ny), lax.rem(x + lax.rem(j, nx), nx)

        @pl.loop(1, plane)
        def _(j):
            stage[d, j] = block_for(*target(j))

        @pl.loop(1, plane)
        def _(j):
            p_copy(d, j, *target(j)).start()

        out[slot_from(d)] = block_for(y, x)

    deliver(0, own)
    for n, (d, a, b) in enumerate(steps):
        pltpu.make_async_copy(recv[n], recv[n], z_recv.at[n]).wait()
        pieces = [(recv[n], a, b)]
        deliver(d, lambda ty, tx: wanted(d, ty, tx, pieces))

    pieces = []
    for h in range(ny):
        if h < len(parts):
            n = len(steps) + h
            pltpu.make_async_copy(recv[n], recv[n], z_recv.at[n]).wait()
            pieces.append((recv[n], *parts[h][1:]))

        def target(j):
            ty = lax.rem(y + j, ny)
            return ty, lax.rem(h + ny - ty, nx)

        @pl.loop(0, nx)
        def _(j):
            stage[far, h * nx + j] = wanted(far, *target(j), pieces)

        @pl.loop(0, nx)
        def _(j):
            ty, tx = target(j)

            @pl.when((ty - y) * nx + tx - x != 0)
            def _():
                p_copy(far, h * nx + j, ty, tx).start()

    out[slot_from(far)] = wanted(far, y, x, pieces)

    pltpu.make_async_copy(send, send, z_send).wait()
    landed = out.at[pl.ds(0, nz * (plane - 1))]
    pltpu.make_async_copy(landed, landed, p_send).wait()
    pltpu.make_async_copy(landed, landed, p_recv).wait()


def body(features, session, owner_map):
    rows_dev, width = features.shape
    blocks = owner_map.shape[1]
    block_rows = rows_dev // blocks
    sizes = tuple(lax.axis_size(name) for name in ROW_GRP)
    ny, nz, nx, ng = sizes
    plane = ny * nx
    slot_cap = max(1, 2 * blocks // (plane * nz))
    slots = plane * nz * slot_cap
    tiles = rows_dev // TILE
    reach = (MOST - 2) // rows_dev + 1
    norm, unpack, pack, most = pl.pallas_call(
        lambda *refs: prelude_kernel(sizes, reach, block_rows, slot_cap, *refs),
        out_shape=(
            jax.ShapeDtypeStruct((blocks, block_rows, width), jnp.bfloat16),
            jax.ShapeDtypeStruct((nz, slots), jnp.int32),
            jax.ShapeDtypeStruct((1, slots), jnp.int32),
            jax.ShapeDtypeStruct((1, TILE), jnp.int32),
        ),
        in_specs=[pl.BlockSpec(memory_space=pltpu.HBM)] * 3,
        out_specs=[pl.BlockSpec(memory_space=pltpu.VMEM)] * 4,
        scratch_shapes=[
            pltpu.VMEM(owner_map.shape, jnp.int32),
            pltpu.VMEM((tiles, TILE), jnp.int32),
            pltpu.VMEM((rows_dev, width), jnp.float32),
            pltpu.VMEM((rows_dev, width), jnp.float32),
            pltpu.VMEM((rows_dev, TILE), jnp.float32),
            pltpu.VMEM((tiles, TILE), jnp.int32),
            pltpu.VMEM((tiles, TILE), jnp.int32),
            pltpu.VMEM((4, TILE), jnp.float32),
            pltpu.VMEM((reach, 4, TILE), jnp.float32),
            pltpu.VMEM((1, slots), jnp.int32),
            pltpu.VMEM((nz * ng - 1, 1, slots), jnp.int32),
            pltpu.VMEM((1, slots), jnp.int32),
            pltpu.VMEM((plane - 1, 1, slots), jnp.int32),
            pltpu.SemaphoreType.DMA((3,)),
        ]
        + [pltpu.SemaphoreType.DMA] * 6,
        compiler_params=pltpu.CompilerParams(
            collective_id=0, has_side_effects=True, vmem_limit_bytes=24 << 20
        ),
        name="prelude",
    )(owner_map, session.reshape(tiles, TILE), features)

    def exchange(room, number):
        block = (block_rows, width)
        return lambda pack, unpack, norm: pl.pallas_call(
            lambda *refs: exchange_kernel(sizes, room, *refs),
            out_shape=jax.ShapeDtypeStruct((slots, *block), jnp.bfloat16),
            in_specs=[
                pl.BlockSpec(memory_space=pltpu.SMEM),
                pl.BlockSpec(memory_space=pltpu.SMEM),
                pl.BlockSpec(memory_space=pltpu.VMEM),
            ],
            out_specs=pl.BlockSpec(memory_space=pltpu.VMEM),
            scratch_shapes=[
                pltpu.VMEM((nz - 1, room, *block), jnp.bfloat16),
                pltpu.VMEM((nz, plane, *block), jnp.bfloat16),
                pltpu.SemaphoreType.DMA,
                pltpu.SemaphoreType.DMA((nz + ny,)),
                pltpu.SemaphoreType.DMA,
                pltpu.SemaphoreType.DMA,
            ]
            + [
                pltpu.VMEM((b - a, *block), jnp.bfloat16)
                for group in arrivals(sizes, room)
                for _, a, b in group
            ],
            compiler_params=pltpu.CompilerParams(
                collective_id=number, has_side_effects=True, vmem_limit_bytes=24 << 20
            ),
            name=f"exchange_{room}",
        )(pack, unpack, norm)

    rooms = ROOMS
    choice = sum((most[0, 0] > room).astype(jnp.int32) for room in rooms[:-1])
    return lax.switch(
        choice, [exchange(room, 1 + n) for n, room in enumerate(rooms)], pack, unpack, norm
    )


def solution(mesh):
    split = Mesh(
        mesh.devices.reshape(4, 8, 4, mesh.shape["grp"]), ("row_0", "row_1", "row_2", "grp")
    )
    return jax.shard_map(
        body,
        mesh=split,
        in_specs=(P(ROW_GRP, None), P(ROW_GRP), P(ROW_GRP, None)),
        out_specs=P(ROW_GRP, None, None),
        check_vma=False,
    )
```

```python
import jax
import jax.numpy as jnp
from jax import lax
from jax.experimental import pallas as pl
from jax.experimental.pallas import tpu as pltpu
from jax.sharding import Mesh
from jax.sharding import PartitionSpec as P

ROW = ("row_0", "row_1", "row_2")
ROW_GRP = ("row_0", "row_1", "row_2", "grp")
MOST = 163840
TILE = 128
ROOMS = (12, 13, 14, 15, 16)
MESH = pl.DeviceIdType.MESH


def coords(d, sizes):
    out = []
    for n in reversed(sizes):
        out.append(lax.rem(d, n))
        d = lax.div(d, n)
    return tuple(reversed(out))


def place():
    return tuple(lax.axis_index(name) for name in ROW_GRP)


def plane_order(y, x, nx):
    return lax.rem(x + y, nx) * nx + y


def prelude_kernel(
    sizes, reach, block_rows, slot_cap,
    owners_hbm, ids_hbm, feat_hbm,
    norm, unpack_out, pack_out, most_out,
    owners_ref, ids_ref, feat, sums, cnt, ends, joins, tail, got, mine, got_line, top, got_plane,
    load_sem, send_sem, recv_sem, line_send, line_recv, plane_send, plane_recv,
):
    ny, nz, nx, ng = sizes
    devices = ny * nz * nx * ng
    me = lax.axis_index(ROW_GRP)
    y, z, x, g = place()
    rows_dev, width = feat.shape
    tiles = rows_dev // TILE
    blocks = rows_dev // block_rows
    line = nz * ng
    plane = ny * nx
    loads = [
        pltpu.make_async_copy(src, dst, load_sem.at[n])
        for n, (src, dst) in enumerate(
            ((ids_hbm, ids_ref), (owners_hbm, owners_ref), (feat_hbm, feat))
        )
    ]
    for load in loads:
        load.start()

    def line_peer(j):
        return (y, lax.rem(z + j // ng, nz), x, lax.rem(g + j % ng, ng))

    def plane_peer(j):
        return (lax.rem(y + j // nx, ny), z, lax.rem(x + j % nx, nx), g)

    barrier = pltpu.get_barrier_semaphore()

    @pl.loop(1, reach + 1)
    def _(k):
        peer = lax.rem(me + devices - k, devices)
        pl.semaphore_signal(barrier, 1, device_id=coords(peer, sizes), device_id_type=MESH)

    for j in range(1, line):
        pl.semaphore_signal(barrier, 1, device_id=line_peer(j), device_id_type=MESH)
    for j in range(1, plane):
        pl.semaphore_signal(barrier, 1, device_id=plane_peer(j), device_id_type=MESH)

    loads[0].wait()
    ids = ids_ref[...]
    last = jnp.broadcast_to(ids[tiles - 1 :, TILE - 1 :], (1, TILE))
    in_last = jnp.where(ids == jnp.broadcast_to(last, ids.shape), 1.0, 0.0)
    count = jnp.sum(jnp.sum(in_last, axis=0, keepdims=True), axis=1, keepdims=True)
    first = jnp.broadcast_to(rows_dev - count.astype(jnp.int32), (8, width))
    step = 64
    sub = lax.broadcasted_iota(jnp.int32, (step, width), 0)
    loads[2].wait()

    @pl.loop(0, rows_dev // step, init_carry=jnp.zeros((step, width), jnp.float32), unroll=4)
    def open_rows(t, acc):
        at = pl.ds(pl.multiple_of(t * step, step), step)
        inside = sub + t * step >= jnp.broadcast_to(first[0:1], (step, width))
        return acc + jnp.where(inside, feat[at, :], 0.0)

    total = jnp.sum(open_rows, axis=0, keepdims=True)
    tail[0:1, :] = total[:, :TILE]
    tail[1:2, :] = total[:, TILE:]
    tail[2:3, :] = last.astype(jnp.float32)
    tail[3:4, :] = jnp.broadcast_to(count, (1, TILE))

    loads[1].wait()
    slots = ny * nz * nx * slot_cap
    owners = owners_ref[...]
    across = jnp.broadcast_to(owners, (blocks, blocks))
    down = jnp.broadcast_to(across.T[:, 0:1], (blocks, blocks))
    earlier = lax.broadcasted_iota(jnp.int32, (blocks, blocks), 1) < (
        lax.broadcasted_iota(jnp.int32, (blocks, blocks), 0)
    )
    rank = jnp.sum(jnp.where((across == down) & earlier, 1.0, 0.0), axis=1, keepdims=True)
    target = down[:, 0:1] * slot_cap + rank.astype(jnp.int32)
    hit = jnp.broadcast_to(target, (blocks, slots)) == (
        lax.broadcasted_iota(jnp.int32, (blocks, slots), 1)
    )
    used = jnp.sum(jnp.where(hit, 1.0, 0.0), axis=0, keepdims=True)
    o_from = lax.broadcasted_iota(jnp.int32, (slots, slots), 0)
    o_to = lax.broadcasted_iota(jnp.int32, (slots, slots), 1)

    def plane_of(o):
        return lax.rem(lax.div(o, nx), nz)

    def order_of(o):
        return plane_order(lax.div(o, nx * nz), lax.rem(o, nx), nx)

    ahead = (plane_of(o_from) == plane_of(o_to)) & (order_of(o_from) < order_of(o_to))
    before = jnp.dot(
        jnp.broadcast_to(used, (8, slots)).astype(jnp.bfloat16),
        jnp.where(ahead, 1.0, 0.0).astype(jnp.bfloat16),
        preferred_element_type=jnp.float32,
    )[0:1]
    spot = jnp.where(used > 0.0, before + 1.0, 0.0)
    mine[...] = spot.astype(jnp.int32)
    key = plane_of(o_to[0:1]).astype(jnp.float32) * plane + before
    block_key = jnp.sum(
        jnp.where(hit, jnp.broadcast_to(key, (blocks, slots)), 0.0), axis=1, keepdims=True
    )
    entry = lax.broadcasted_iota(jnp.int32, (blocks, slots), 1).astype(jnp.float32)
    order = lax.broadcasted_iota(jnp.int32, (blocks, slots), 0)
    pack_out[...] = jnp.sum(
        jnp.where(jnp.broadcast_to(block_key, (blocks, slots)) == entry, order, 0),
        axis=0, keepdims=True,
    )

    lane = lax.broadcasted_iota(jnp.int32, ids.shape, 1)
    after = pltpu.roll(ids, TILE - 1, 1)
    end = jnp.where((after != ids) | (lane == TILE - 1), lane, TILE)
    hop = 1
    while hop < TILE:
        nxt = jnp.where(lane + hop < TILE, pltpu.roll(end, TILE - hop, 1), TILE)
        end = jnp.minimum(end, nxt)
        hop *= 2
    ends[...] = end
    prior = jnp.concatenate([jnp.full((1, TILE), -1, jnp.int32), ids[:-1]], axis=0)
    prior = jnp.broadcast_to(prior[:, TILE - 1 :], ids.shape)
    goes_on = jnp.sum(jnp.where(ids == prior, 1.0, 0.0), axis=1, keepdims=True)
    joins[...] = jnp.broadcast_to(goes_on.astype(jnp.int32), ids.shape)

    pl.semaphore_wait(barrier, reach + line - 1 + plane - 1)

    @pl.loop(1, reach + 1)
    def _(k):
        peer = lax.rem(me + k, devices)
        pltpu.make_async_remote_copy(
            src_ref=tail, dst_ref=got.at[k - 1], send_sem=send_sem, recv_sem=recv_sem,
            device_id=coords(peer, sizes), device_id_type=MESH,
        ).start()

    for j in range(1, line):
        pltpu.make_async_remote_copy(
            src_ref=mine, dst_ref=got_line.at[j - 1], send_sem=line_send, recv_sem=line_recv,
            device_id=line_peer(j), device_id_type=MESH,
        ).start()

    row = lax.broadcasted_iota(jnp.int32, (TILE, TILE), 0)
    col = lax.broadcasted_iota(jnp.int32, (TILE, TILE), 1)
    causal = col <= row
    ones = jnp.ones((TILE, TILE), jnp.bfloat16)

    @pl.loop(
        0, tiles,
        init_carry=(jnp.zeros((1, width), jnp.float32), jnp.zeros((1, TILE), jnp.float32)),
        unroll=4,
    )
    def _(t, carry):
        open_sum, open_count = carry
        at = pl.ds(pl.multiple_of(t * TILE, TILE), TILE)
        alive = row <= jnp.broadcast_to(ends[pl.ds(t, 1), :], (TILE, TILE))
        mask = jnp.where(alive & causal, 1.0, 0.0).astype(jnp.bfloat16)
        rows = feat[at, :]
        high = rows.astype(jnp.bfloat16)
        rest = rows - high.astype(jnp.float32)
        mid = rest.astype(jnp.bfloat16)
        low = (rest - mid.astype(jnp.float32)).astype(jnp.bfloat16)
        inside = (
            jnp.dot(mask, high, preferred_element_type=jnp.float32)
            + jnp.dot(mask, mid, preferred_element_type=jnp.float32)
            + jnp.dot(mask, low, preferred_element_type=jnp.float32)
        )
        number = jnp.dot(mask, ones, preferred_element_type=jnp.float32)
        joined = row < jnp.broadcast_to(joins[pl.ds(t, 1), :], (TILE, TILE))
        both = jnp.concatenate([joined, joined], axis=1)
        inside = inside + jnp.where(both, jnp.broadcast_to(open_sum, (TILE, width)), 0.0)
        number = number + jnp.where(joined, jnp.broadcast_to(open_count, (TILE, TILE)), 0.0)
        sums[at, :] = inside
        cnt[at, :] = number
        return inside[TILE - 1 :, :], number[TILE - 1 :, :]

    pltpu.make_async_copy(got_line, got_line, line_recv).wait()
    spots = mine[...]
    unpack_out[0:1, :] = spots
    largest = spots
    for j in range(1, line):
        spots = got_line[j - 1]
        largest = jnp.maximum(largest, spots)
        if j % ng == 0:
            unpack_out[j // ng : j // ng + 1, :] = spots
    top[...] = largest

    pltpu.make_async_copy(got, got, recv_sem).wait()

    for j in range(1, plane):
        pltpu.make_async_remote_copy(
            src_ref=top, dst_ref=got_plane.at[j - 1], send_sem=plane_send,
            recv_sem=plane_recv, device_id=plane_peer(j), device_id_type=MESH,
        ).start()

    arrived = got[...]
    open_id = arrived[0, 2:3, :]
    age = lax.broadcasted_iota(jnp.int32, arrived.shape, 0) + 1
    same = jnp.broadcast_to(arrived[:, 2:3, :], arrived.shape) == jnp.broadcast_to(
        open_id[None], arrived.shape
    )
    merged = jnp.sum(jnp.where(same & (age <= me), arrived, 0.0), axis=0)
    open_sum = jnp.concatenate([merged[0:1, :], merged[1:2, :]], axis=1)
    open_count = merged[3:4, :]
    in_open = jnp.where(
        ids.astype(jnp.float32) == jnp.broadcast_to(open_id, ids.shape), 1.0, 0.0
    )
    reached = jnp.sum(jnp.sum(in_open, axis=0, keepdims=True), axis=1, keepdims=True)
    reached = jnp.broadcast_to(reached.astype(jnp.int32), (1, TILE))
    sub = lax.broadcasted_iota(jnp.int32, (block_rows, TILE), 0)

    @pl.loop(0, blocks, unroll=4)
    def _(b):
        at = pl.ds(pl.multiple_of(b * block_rows, block_rows), block_rows)
        joined = sub + b * block_rows < jnp.broadcast_to(reached, (block_rows, TILE))
        number = cnt[at, :] + jnp.where(
            joined, jnp.broadcast_to(open_count, (block_rows, TILE)), 0.0
        )
        scale = 1.0 / jnp.sqrt(number)
        both = jnp.concatenate([joined, joined], axis=1)
        rows = sums[at, :] + jnp.where(
            both, jnp.broadcast_to(open_sum, (block_rows, width)), 0.0
        )
        norm[b] = (rows * jnp.concatenate([scale, scale], axis=1)).astype(jnp.bfloat16)

    pltpu.make_async_copy(got_plane, got_plane, plane_recv).wait()
    for j in range(1, plane):
        largest = jnp.maximum(largest, got_plane[j - 1])
    most = jnp.max(largest.astype(jnp.float32), axis=1, keepdims=True).astype(jnp.int32)
    most_out[...] = jnp.broadcast_to(most, most_out.shape)
    pltpu.make_async_copy(got, got, send_sem).wait()
    pltpu.make_async_copy(got_line, got_line, line_send).wait()
    pltpu.make_async_copy(got_plane, got_plane, plane_send).wait()


def arrivals(sizes, room):
    ny, nz, nx, ng = sizes
    steps = []
    for d in range(1, nz // 2):
        steps += [(d, 0, room), (nz - d, 0, room)]
    cuts = list(range(0, room, nx))[:ny] + [room]
    return steps, [(nz // 2, a, b) for a, b in zip(cuts[:-1], cuts[1:])]


def exchange_kernel(
    sizes, room,
    pack, unpack, norm, out,
    send, stage, z_send, z_recv, p_send, p_recv, *recv,
):
    ny, nz, nx, ng = sizes
    plane = ny * nx
    y, z, x, g = place()
    steps, parts = arrivals(sizes, room)
    far = nz // 2
    barrier = pltpu.get_barrier_semaphore()

    def z_peer(d):
        return (y, lax.rem(z + d, nz), x, g)

    for d in range(1, nz):
        pl.semaphore_signal(barrier, 1, device_id=z_peer(d), device_id_type=MESH)
    for j in range(1, plane):
        pl.semaphore_signal(
            barrier, 1, device_id_type=MESH,
            device_id=(lax.rem(y + j // nx, ny), z, lax.rem(x + j % nx, nx), g),
        )

    for d in [d for d, _, _ in steps] + [far]:
        first = lax.rem(z + d, nz) * plane

        @pl.loop(0, room)
        def _(k):
            send[d - 1, k] = norm[pack[0, first + k]]

    pl.semaphore_wait(barrier, nz - 1 + plane - 1)

    for n, (d, a, b) in enumerate(steps + parts):
        pltpu.make_async_remote_copy(
            src_ref=send.at[d - 1, pl.ds(a, b - a)], dst_ref=recv[n],
            send_sem=z_send, recv_sem=z_recv.at[n],
            device_id=z_peer(d), device_id_type=MESH,
        ).start()

    def wanted(d, ty, tx, pieces):
        spot = unpack[d, (ty * nz + z) * nx + tx]
        block = None
        for ref, a, b in pieces:
            one = ref[jnp.clip(spot - 1 - a, 0, b - a - 1)]
            block = one if block is None else jnp.where(spot > a, one, block)
        return jnp.where(spot > 0, block, jnp.zeros_like(block))

    def own(ty, tx):
        spot = unpack[0, (ty * nz + z) * nx + tx]
        block = norm[pack[0, z * plane + jnp.maximum(spot, 1) - 1]]
        return jnp.where(spot > 0, block, jnp.zeros_like(block))

    def slot_from(d):
        return (y * nz + lax.rem(z + nz - d, nz)) * nx + x

    def p_copy(d, j, ty, tx):
        return pltpu.make_async_remote_copy(
            src_ref=stage.at[d, j], dst_ref=out.at[slot_from(d)],
            send_sem=p_send, recv_sem=p_recv,
            device_id=(ty, z, tx, g), device_id_type=MESH,
        )

    def deliver(d, block_for):
        def target(j):
            return lax.rem(y + lax.div(j, nx), ny), lax.rem(x + lax.rem(j, nx), nx)

        @pl.loop(1, plane)
        def _(j):
            stage[d, j] = block_for(*target(j))

        @pl.loop(1, plane)
        def _(j):
            p_copy(d, j, *target(j)).start()

        out[slot_from(d)] = block_for(y, x)

    deliver(0, own)
    for n, (d, a, b) in enumerate(steps):
        pltpu.make_async_copy(recv[n], recv[n], z_recv.at[n]).wait()
        pieces = [(recv[n], a, b)]
        deliver(d, lambda ty, tx: wanted(d, ty, tx, pieces))

    pieces = []
    for h in range(ny):
        if h < len(parts):
            n = len(steps) + h
            pltpu.make_async_copy(recv[n], recv[n], z_recv.at[n]).wait()
            pieces.append((recv[n], *parts[h][1:]))

        def target(j):
            ty = lax.rem(y + j, ny)
            return ty, lax.rem(h + ny - ty, nx)

        @pl.loop(0, nx)
        def _(j):
            stage[far, h * nx + j] = wanted(far, *target(j), pieces)

        @pl.loop(0, nx)
        def _(j):
            ty, tx = target(j)

            @pl.when((ty - y) * nx + tx - x != 0)
            def _():
                p_copy(far, h * nx + j, ty, tx).start()

    out[slot_from(far)] = wanted(far, y, x, pieces)

    pltpu.make_async_copy(send, send, z_send).wait()
    landed = out.at[pl.ds(0, nz * (plane - 1))]
    pltpu.make_async_copy(landed, landed, p_send).wait()
    pltpu.make_async_copy(landed, landed, p_recv).wait()


def to_hbm_kernel(src, out, sem):
    parts = sem.shape[0]
    size = src.shape[0] // parts
    copies = [
        pltpu.make_async_copy(
            src.at[pl.ds(n * size, size)], out.at[pl.ds(n * size, size)], sem.at[n]
        )
        for n in range(parts)
    ]
    for copy in copies:
        copy.start()
    for copy in copies:
        copy.wait()


def to_hbm(array):
    return pl.pallas_call(
        to_hbm_kernel,
        out_shape=pltpu.HBM(array.shape, array.dtype),
        in_specs=[pl.BlockSpec(memory_space=pltpu.VMEM)],
        out_specs=pl.BlockSpec(memory_space=pltpu.HBM),
        scratch_shapes=[pltpu.SemaphoreType.DMA((4,))],
        compiler_params=pltpu.CompilerParams(vmem_limit_bytes=1 << 20),
        name="to_hbm",
    )(array)


def body(features, session, owner_map):
    rows_dev, width = features.shape
    blocks = owner_map.shape[1]
    block_rows = rows_dev // blocks
    sizes = tuple(lax.axis_size(name) for name in ROW_GRP)
    ny, nz, nx, ng = sizes
    plane = ny * nx
    slot_cap = max(1, 2 * blocks // (plane * nz))
    slots = plane * nz * slot_cap
    tiles = rows_dev // TILE
    reach = (MOST - 2) // rows_dev + 1
    norm, unpack, pack, most = pl.pallas_call(
        lambda *refs: prelude_kernel(sizes, reach, block_rows, slot_cap, *refs),
        out_shape=(
            jax.ShapeDtypeStruct((blocks, block_rows, width), jnp.bfloat16),
            jax.ShapeDtypeStruct((nz, slots), jnp.int32),
            jax.ShapeDtypeStruct((1, slots), jnp.int32),
            jax.ShapeDtypeStruct((1, TILE), jnp.int32),
        ),
        in_specs=[pl.BlockSpec(memory_space=pltpu.HBM)] * 3,
        out_specs=[pl.BlockSpec(memory_space=pltpu.VMEM)] * 4,
        scratch_shapes=[
            pltpu.VMEM(owner_map.shape, jnp.int32),
            pltpu.VMEM((tiles, TILE), jnp.int32),
            pltpu.VMEM((rows_dev, width), jnp.float32),
            pltpu.VMEM((rows_dev, width), jnp.float32),
            pltpu.VMEM((rows_dev, TILE), jnp.float32),
            pltpu.VMEM((tiles, TILE), jnp.int32),
            pltpu.VMEM((tiles, TILE), jnp.int32),
            pltpu.VMEM((4, TILE), jnp.float32),
            pltpu.VMEM((reach, 4, TILE), jnp.float32),
            pltpu.VMEM((1, slots), jnp.int32),
            pltpu.VMEM((nz * ng - 1, 1, slots), jnp.int32),
            pltpu.VMEM((1, slots), jnp.int32),
            pltpu.VMEM((plane - 1, 1, slots), jnp.int32),
            pltpu.SemaphoreType.DMA((3,)),
        ]
        + [pltpu.SemaphoreType.DMA] * 6,
        compiler_params=pltpu.CompilerParams(
            collective_id=0, has_side_effects=True, vmem_limit_bytes=24 << 20
        ),
        name="prelude",
    )(
        *(
            pltpu.with_memory_space_constraint(arg, pltpu.HBM)
            for arg in (owner_map, session.reshape(tiles, TILE), features)
        )
    )

    def exchange(room, number):
        block = (block_rows, width)
        return lambda pack, unpack, norm: to_hbm(pl.pallas_call(
            lambda *refs: exchange_kernel(sizes, room, *refs),
            out_shape=pltpu.VMEM((slots, *block), jnp.bfloat16),
            in_specs=[
                pl.BlockSpec(memory_space=pltpu.SMEM),
                pl.BlockSpec(memory_space=pltpu.SMEM),
                pl.BlockSpec(memory_space=pltpu.VMEM),
            ],
            out_specs=pl.BlockSpec(memory_space=pltpu.VMEM),
            scratch_shapes=[
                pltpu.VMEM((nz - 1, room, *block), jnp.bfloat16),
                pltpu.VMEM((nz, plane, *block), jnp.bfloat16),
                pltpu.SemaphoreType.DMA,
                pltpu.SemaphoreType.DMA((nz + ny,)),
                pltpu.SemaphoreType.DMA,
                pltpu.SemaphoreType.DMA,
            ]
            + [
                pltpu.VMEM((b - a, *block), jnp.bfloat16)
                for group in arrivals(sizes, room)
                for _, a, b in group
            ],
            compiler_params=pltpu.CompilerParams(
                collective_id=number, has_side_effects=True, vmem_limit_bytes=24 << 20
            ),
            name=f"exchange_{room}",
        )(pack, unpack, norm))

    rooms = ROOMS
    choice = sum((most[0, 0] > room).astype(jnp.int32) for room in rooms[:-1])
    return lax.switch(
        choice, [exchange(room, 1 + n) for n, room in enumerate(rooms)], pack, unpack, norm
    )


def solution(mesh):
    split = Mesh(
        mesh.devices.reshape(4, 8, 4, mesh.shape["grp"]), ("row_0", "row_1", "row_2", "grp")
    )
    return jax.shard_map(
        body,
        mesh=split,
        in_specs=(P(ROW_GRP, None), P(ROW_GRP), P(ROW_GRP, None)),
        out_specs=P(ROW_GRP, None, None),
        check_vma=False,
    )
```

```python
import jax
import jax.numpy as jnp
from jax import lax
from jax.experimental import pallas as pl
from jax.experimental.pallas import tpu as pltpu
from jax.sharding import Mesh
from jax.sharding import PartitionSpec as P

ROW = ("row_0", "row_1", "row_2")
ROW_GRP = ("row_0", "row_1", "row_2", "grp")
MOST = 163840
TILE = 128
ROOMS = (12, 13, 14, 15, 16)
MESH = pl.DeviceIdType.MESH


def coords(d, sizes):
    out = []
    for n in reversed(sizes):
        out.append(lax.rem(d, n))
        d = lax.div(d, n)
    return tuple(reversed(out))


def place():
    return tuple(lax.axis_index(name) for name in ROW_GRP)


def plane_order(y, x, nx):
    return lax.rem(x + y, nx) * nx + y


def prelude_kernel(
    sizes, reach, block_rows, slot_cap,
    owners_hbm, ids_hbm, feat_hbm,
    norm, unpack_out, pack_out, most_out,
    owners_ref, ids_ref, feat, sums, cnt, ends, joins, tail, got, mine, got_line, top, got_plane,
    load_sem, send_sem, recv_sem, line_send, line_recv, plane_send, plane_recv,
):
    ny, nz, nx, ng = sizes
    devices = ny * nz * nx * ng
    me = lax.axis_index(ROW_GRP)
    y, z, x, g = place()
    rows_dev, width = feat.shape
    tiles = rows_dev // TILE
    blocks = rows_dev // block_rows
    line = nz * ng
    plane = ny * nx
    loads = [
        pltpu.make_async_copy(src, dst, load_sem.at[n])
        for n, (src, dst) in enumerate(
            ((ids_hbm, ids_ref), (owners_hbm, owners_ref), (feat_hbm, feat))
        )
    ]
    for load in loads:
        load.start()

    def line_peer(j):
        return (y, lax.rem(z + j // ng, nz), x, lax.rem(g + j % ng, ng))

    def plane_peer(j):
        return (lax.rem(y + j // nx, ny), z, lax.rem(x + j % nx, nx), g)

    barrier = pltpu.get_barrier_semaphore()

    @pl.loop(1, reach + 1)
    def _(k):
        peer = lax.rem(me + devices - k, devices)
        pl.semaphore_signal(barrier, 1, device_id=coords(peer, sizes), device_id_type=MESH)

    for j in range(1, line):
        pl.semaphore_signal(barrier, 1, device_id=line_peer(j), device_id_type=MESH)
    for j in range(1, plane):
        pl.semaphore_signal(barrier, 1, device_id=plane_peer(j), device_id_type=MESH)

    loads[0].wait()
    ids = ids_ref[...]
    last = jnp.broadcast_to(ids[tiles - 1 :, TILE - 1 :], (1, TILE))
    in_last = jnp.where(ids == jnp.broadcast_to(last, ids.shape), 1.0, 0.0)
    count = jnp.sum(jnp.sum(in_last, axis=0, keepdims=True), axis=1, keepdims=True)
    first = jnp.broadcast_to(rows_dev - count.astype(jnp.int32), (8, width))
    step = 64
    sub = lax.broadcasted_iota(jnp.int32, (step, width), 0)
    loads[2].wait()

    @pl.loop(0, rows_dev // step, init_carry=jnp.zeros((step, width), jnp.float32), unroll=4)
    def open_rows(t, acc):
        at = pl.ds(pl.multiple_of(t * step, step), step)
        inside = sub + t * step >= jnp.broadcast_to(first[0:1], (step, width))
        return acc + jnp.where(inside, feat[at, :], 0.0)

    total = jnp.sum(open_rows, axis=0, keepdims=True)
    tail[0:1, :] = total[:, :TILE]
    tail[1:2, :] = total[:, TILE:]
    tail[2:3, :] = last.astype(jnp.float32)
    tail[3:4, :] = jnp.broadcast_to(count, (1, TILE))

    loads[1].wait()
    slots = ny * nz * nx * slot_cap
    owners = owners_ref[...]
    across = jnp.broadcast_to(owners, (blocks, blocks))
    down = jnp.broadcast_to(across.T[:, 0:1], (blocks, blocks))
    earlier = lax.broadcasted_iota(jnp.int32, (blocks, blocks), 1) < (
        lax.broadcasted_iota(jnp.int32, (blocks, blocks), 0)
    )
    rank = jnp.sum(jnp.where((across == down) & earlier, 1.0, 0.0), axis=1, keepdims=True)
    target = down[:, 0:1] * slot_cap + rank.astype(jnp.int32)
    hit = jnp.broadcast_to(target, (blocks, slots)) == (
        lax.broadcasted_iota(jnp.int32, (blocks, slots), 1)
    )
    used = jnp.sum(jnp.where(hit, 1.0, 0.0), axis=0, keepdims=True)
    o_from = lax.broadcasted_iota(jnp.int32, (slots, slots), 0)
    o_to = lax.broadcasted_iota(jnp.int32, (slots, slots), 1)

    def plane_of(o):
        return lax.rem(lax.div(o, nx), nz)

    def order_of(o):
        return plane_order(lax.div(o, nx * nz), lax.rem(o, nx), nx)

    ahead = (plane_of(o_from) == plane_of(o_to)) & (order_of(o_from) < order_of(o_to))
    before = jnp.dot(
        jnp.broadcast_to(used, (8, slots)).astype(jnp.bfloat16),
        jnp.where(ahead, 1.0, 0.0).astype(jnp.bfloat16),
        preferred_element_type=jnp.float32,
    )[0:1]
    spot = jnp.where(used > 0.0, before + 1.0, 0.0)
    mine[...] = spot.astype(jnp.int32)
    key = plane_of(o_to[0:1]).astype(jnp.float32) * plane + before
    block_key = jnp.sum(
        jnp.where(hit, jnp.broadcast_to(key, (blocks, slots)), 0.0), axis=1, keepdims=True
    )
    entry = lax.broadcasted_iota(jnp.int32, (blocks, slots), 1).astype(jnp.float32)
    order = lax.broadcasted_iota(jnp.int32, (blocks, slots), 0)
    pack_out[...] = jnp.sum(
        jnp.where(jnp.broadcast_to(block_key, (blocks, slots)) == entry, order, 0),
        axis=0, keepdims=True,
    )

    lane = lax.broadcasted_iota(jnp.int32, ids.shape, 1)
    after = pltpu.roll(ids, TILE - 1, 1)
    end = jnp.where((after != ids) | (lane == TILE - 1), lane, TILE)
    hop = 1
    while hop < TILE:
        nxt = jnp.where(lane + hop < TILE, pltpu.roll(end, TILE - hop, 1), TILE)
        end = jnp.minimum(end, nxt)
        hop *= 2
    ends[...] = end
    prior = jnp.concatenate([jnp.full((1, TILE), -1, jnp.int32), ids[:-1]], axis=0)
    prior = jnp.broadcast_to(prior[:, TILE - 1 :], ids.shape)
    goes_on = jnp.sum(jnp.where(ids == prior, 1.0, 0.0), axis=1, keepdims=True)
    joins[...] = jnp.broadcast_to(goes_on.astype(jnp.int32), ids.shape)

    pl.semaphore_wait(barrier, reach + line - 1 + plane - 1)

    @pl.loop(1, reach + 1)
    def _(k):
        peer = lax.rem(me + k, devices)
        pltpu.make_async_remote_copy(
            src_ref=tail, dst_ref=got.at[k - 1], send_sem=send_sem, recv_sem=recv_sem,
            device_id=coords(peer, sizes), device_id_type=MESH,
        ).start()

    for j in range(1, line):
        pltpu.make_async_remote_copy(
            src_ref=mine, dst_ref=got_line.at[j - 1], send_sem=line_send, recv_sem=line_recv,
            device_id=line_peer(j), device_id_type=MESH,
        ).start()

    row = lax.broadcasted_iota(jnp.int32, (TILE, TILE), 0)
    col = lax.broadcasted_iota(jnp.int32, (TILE, TILE), 1)
    causal = col <= row
    ones = jnp.ones((TILE, TILE), jnp.bfloat16)

    @pl.loop(
        0, tiles,
        init_carry=(jnp.zeros((1, width), jnp.float32), jnp.zeros((1, TILE), jnp.float32)),
        unroll=4,
    )
    def _(t, carry):
        open_sum, open_count = carry
        at = pl.ds(pl.multiple_of(t * TILE, TILE), TILE)
        alive = row <= jnp.broadcast_to(ends[pl.ds(t, 1), :], (TILE, TILE))
        mask = jnp.where(alive & causal, 1.0, 0.0).astype(jnp.bfloat16)
        rows = feat[at, :]
        high = rows.astype(jnp.bfloat16)
        rest = rows - high.astype(jnp.float32)
        mid = rest.astype(jnp.bfloat16)
        low = (rest - mid.astype(jnp.float32)).astype(jnp.bfloat16)
        inside = (
            jnp.dot(mask, high, preferred_element_type=jnp.float32)
            + jnp.dot(mask, mid, preferred_element_type=jnp.float32)
            + jnp.dot(mask, low, preferred_element_type=jnp.float32)
        )
        number = jnp.dot(mask, ones, preferred_element_type=jnp.float32)
        joined = row < jnp.broadcast_to(joins[pl.ds(t, 1), :], (TILE, TILE))
        both = jnp.concatenate([joined, joined], axis=1)
        inside = inside + jnp.where(both, jnp.broadcast_to(open_sum, (TILE, width)), 0.0)
        number = number + jnp.where(joined, jnp.broadcast_to(open_count, (TILE, TILE)), 0.0)
        sums[at, :] = inside
        cnt[at, :] = number
        return inside[TILE - 1 :, :], number[TILE - 1 :, :]

    pltpu.make_async_copy(got_line, got_line, line_recv).wait()
    spots = mine[...]
    unpack_out[0:1, :] = spots
    largest = spots
    for j in range(1, line):
        spots = got_line[j - 1]
        largest = jnp.maximum(largest, spots)
        if j % ng == 0:
            unpack_out[j // ng : j // ng + 1, :] = spots
    top[...] = largest

    pltpu.make_async_copy(got, got, recv_sem).wait()

    for j in range(1, plane):
        pltpu.make_async_remote_copy(
            src_ref=top, dst_ref=got_plane.at[j - 1], send_sem=plane_send,
            recv_sem=plane_recv, device_id=plane_peer(j), device_id_type=MESH,
        ).start()

    arrived = got[...]
    open_id = arrived[0, 2:3, :]
    age = lax.broadcasted_iota(jnp.int32, arrived.shape, 0) + 1
    same = jnp.broadcast_to(arrived[:, 2:3, :], arrived.shape) == jnp.broadcast_to(
        open_id[None], arrived.shape
    )
    merged = jnp.sum(jnp.where(same & (age <= me), arrived, 0.0), axis=0)
    open_sum = jnp.concatenate([merged[0:1, :], merged[1:2, :]], axis=1)
    open_count = merged[3:4, :]
    in_open = jnp.where(
        ids.astype(jnp.float32) == jnp.broadcast_to(open_id, ids.shape), 1.0, 0.0
    )
    reached = jnp.sum(jnp.sum(in_open, axis=0, keepdims=True), axis=1, keepdims=True)
    reached = jnp.broadcast_to(reached.astype(jnp.int32), (1, TILE))
    sub = lax.broadcasted_iota(jnp.int32, (block_rows, TILE), 0)

    @pl.loop(0, blocks, unroll=4)
    def _(b):
        at = pl.ds(pl.multiple_of(b * block_rows, block_rows), block_rows)
        joined = sub + b * block_rows < jnp.broadcast_to(reached, (block_rows, TILE))
        number = cnt[at, :] + jnp.where(
            joined, jnp.broadcast_to(open_count, (block_rows, TILE)), 0.0
        )
        scale = 1.0 / jnp.sqrt(number)
        both = jnp.concatenate([joined, joined], axis=1)
        rows = sums[at, :] + jnp.where(
            both, jnp.broadcast_to(open_sum, (block_rows, width)), 0.0
        )
        norm[b] = (rows * jnp.concatenate([scale, scale], axis=1)).astype(jnp.bfloat16)

    pltpu.make_async_copy(got_plane, got_plane, plane_recv).wait()
    for j in range(1, plane):
        largest = jnp.maximum(largest, got_plane[j - 1])
    most = jnp.max(largest.astype(jnp.float32), axis=1, keepdims=True).astype(jnp.int32)
    most_out[...] = jnp.broadcast_to(most, most_out.shape)
    pltpu.make_async_copy(got, got, send_sem).wait()
    pltpu.make_async_copy(got_line, got_line, line_send).wait()
    pltpu.make_async_copy(got_plane, got_plane, plane_send).wait()


def relay_plan(sizes, room):
    far = sizes[1] // 2
    mid = (room + 1) // 2
    cuts = ((0, sizes[2], mid), (mid, (mid + room + 1) // 2, room))
    plan = {}
    for way in (0, 1):
        for d in range(1, far):
            for hop in range(1, d + 1):
                plan[way, d, hop, 0] = (0, room)
        for hop in range(1, far + 1):
            for piece in (0, 1):
                plan[way, far, hop, piece] = cuts[way][piece : piece + 2]
    return plan


def exchange_kernel(
    sizes, room,
    pack, unpack, norm, out,
    send, stage, z_send, z_recv, p_send, p_recv, *recv,
):
    ny, nz, nx, ng = sizes
    plane = ny * nx
    y, z, x, g = place()
    far = nz // 2
    plan = relay_plan(sizes, room)
    number = {key: n for n, key in enumerate(plan)}
    barrier = pltpu.get_barrier_semaphore()

    def z_peer(d):
        return (y, lax.rem(z + d, nz), x, g)

    for d in (1, nz - 1):
        pl.semaphore_signal(barrier, 1, device_id=z_peer(d), device_id_type=MESH)
    for j in range(1, plane):
        pl.semaphore_signal(
            barrier, 1, device_id_type=MESH,
            device_id=(lax.rem(y + j // nx, ny), z, lax.rem(x + j % nx, nx), g),
        )

    for d in range(1, nz):
        first = lax.rem(z + d, nz) * plane

        @pl.loop(0, room)
        def _(k):
            send[d - 1, k] = norm[pack[0, first + k]]

    pl.semaphore_wait(barrier, 2 + plane - 1)

    def relay(way, d, hop, piece):
        key = (way, d, hop, piece)
        a, b = plan[key]
        if hop == 1:
            src = send.at[(nz - d if way else d) - 1, pl.ds(a, b - a)]
        else:
            src = recv[number[way, d, hop - 1, piece]]
        n = number[key]
        return pltpu.make_async_remote_copy(
            src_ref=src, dst_ref=recv[n], send_sem=z_send.at[n], recv_sem=z_recv.at[n],
            device_id=z_peer(nz - 1 if way else 1), device_id_type=MESH,
        )

    def go(d, hop, piece=0):
        for way in (0, 1):
            relay(way, d, hop, piece).start()

    def arrived(d, hop, piece=0):
        for way in (0, 1):
            relay(way, d, hop, piece).wait_recv()

    def wanted(d, ty, tx, pieces):
        spot = unpack[d, (ty * nz + z) * nx + tx]
        block = None
        for ref, a, b in pieces:
            one = ref[jnp.clip(spot - 1 - a, 0, b - a - 1)]
            block = one if block is None else jnp.where(spot > a, one, block)
        return jnp.where(spot > 0, block, jnp.zeros_like(block))

    def own(ty, tx):
        spot = unpack[0, (ty * nz + z) * nx + tx]
        block = norm[pack[0, z * plane + jnp.maximum(spot, 1) - 1]]
        return jnp.where(spot > 0, block, jnp.zeros_like(block))

    def slot_from(d):
        return (y * nz + lax.rem(z + nz - d, nz)) * nx + x

    def p_copy(d, j, ty, tx):
        return pltpu.make_async_remote_copy(
            src_ref=stage.at[d, j], dst_ref=out.at[slot_from(d)],
            send_sem=p_send, recv_sem=p_recv,
            device_id=(ty, z, tx, g), device_id_type=MESH,
        )

    def deliver(d, block_for):
        def target(j):
            return lax.rem(y + lax.div(j, nx), ny), lax.rem(x + lax.rem(j, nx), nx)

        @pl.loop(1, plane)
        def _(j):
            stage[d, j] = block_for(*target(j))

        @pl.loop(1, plane)
        def _(j):
            p_copy(d, j, *target(j)).start()

        out[slot_from(d)] = block_for(y, x)

    def deliver_from(d):
        for way in (0, 1):
            key = (way, d, d, 0)
            pieces = [(recv[number[key]], *plan[key])]
            deliver(nz - d if way else d, lambda ty, tx: wanted(
                nz - d if way else d, ty, tx, pieces
            ))

    def deliver_far(group, pieces):
        def target(j):
            ty = lax.rem(y + j, ny)
            return ty, lax.rem(group + ny - ty, nx)

        @pl.loop(0, nx)
        def _(j):
            stage[far, group * nx + j] = wanted(far, *target(j), pieces)

        @pl.loop(0, nx)
        def _(j):
            ty, tx = target(j)

            @pl.when((ty - y) * nx + tx - x != 0)
            def _():
                p_copy(far, group * nx + j, ty, tx).start()

    for d in range(1, far):
        go(d, 1)
    deliver(0, own)
    arrived(1, 1)
    deliver_from(1)
    arrived(2, 1)
    go(2, 2)
    arrived(3, 1)
    go(3, 2)
    go(4, 1, 0)
    go(4, 1, 1)
    arrived(2, 2)
    deliver_from(2)
    arrived(3, 2)
    go(3, 3)
    for piece in (0, 1):
        arrived(4, 1, piece)
        go(4, 2, piece)
    arrived(3, 3)
    deliver_from(3)
    for hop in (2, 3):
        for piece in (0, 1):
            arrived(4, hop, piece)
            go(4, hop + 1, piece)
    pieces = [
        (recv[number[way, far, far, piece]], *plan[way, far, far, piece])
        for way in (0, 1)
        for piece in (0, 1)
    ]
    arrived(4, 4, 0)
    deliver_far(0, pieces[:1])
    arrived(4, 4, 1)
    for group in range(1, ny):
        deliver_far(group, pieces)
    out[slot_from(far)] = wanted(far, y, x, pieces)

    for key in plan:
        relay(*key).wait_send()
    landed = out.at[pl.ds(0, nz * (plane - 1))]
    pltpu.make_async_copy(landed, landed, p_send).wait()
    pltpu.make_async_copy(landed, landed, p_recv).wait()


def to_hbm_kernel(src, out, sem):
    parts = sem.shape[0]
    size = src.shape[0] // parts
    copies = [
        pltpu.make_async_copy(
            src.at[pl.ds(n * size, size)], out.at[pl.ds(n * size, size)], sem.at[n]
        )
        for n in range(parts)
    ]
    for copy in copies:
        copy.start()
    for copy in copies:
        copy.wait()


def to_hbm(array):
    return pl.pallas_call(
        to_hbm_kernel,
        out_shape=pltpu.HBM(array.shape, array.dtype),
        in_specs=[pl.BlockSpec(memory_space=pltpu.VMEM)],
        out_specs=pl.BlockSpec(memory_space=pltpu.HBM),
        scratch_shapes=[pltpu.SemaphoreType.DMA((4,))],
        compiler_params=pltpu.CompilerParams(vmem_limit_bytes=1 << 20),
        name="to_hbm",
    )(array)


def body(features, session, owner_map):
    rows_dev, width = features.shape
    blocks = owner_map.shape[1]
    block_rows = rows_dev // blocks
    sizes = tuple(lax.axis_size(name) for name in ROW_GRP)
    ny, nz, nx, ng = sizes
    plane = ny * nx
    slot_cap = max(1, 2 * blocks // (plane * nz))
    slots = plane * nz * slot_cap
    tiles = rows_dev // TILE
    reach = (MOST - 2) // rows_dev + 1
    norm, unpack, pack, most = pl.pallas_call(
        lambda *refs: prelude_kernel(sizes, reach, block_rows, slot_cap, *refs),
        out_shape=(
            jax.ShapeDtypeStruct((blocks, block_rows, width), jnp.bfloat16),
            jax.ShapeDtypeStruct((nz, slots), jnp.int32),
            jax.ShapeDtypeStruct((1, slots), jnp.int32),
            jax.ShapeDtypeStruct((1, TILE), jnp.int32),
        ),
        in_specs=[pl.BlockSpec(memory_space=pltpu.HBM)] * 3,
        out_specs=[pl.BlockSpec(memory_space=pltpu.VMEM)] * 4,
        scratch_shapes=[
            pltpu.VMEM(owner_map.shape, jnp.int32),
            pltpu.VMEM((tiles, TILE), jnp.int32),
            pltpu.VMEM((rows_dev, width), jnp.float32),
            pltpu.VMEM((rows_dev, width), jnp.float32),
            pltpu.VMEM((rows_dev, TILE), jnp.float32),
            pltpu.VMEM((tiles, TILE), jnp.int32),
            pltpu.VMEM((tiles, TILE), jnp.int32),
            pltpu.VMEM((4, TILE), jnp.float32),
            pltpu.VMEM((reach, 4, TILE), jnp.float32),
            pltpu.VMEM((1, slots), jnp.int32),
            pltpu.VMEM((nz * ng - 1, 1, slots), jnp.int32),
            pltpu.VMEM((1, slots), jnp.int32),
            pltpu.VMEM((plane - 1, 1, slots), jnp.int32),
            pltpu.SemaphoreType.DMA((3,)),
        ]
        + [pltpu.SemaphoreType.DMA] * 6,
        compiler_params=pltpu.CompilerParams(
            collective_id=0, has_side_effects=True, vmem_limit_bytes=24 << 20
        ),
        name="prelude",
    )(
        *(
            pltpu.with_memory_space_constraint(arg, pltpu.HBM)
            for arg in (owner_map, session.reshape(tiles, TILE), features)
        )
    )

    def exchange(room, number):
        block = (block_rows, width)
        return lambda pack, unpack, norm: to_hbm(pl.pallas_call(
            lambda *refs: exchange_kernel(sizes, room, *refs),
            out_shape=pltpu.VMEM((slots, *block), jnp.bfloat16),
            in_specs=[
                pl.BlockSpec(memory_space=pltpu.SMEM),
                pl.BlockSpec(memory_space=pltpu.SMEM),
                pl.BlockSpec(memory_space=pltpu.VMEM),
            ],
            out_specs=pl.BlockSpec(memory_space=pltpu.VMEM),
            scratch_shapes=[
                pltpu.VMEM((nz - 1, room, *block), jnp.bfloat16),
                pltpu.VMEM((nz, plane, *block), jnp.bfloat16),
                pltpu.SemaphoreType.DMA((len(relay_plan(sizes, room)),)),
                pltpu.SemaphoreType.DMA((len(relay_plan(sizes, room)),)),
                pltpu.SemaphoreType.DMA,
                pltpu.SemaphoreType.DMA,
            ]
            + [
                pltpu.VMEM((b - a, *block), jnp.bfloat16)
                for a, b in relay_plan(sizes, room).values()
            ],
            compiler_params=pltpu.CompilerParams(
                collective_id=number, has_side_effects=True, vmem_limit_bytes=24 << 20
            ),
            name=f"exchange_{room}",
        )(pack, unpack, norm))

    rooms = ROOMS
    choice = sum((most[0, 0] > room).astype(jnp.int32) for room in rooms[:-1])
    return lax.switch(
        choice, [exchange(room, 1 + n) for n, room in enumerate(rooms)], pack, unpack, norm
    )


def solution(mesh):
    split = Mesh(
        mesh.devices.reshape(4, 8, 4, mesh.shape["grp"]), ("row_0", "row_1", "row_2", "grp")
    )
    return jax.shard_map(
        body,
        mesh=split,
        in_specs=(P(ROW_GRP, None), P(ROW_GRP), P(ROW_GRP, None)),
        out_specs=P(ROW_GRP, None, None),
        check_vma=False,
    )
```

```python
import jax
import jax.numpy as jnp
from jax import lax
from jax.experimental import pallas as pl
from jax.experimental.pallas import tpu as pltpu
from jax.sharding import Mesh
from jax.sharding import PartitionSpec as P

ROW = ("row_0", "row_1", "row_2")
ROW_GRP = ("row_0", "row_1", "row_2", "grp")
MOST = 163840
TILE = 128
ROOMS = (12, 13, 14, 15, 16)
MESH = pl.DeviceIdType.MESH


def coords(d, sizes):
    out = []
    for n in reversed(sizes):
        out.append(lax.rem(d, n))
        d = lax.div(d, n)
    return tuple(reversed(out))


def place():
    return tuple(lax.axis_index(name) for name in ROW_GRP)


def plane_order(y, x, nx):
    return lax.rem(x + y, nx) * nx + y


def prelude_kernel(
    sizes, reach, block_rows, slot_cap,
    owners_hbm, ids_hbm, feat_hbm,
    sums, cnt, open_out, unpack_out, pack_out, most_out,
    owners_ref, ids_ref, feat, ends, joins, tail, got, mine, got_line, top, got_plane,
    load_sem, send_sem, recv_sem, line_send, line_recv, plane_send, plane_recv,
):
    ny, nz, nx, ng = sizes
    devices = ny * nz * nx * ng
    me = lax.axis_index(ROW_GRP)
    y, z, x, g = place()
    rows_dev, width = feat.shape
    tiles = rows_dev // TILE
    blocks = rows_dev // block_rows
    line = nz * ng
    plane = ny * nx
    loads = [
        pltpu.make_async_copy(src, dst, load_sem.at[n])
        for n, (src, dst) in enumerate(
            ((ids_hbm, ids_ref), (owners_hbm, owners_ref), (feat_hbm, feat))
        )
    ]
    for load in loads:
        load.start()

    def line_peer(j):
        return (y, lax.rem(z + j // ng, nz), x, lax.rem(g + j % ng, ng))

    def plane_peer(j):
        return (lax.rem(y + j // nx, ny), z, lax.rem(x + j % nx, nx), g)

    barrier = pltpu.get_barrier_semaphore()

    @pl.loop(0, reach)
    def _(n):
        peer = lax.rem(me + devices - reach + n, devices)
        pl.semaphore_signal(barrier, 1, device_id=coords(peer, sizes), device_id_type=MESH)

    for j in range(1, line):
        pl.semaphore_signal(barrier, 1, device_id=line_peer(j), device_id_type=MESH)
    for j in range(1, plane):
        pl.semaphore_signal(barrier, 1, device_id=plane_peer(j), device_id_type=MESH)

    loads[0].wait()
    ids = ids_ref[...]
    last = jnp.broadcast_to(ids[tiles - 1 :, TILE - 1 :], (1, TILE))
    in_last = jnp.where(ids == jnp.broadcast_to(last, ids.shape), 1.0, 0.0)
    count = jnp.sum(jnp.sum(in_last, axis=0, keepdims=True), axis=1, keepdims=True)
    first = jnp.broadcast_to(rows_dev - count.astype(jnp.int32), (8, width))
    step = 64
    sub = lax.broadcasted_iota(jnp.int32, (step, width), 0)
    loads[2].wait()

    @pl.loop(0, rows_dev // step, init_carry=jnp.zeros((step, width), jnp.float32), unroll=4)
    def open_rows(t, acc):
        at = pl.ds(pl.multiple_of(t * step, step), step)
        inside = sub + t * step >= jnp.broadcast_to(first[0:1], (step, width))
        return acc + jnp.where(inside, feat[at, :], 0.0)

    total = jnp.sum(open_rows, axis=0, keepdims=True)
    tail[0:1, :] = total[:, :TILE]
    tail[1:2, :] = total[:, TILE:]
    tail[2:3, :] = last.astype(jnp.float32)
    tail[3:4, :] = jnp.broadcast_to(count, (1, TILE))

    loads[1].wait()
    slots = ny * nz * nx * slot_cap
    owners = owners_ref[...]
    across = jnp.broadcast_to(owners, (blocks, blocks))
    down = jnp.broadcast_to(across.T[:, 0:1], (blocks, blocks))
    earlier = lax.broadcasted_iota(jnp.int32, (blocks, blocks), 1) < (
        lax.broadcasted_iota(jnp.int32, (blocks, blocks), 0)
    )
    rank = jnp.sum(jnp.where((across == down) & earlier, 1.0, 0.0), axis=1, keepdims=True)
    target = down[:, 0:1] * slot_cap + rank.astype(jnp.int32)
    hit = jnp.broadcast_to(target, (blocks, slots)) == (
        lax.broadcasted_iota(jnp.int32, (blocks, slots), 1)
    )
    used = jnp.sum(jnp.where(hit, 1.0, 0.0), axis=0, keepdims=True)
    o_from = lax.broadcasted_iota(jnp.int32, (slots, slots), 0)
    o_to = lax.broadcasted_iota(jnp.int32, (slots, slots), 1)

    def plane_of(o):
        return lax.rem(lax.div(o, nx), nz)

    def order_of(o):
        return plane_order(lax.div(o, nx * nz), lax.rem(o, nx), nx)

    ahead = (plane_of(o_from) == plane_of(o_to)) & (order_of(o_from) < order_of(o_to))
    before = jnp.dot(
        jnp.broadcast_to(used, (8, slots)).astype(jnp.bfloat16),
        jnp.where(ahead, 1.0, 0.0).astype(jnp.bfloat16),
        preferred_element_type=jnp.float32,
    )[0:1]
    spot = jnp.where(used > 0.0, before + 1.0, 0.0)
    mine[...] = spot.astype(jnp.int32)
    key = plane_of(o_to[0:1]).astype(jnp.float32) * plane + before
    block_key = jnp.sum(
        jnp.where(hit, jnp.broadcast_to(key, (blocks, slots)), 0.0), axis=1, keepdims=True
    )
    entry = lax.broadcasted_iota(jnp.int32, (blocks, slots), 1).astype(jnp.float32)
    order = lax.broadcasted_iota(jnp.int32, (blocks, slots), 0)
    pack_out[...] = jnp.sum(
        jnp.where(jnp.broadcast_to(block_key, (blocks, slots)) == entry, order, 0),
        axis=0, keepdims=True,
    )

    lane = lax.broadcasted_iota(jnp.int32, ids.shape, 1)
    after = pltpu.roll(ids, TILE - 1, 1)
    end = jnp.where((after != ids) | (lane == TILE - 1), lane, TILE)
    hop = 1
    while hop < TILE:
        nxt = jnp.where(lane + hop < TILE, pltpu.roll(end, TILE - hop, 1), TILE)
        end = jnp.minimum(end, nxt)
        hop *= 2
    ends[...] = end
    prior = jnp.concatenate([jnp.full((1, TILE), -1, jnp.int32), ids[:-1]], axis=0)
    prior = jnp.broadcast_to(prior[:, TILE - 1 :], ids.shape)
    goes_on = jnp.sum(jnp.where(ids == prior, 1.0, 0.0), axis=1, keepdims=True)
    joins[...] = jnp.broadcast_to(goes_on.astype(jnp.int32), ids.shape)

    pl.semaphore_wait(barrier, reach + line - 1 + plane - 1)

    for j in range(1, line):
        pltpu.make_async_remote_copy(
            src_ref=mine, dst_ref=got_line.at[j - 1], send_sem=line_send, recv_sem=line_recv,
            device_id=line_peer(j), device_id_type=MESH,
        ).start()

    @pl.loop(0, reach)
    def _(n):
        k = reach - n
        peer = lax.rem(me + k, devices)
        pltpu.make_async_remote_copy(
            src_ref=tail, dst_ref=got.at[k - 1], send_sem=send_sem, recv_sem=recv_sem,
            device_id=coords(peer, sizes), device_id_type=MESH,
        ).start()

    row = lax.broadcasted_iota(jnp.int32, (TILE, TILE), 0)
    col = lax.broadcasted_iota(jnp.int32, (TILE, TILE), 1)
    causal = col <= row
    ones = jnp.ones((TILE, TILE), jnp.bfloat16)

    @pl.loop(
        0, tiles,
        init_carry=(jnp.zeros((1, width), jnp.float32), jnp.zeros((1, TILE), jnp.float32)),
        unroll=4,
    )
    def _(t, carry):
        open_sum, open_count = carry
        at = pl.ds(pl.multiple_of(t * TILE, TILE), TILE)
        alive = row <= jnp.broadcast_to(ends[pl.ds(t, 1), :], (TILE, TILE))
        mask = jnp.where(alive & causal, 1.0, 0.0).astype(jnp.bfloat16)
        rows = feat[at, :]
        high = rows.astype(jnp.bfloat16)
        rest = rows - high.astype(jnp.float32)
        mid = rest.astype(jnp.bfloat16)
        low = (rest - mid.astype(jnp.float32)).astype(jnp.bfloat16)
        inside = (
            jnp.dot(mask, high, preferred_element_type=jnp.float32)
            + jnp.dot(mask, mid, preferred_element_type=jnp.float32)
            + jnp.dot(mask, low, preferred_element_type=jnp.float32)
        )
        number = jnp.dot(mask, ones, preferred_element_type=jnp.float32)
        joined = row < jnp.broadcast_to(joins[pl.ds(t, 1), :], (TILE, TILE))
        both = jnp.concatenate([joined, joined], axis=1)
        inside = inside + jnp.where(both, jnp.broadcast_to(open_sum, (TILE, width)), 0.0)
        number = number + jnp.where(joined, jnp.broadcast_to(open_count, (TILE, TILE)), 0.0)
        sums[at, :] = inside
        cnt[at, :] = number
        return inside[TILE - 1 :, :], number[TILE - 1 :, :]

    pltpu.make_async_copy(got_line, got_line, line_recv).wait()
    spots = mine[...]
    unpack_out[0:1, :] = spots
    largest = spots
    for j in range(1, line):
        spots = got_line[j - 1]
        largest = jnp.maximum(largest, spots)
        if j % ng == 0:
            unpack_out[j // ng : j // ng + 1, :] = spots
    top[...] = largest

    for j in range(1, plane):
        pltpu.make_async_remote_copy(
            src_ref=top, dst_ref=got_plane.at[j - 1], send_sem=plane_send,
            recv_sem=plane_recv, device_id=plane_peer(j), device_id_type=MESH,
        ).start()

    pltpu.make_async_copy(got, got, recv_sem).wait()
    arrived = got[...]
    open_id = arrived[0, 2:3, :]
    age = lax.broadcasted_iota(jnp.int32, arrived.shape, 0) + 1
    same = jnp.broadcast_to(arrived[:, 2:3, :], arrived.shape) == jnp.broadcast_to(
        open_id[None], arrived.shape
    )
    merged = jnp.sum(jnp.where(same & (age <= me), arrived, 0.0), axis=0)
    open_out[0:4, :] = merged
    in_open = jnp.where(
        ids.astype(jnp.float32) == jnp.broadcast_to(open_id, ids.shape), 1.0, 0.0
    )
    reached = jnp.sum(jnp.sum(in_open, axis=0, keepdims=True), axis=1, keepdims=True)
    open_out[4:8, :] = jnp.broadcast_to(reached, (4, TILE))

    pltpu.make_async_copy(got_plane, got_plane, plane_recv).wait()
    for j in range(1, plane):
        largest = jnp.maximum(largest, got_plane[j - 1])
    most = jnp.max(largest.astype(jnp.float32), axis=1, keepdims=True).astype(jnp.int32)
    most_out[...] = jnp.broadcast_to(most, most_out.shape)
    pltpu.make_async_copy(got, got, send_sem).wait()
    pltpu.make_async_copy(got_line, got_line, line_send).wait()
    pltpu.make_async_copy(got_plane, got_plane, plane_send).wait()


def relay_plan(sizes, room):
    far = sizes[1] // 2
    nx = sizes[2]
    early = nx + (room // 2 + 1) // 2
    late = early + (room + 1) // 2 - nx
    cuts = (((0, nx), (early, late)), ((nx, early), (late, room)))
    plan = {}
    for way in (0, 1):
        for d in range(1, far):
            for hop in range(1, d + 1):
                plan[way, d, hop, 0] = (0, room)
        for hop in range(1, far + 1):
            for piece in (0, 1):
                plan[way, far, hop, piece] = cuts[way][piece]
    return plan


def exchange_kernel(
    sizes, room,
    pack_ref, unpack_ref, sums, cnt, open_ref, out,
    pack, unpack, norm, send, stage, table_sem, z_send, z_recv, p_send, p_recv, *recv,
):
    ny, nz, nx, ng = sizes
    plane = ny * nx
    y, z, x, g = place()
    far = nz // 2
    plan = relay_plan(sizes, room)
    number = {key: n for n, key in enumerate(plan)}
    barrier = pltpu.get_barrier_semaphore()

    def z_peer(d):
        return (y, lax.rem(z + d, nz), x, g)

    tables = [
        pltpu.make_async_copy(pack_ref, pack, table_sem.at[0]),
        pltpu.make_async_copy(unpack_ref, unpack, table_sem.at[1]),
    ]
    for table in tables:
        table.start()
    for d in (1, nz - 1):
        pl.semaphore_signal(barrier, 1, device_id=z_peer(d), device_id_type=MESH)
    for j in range(1, plane):
        pl.semaphore_signal(
            barrier, 1, device_id_type=MESH,
            device_id=(lax.rem(y + j // nx, ny), z, lax.rem(x + j % nx, nx), g),
        )

    blocks, block_rows, width = norm.shape
    open_sum = jnp.concatenate([open_ref[0:1, :], open_ref[1:2, :]], axis=1)
    open_count = open_ref[3:4, :]
    reached = open_ref[4:5, :].astype(jnp.int32)
    sub = lax.broadcasted_iota(jnp.int32, (block_rows, TILE), 0)

    @pl.loop(0, blocks, unroll=4)
    def _(b):
        at = pl.ds(pl.multiple_of(b * block_rows, block_rows), block_rows)
        joined = sub + b * block_rows < jnp.broadcast_to(reached, (block_rows, TILE))
        count = cnt[at, :] + jnp.where(
            joined, jnp.broadcast_to(open_count, (block_rows, TILE)), 0.0
        )
        scale = 1.0 / jnp.sqrt(count)
        both = jnp.concatenate([joined, joined], axis=1)
        rows = sums[at, :] + jnp.where(
            both, jnp.broadcast_to(open_sum, (block_rows, width)), 0.0
        )
        norm[b] = (rows * jnp.concatenate([scale, scale], axis=1)).astype(jnp.bfloat16)

    for table in tables:
        table.wait()
    for d in range(1, nz):
        first = lax.rem(z + d, nz) * plane

        @pl.loop(0, room)
        def _(k):
            send[d - 1, k] = norm[pack[0, first + k]]

    pl.semaphore_wait(barrier, 2 + plane - 1)

    def relay(way, d, hop, piece):
        key = (way, d, hop, piece)
        a, b = plan[key]
        if hop == 1:
            src = send.at[(nz - d if way else d) - 1, pl.ds(a, b - a)]
        else:
            src = recv[number[way, d, hop - 1, piece]]
        n = number[key]
        return pltpu.make_async_remote_copy(
            src_ref=src, dst_ref=recv[n], send_sem=z_send.at[n], recv_sem=z_recv.at[n],
            device_id=z_peer(nz - 1 if way else 1), device_id_type=MESH,
        )

    def go(d, hop, piece=0):
        for way in (0, 1):
            relay(way, d, hop, piece).start()

    def arrived(d, hop, piece=0):
        for way in (0, 1):
            relay(way, d, hop, piece).wait_recv()

    def wanted(d, ty, tx, pieces):
        spot = unpack[d, (ty * nz + z) * nx + tx]
        block = None
        for ref, a, b in pieces:
            one = ref[jnp.clip(spot - 1 - a, 0, b - a - 1)]
            block = one if block is None else jnp.where(spot > a, one, block)
        return jnp.where(spot > 0, block, jnp.zeros_like(block))

    def own(ty, tx):
        spot = unpack[0, (ty * nz + z) * nx + tx]
        block = norm[pack[0, z * plane + jnp.maximum(spot, 1) - 1]]
        return jnp.where(spot > 0, block, jnp.zeros_like(block))

    def slot_from(d):
        return (y * nz + lax.rem(z + nz - d, nz)) * nx + x

    def p_copy(d, j, ty, tx):
        return pltpu.make_async_remote_copy(
            src_ref=stage.at[d, j], dst_ref=out.at[slot_from(d)],
            send_sem=p_send, recv_sem=p_recv,
            device_id=(ty, z, tx, g), device_id_type=MESH,
        )

    def deliver(d, block_for):
        def target(j):
            return lax.rem(y + lax.div(j, nx), ny), lax.rem(x + lax.rem(j, nx), nx)

        @pl.loop(1, plane)
        def _(j):
            stage[d, j] = block_for(*target(j))

        @pl.loop(1, plane)
        def _(j):
            p_copy(d, j, *target(j)).start()

        out[slot_from(d)] = block_for(y, x)

    def deliver_from(d):
        for way in (0, 1):
            key = (way, d, d, 0)
            pieces = [(recv[number[key]], *plan[key])]
            deliver(nz - d if way else d, lambda ty, tx: wanted(
                nz - d if way else d, ty, tx, pieces
            ))

    def deliver_far(group, low, high, pieces):
        def target(j):
            ty = lax.rem(y + j, ny) if high - low == ny else low + j
            return ty, lax.rem(group + ny - ty, nx)

        @pl.loop(0, high - low)
        def _(j):
            stage[far, group * nx + low + j] = wanted(far, *target(j), pieces)

        @pl.loop(0, high - low)
        def _(j):
            ty, tx = target(j)

            @pl.when((ty - y) * nx + tx - x != 0)
            def _():
                p_copy(far, group * nx + low + j, ty, tx).start()

    for d in range(1, far):
        go(d, 1)
    deliver(0, own)
    arrived(1, 1)
    deliver_from(1)
    arrived(2, 1)
    go(2, 2)
    arrived(3, 1)
    go(3, 2)
    go(4, 1, 0)
    go(4, 1, 1)
    arrived(2, 2)
    deliver_from(2)
    arrived(3, 2)
    go(3, 3)
    for piece in (0, 1):
        arrived(4, 1, piece)
        go(4, 2, piece)
    arrived(3, 3)
    deliver_from(3)
    for hop in (2, 3):
        for piece in (0, 1):
            arrived(4, hop, piece)
            go(4, hop + 1, piece)
    pieces = [
        (recv[number[way, far, far, piece]], *plan[way, far, far, piece])
        for piece in (0, 1)
        for way in (0, 1)
    ]
    early = pieces[1][2] - ny
    arrived(4, 4, 0)
    deliver_far(0, 0, ny, pieces[:2])
    deliver_far(1, 0, early, pieces[:2])
    arrived(4, 4, 1)
    if early < ny:
        deliver_far(1, early, ny, pieces)
    for group in range(2, ny):
        deliver_far(group, 0, ny, pieces)
    out[slot_from(far)] = wanted(far, y, x, pieces)

    for key in plan:
        relay(*key).wait_send()
    landed = out.at[pl.ds(0, nz * (plane - 1))]
    pltpu.make_async_copy(landed, landed, p_send).wait()
    pltpu.make_async_copy(landed, landed, p_recv).wait()


def to_hbm_kernel(src, out, sem):
    parts = sem.shape[0]
    size = src.shape[0] // parts
    copies = [
        pltpu.make_async_copy(
            src.at[pl.ds(n * size, size)], out.at[pl.ds(n * size, size)], sem.at[n]
        )
        for n in range(parts)
    ]
    for copy in copies:
        copy.start()
    for copy in copies:
        copy.wait()


def to_hbm(array):
    return pl.pallas_call(
        to_hbm_kernel,
        out_shape=pltpu.HBM(array.shape, array.dtype),
        in_specs=[pl.BlockSpec(memory_space=pltpu.VMEM)],
        out_specs=pl.BlockSpec(memory_space=pltpu.HBM),
        scratch_shapes=[pltpu.SemaphoreType.DMA((4,))],
        compiler_params=pltpu.CompilerParams(vmem_limit_bytes=1 << 20),
        name="to_hbm",
    )(array)


def body(features, session, owner_map):
    rows_dev, width = features.shape
    blocks = owner_map.shape[1]
    block_rows = rows_dev // blocks
    sizes = tuple(lax.axis_size(name) for name in ROW_GRP)
    ny, nz, nx, ng = sizes
    plane = ny * nx
    slot_cap = max(1, 2 * blocks // (plane * nz))
    slots = plane * nz * slot_cap
    tiles = rows_dev // TILE
    reach = (MOST - 2) // rows_dev + 1
    sums, cnt, open_rows, unpack, pack, most = pl.pallas_call(
        lambda *refs: prelude_kernel(sizes, reach, block_rows, slot_cap, *refs),
        out_shape=(
            jax.ShapeDtypeStruct((rows_dev, width), jnp.float32),
            jax.ShapeDtypeStruct((rows_dev, TILE), jnp.float32),
            jax.ShapeDtypeStruct((8, TILE), jnp.float32),
            jax.ShapeDtypeStruct((nz, slots), jnp.int32),
            jax.ShapeDtypeStruct((1, slots), jnp.int32),
            jax.ShapeDtypeStruct((1, TILE), jnp.int32),
        ),
        in_specs=[pl.BlockSpec(memory_space=pltpu.HBM)] * 3,
        out_specs=[pl.BlockSpec(memory_space=pltpu.VMEM)] * 6,
        scratch_shapes=[
            pltpu.VMEM(owner_map.shape, jnp.int32),
            pltpu.VMEM((tiles, TILE), jnp.int32),
            pltpu.VMEM((rows_dev, width), jnp.float32),
            pltpu.VMEM((tiles, TILE), jnp.int32),
            pltpu.VMEM((tiles, TILE), jnp.int32),
            pltpu.VMEM((4, TILE), jnp.float32),
            pltpu.VMEM((reach, 4, TILE), jnp.float32),
            pltpu.VMEM((1, slots), jnp.int32),
            pltpu.VMEM((nz * ng - 1, 1, slots), jnp.int32),
            pltpu.VMEM((1, slots), jnp.int32),
            pltpu.VMEM((plane - 1, 1, slots), jnp.int32),
            pltpu.SemaphoreType.DMA((3,)),
        ]
        + [pltpu.SemaphoreType.DMA] * 6,
        compiler_params=pltpu.CompilerParams(
            collective_id=0, has_side_effects=True, vmem_limit_bytes=24 << 20
        ),
        name="prelude",
    )(
        *(
            pltpu.with_memory_space_constraint(arg, pltpu.HBM)
            for arg in (owner_map, session.reshape(tiles, TILE), features)
        )
    )

    def exchange(room, number):
        block = (block_rows, width)
        return lambda pack, unpack, *rows: to_hbm(pl.pallas_call(
            lambda *refs: exchange_kernel(sizes, room, *refs),
            out_shape=pltpu.VMEM((slots, *block), jnp.bfloat16),
            in_specs=[pl.BlockSpec(memory_space=pltpu.VMEM)] * 5,
            out_specs=pl.BlockSpec(memory_space=pltpu.VMEM),
            scratch_shapes=[
                pltpu.SMEM((1, slots), jnp.int32),
                pltpu.SMEM((nz, slots), jnp.int32),
                pltpu.VMEM((blocks, *block), jnp.bfloat16),
                pltpu.VMEM((nz - 1, room, *block), jnp.bfloat16),
                pltpu.VMEM((nz, plane, *block), jnp.bfloat16),
                pltpu.SemaphoreType.DMA((2,)),
                pltpu.SemaphoreType.DMA((len(relay_plan(sizes, room)),)),
                pltpu.SemaphoreType.DMA((len(relay_plan(sizes, room)),)),
                pltpu.SemaphoreType.DMA,
                pltpu.SemaphoreType.DMA,
            ]
            + [
                pltpu.VMEM((b - a, *block), jnp.bfloat16)
                for a, b in relay_plan(sizes, room).values()
            ],
            compiler_params=pltpu.CompilerParams(
                collective_id=number, has_side_effects=True, vmem_limit_bytes=24 << 20
            ),
            name=f"exchange_{room}",
        )(pack, unpack, *rows))

    rooms = ROOMS
    choice = sum((most[0, 0] > room).astype(jnp.int32) for room in rooms[:-1])
    return lax.switch(
        choice, [exchange(room, 1 + n) for n, room in enumerate(rooms)],
        pack, unpack, sums, cnt, open_rows,
    )


def solution(mesh):
    split = Mesh(
        mesh.devices.reshape(4, 8, 4, mesh.shape["grp"]), ("row_0", "row_1", "row_2", "grp")
    )
    return jax.shard_map(
        body,
        mesh=split,
        in_specs=(P(ROW_GRP, None), P(ROW_GRP), P(ROW_GRP, None)),
        out_specs=P(ROW_GRP, None, None),
        check_vma=False,
    )
```

```python
import jax
import jax.numpy as jnp
from jax import lax
from jax.experimental import pallas as pl
from jax.experimental.pallas import tpu as pltpu
from jax.sharding import Mesh
from jax.sharding import PartitionSpec as P

ROW = ("row_0", "row_1", "row_2")
ROW_GRP = ("row_0", "row_1", "row_2", "grp")
MOST = 163840
TILE = 128
ROOMS = ((35, 26, 17, 6), (36, 27, 18, 7), (37, 28, 19, 7), (40, 30, 21, 8), (56, 40, 24, 8))
MESH = pl.DeviceIdType.MESH


def coords(d, sizes):
    out = []
    for n in reversed(sizes):
        out.append(lax.rem(d, n))
        d = lax.div(d, n)
    return tuple(reversed(out))


def place():
    return tuple(lax.axis_index(name) for name in ROW_GRP)


def plane_order(y, x, nx):
    return lax.rem(x + y, nx) * nx + y


def prelude_kernel(
    sizes, reach, block_rows, slot_cap,
    owners_hbm, ids_hbm, feat_hbm,
    sums, cnt, open_out, unpack_out, pack_out, most_out,
    owners_ref, ids_ref, feat, ends, joins, tail, got, mine, got_line, top, got_plane,
    load_sem, send_sem, recv_sem, line_send, line_recv, plane_send, plane_recv,
):
    ny, nz, nx, ng = sizes
    devices = ny * nz * nx * ng
    me = lax.axis_index(ROW_GRP)
    y, z, x, g = place()
    rows_dev, width = feat.shape
    tiles = rows_dev // TILE
    blocks = rows_dev // block_rows
    line = nz * ng
    plane = ny * nx
    loads = [
        pltpu.make_async_copy(src, dst, load_sem.at[n])
        for n, (src, dst) in enumerate(
            ((ids_hbm, ids_ref), (owners_hbm, owners_ref), (feat_hbm, feat))
        )
    ]
    for load in loads:
        load.start()

    def line_peer(j):
        return (y, lax.rem(z + j // ng, nz), x, lax.rem(g + j % ng, ng))

    def plane_peer(j):
        return (lax.rem(y + j // nx, ny), z, lax.rem(x + j % nx, nx), g)

    barrier = pltpu.get_barrier_semaphore()

    @pl.loop(0, reach)
    def _(n):
        peer = lax.rem(me + devices - reach + n, devices)
        pl.semaphore_signal(barrier, 1, device_id=coords(peer, sizes), device_id_type=MESH)

    for j in range(1, line):
        pl.semaphore_signal(barrier, 1, device_id=line_peer(j), device_id_type=MESH)
    for j in range(1, plane):
        pl.semaphore_signal(barrier, 1, device_id=plane_peer(j), device_id_type=MESH)

    loads[0].wait()
    ids = ids_ref[...]
    last = jnp.broadcast_to(ids[tiles - 1 :, TILE - 1 :], (1, TILE))
    in_last = jnp.where(ids == jnp.broadcast_to(last, ids.shape), 1.0, 0.0)
    count = jnp.sum(jnp.sum(in_last, axis=0, keepdims=True), axis=1, keepdims=True)
    first = jnp.broadcast_to(rows_dev - count.astype(jnp.int32), (8, width))
    step = 64
    sub = lax.broadcasted_iota(jnp.int32, (step, width), 0)
    loads[2].wait()

    @pl.loop(0, rows_dev // step, init_carry=jnp.zeros((step, width), jnp.float32), unroll=4)
    def open_rows(t, acc):
        at = pl.ds(pl.multiple_of(t * step, step), step)
        inside = sub + t * step >= jnp.broadcast_to(first[0:1], (step, width))
        return acc + jnp.where(inside, feat[at, :], 0.0)

    total = jnp.sum(open_rows, axis=0, keepdims=True)
    tail[0:1, :] = total[:, :TILE]
    tail[1:2, :] = total[:, TILE:]
    tail[2:3, :] = last.astype(jnp.float32)
    tail[3:4, :] = jnp.broadcast_to(count, (1, TILE))

    loads[1].wait()
    slots = ny * nz * nx * slot_cap
    owners = owners_ref[...]
    across = jnp.broadcast_to(owners, (blocks, blocks))
    down = jnp.broadcast_to(across.T[:, 0:1], (blocks, blocks))
    earlier = lax.broadcasted_iota(jnp.int32, (blocks, blocks), 1) < (
        lax.broadcasted_iota(jnp.int32, (blocks, blocks), 0)
    )
    rank = jnp.sum(jnp.where((across == down) & earlier, 1.0, 0.0), axis=1, keepdims=True)
    target = down[:, 0:1] * slot_cap + rank.astype(jnp.int32)
    hit = jnp.broadcast_to(target, (blocks, slots)) == (
        lax.broadcasted_iota(jnp.int32, (blocks, slots), 1)
    )
    used = jnp.sum(jnp.where(hit, 1.0, 0.0), axis=0, keepdims=True)
    o_from = lax.broadcasted_iota(jnp.int32, (slots, slots), 0)
    o_to = lax.broadcasted_iota(jnp.int32, (slots, slots), 1)

    def plane_of(o):
        return lax.rem(lax.div(o, nx), nz)

    def order_of(o):
        return plane_order(lax.div(o, nx * nz), lax.rem(o, nx), nx)

    ahead = (plane_of(o_from) == plane_of(o_to)) & (order_of(o_from) < order_of(o_to))
    before = jnp.dot(
        jnp.broadcast_to(used, (8, slots)).astype(jnp.bfloat16),
        jnp.where(ahead, 1.0, 0.0).astype(jnp.bfloat16),
        preferred_element_type=jnp.float32,
    )[0:1]
    spot = jnp.where(used > 0.0, before + 1.0, 0.0)
    mine[0:1, :] = spot.astype(jnp.int32)
    home = plane_of(o_to[0:1])
    key = home.astype(jnp.float32) * plane + before

    far = nz // 2
    away = lax.rem(home - z + nz, nz)
    number = [
        jnp.sum(jnp.where(away == d, used, 0.0), axis=1, keepdims=True) for d in range(nz)
    ]
    upper = jnp.floor((number[far] + 1.0) * 0.5)
    listed = jnp.full((1, slots), -1.0, jnp.float32)
    loads_by_hop = []
    for way, shift in ((0, 0.0), (1, 64.0)):
        start = jnp.full((1, 1), shift, jnp.float32)
        starts = []
        for d in range(1, far):
            at = nz - d if way else d
            starts.append(start)
            listed = jnp.where(away == at, before + start, listed)
            start = start + number[at]
        starts.append(start)
        half = (before >= upper) if way else (before < upper)
        skip = upper if way else jnp.zeros_like(upper)
        listed = jnp.where((away == far) & half, before + (start - skip), listed)
        end = start + ((number[far] - upper) if way else upper)
        loads_by_hop.append([end - first for first in starts])
    stats = jnp.zeros((1, slots), jnp.float32)
    hop_lane = lax.broadcasted_iota(jnp.int32, (1, slots), 1)
    for hop in range(far):
        load_here = jnp.maximum(loads_by_hop[0][hop], loads_by_hop[1][hop])
        stats = jnp.where(hop_lane == hop, load_here, stats)
    mine[1:2, :] = stats.astype(jnp.int32)
    list_key = jnp.sum(
        jnp.where(hit, jnp.broadcast_to(listed, (blocks, slots)), 0.0), axis=1, keepdims=True
    )
    block_key = jnp.sum(
        jnp.where(hit, jnp.broadcast_to(key, (blocks, slots)), 0.0), axis=1, keepdims=True
    )
    entry = lax.broadcasted_iota(jnp.int32, (blocks, slots), 1).astype(jnp.float32)
    order = lax.broadcasted_iota(jnp.int32, (blocks, slots), 0)
    for n, one in enumerate((block_key, list_key)):
        pack_out[n : n + 1, :] = jnp.sum(
            jnp.where(jnp.broadcast_to(one, (blocks, slots)) == entry, order, 0),
            axis=0, keepdims=True,
        )

    lane = lax.broadcasted_iota(jnp.int32, ids.shape, 1)
    after = pltpu.roll(ids, TILE - 1, 1)
    end = jnp.where((after != ids) | (lane == TILE - 1), lane, TILE)
    hop = 1
    while hop < TILE:
        nxt = jnp.where(lane + hop < TILE, pltpu.roll(end, TILE - hop, 1), TILE)
        end = jnp.minimum(end, nxt)
        hop *= 2
    ends[...] = end
    prior = jnp.concatenate([jnp.full((1, TILE), -1, jnp.int32), ids[:-1]], axis=0)
    prior = jnp.broadcast_to(prior[:, TILE - 1 :], ids.shape)
    goes_on = jnp.sum(jnp.where(ids == prior, 1.0, 0.0), axis=1, keepdims=True)
    joins[...] = jnp.broadcast_to(goes_on.astype(jnp.int32), ids.shape)

    pl.semaphore_wait(barrier, reach + line - 1 + plane - 1)

    for j in range(1, line):
        pltpu.make_async_remote_copy(
            src_ref=mine, dst_ref=got_line.at[j - 1], send_sem=line_send, recv_sem=line_recv,
            device_id=line_peer(j), device_id_type=MESH,
        ).start()

    @pl.loop(0, reach)
    def _(n):
        k = reach - n
        peer = lax.rem(me + k, devices)
        pltpu.make_async_remote_copy(
            src_ref=tail, dst_ref=got.at[k - 1], send_sem=send_sem, recv_sem=recv_sem,
            device_id=coords(peer, sizes), device_id_type=MESH,
        ).start()

    row = lax.broadcasted_iota(jnp.int32, (TILE, TILE), 0)
    col = lax.broadcasted_iota(jnp.int32, (TILE, TILE), 1)
    causal = col <= row
    ones = jnp.ones((TILE, TILE), jnp.bfloat16)

    @pl.loop(
        0, tiles,
        init_carry=(jnp.zeros((1, width), jnp.float32), jnp.zeros((1, TILE), jnp.float32)),
        unroll=4,
    )
    def _(t, carry):
        open_sum, open_count = carry
        at = pl.ds(pl.multiple_of(t * TILE, TILE), TILE)
        alive = row <= jnp.broadcast_to(ends[pl.ds(t, 1), :], (TILE, TILE))
        mask = jnp.where(alive & causal, 1.0, 0.0).astype(jnp.bfloat16)
        rows = feat[at, :]
        high = rows.astype(jnp.bfloat16)
        rest = rows - high.astype(jnp.float32)
        mid = rest.astype(jnp.bfloat16)
        low = (rest - mid.astype(jnp.float32)).astype(jnp.bfloat16)
        inside = (
            jnp.dot(mask, high, preferred_element_type=jnp.float32)
            + jnp.dot(mask, mid, preferred_element_type=jnp.float32)
            + jnp.dot(mask, low, preferred_element_type=jnp.float32)
        )
        number = jnp.dot(mask, ones, preferred_element_type=jnp.float32)
        joined = row < jnp.broadcast_to(joins[pl.ds(t, 1), :], (TILE, TILE))
        both = jnp.concatenate([joined, joined], axis=1)
        inside = inside + jnp.where(both, jnp.broadcast_to(open_sum, (TILE, width)), 0.0)
        number = number + jnp.where(joined, jnp.broadcast_to(open_count, (TILE, TILE)), 0.0)
        sums[at, :] = inside
        cnt[at, :] = number
        return inside[TILE - 1 :, :], number[TILE - 1 :, :]

    pltpu.make_async_copy(got_line, got_line, line_recv).wait()
    unpack_out[0:1, :] = mine[0:1, :]
    largest = mine[1:2, :]
    for j in range(1, line):
        both = got_line[j - 1]
        largest = jnp.maximum(largest, both[1:2, :])
        if j % ng == 0:
            unpack_out[j // ng : j // ng + 1, :] = both[0:1, :]
    spots = unpack_out[0:nz, :].astype(jnp.float32)
    here = jnp.broadcast_to(plane_of(o_to[0:1]) == z, spots.shape)
    taken = jnp.max(jnp.where(here, spots, 0.0), axis=1, keepdims=True)
    unpack_out[nz : 2 * nz, :] = jnp.broadcast_to(taken, spots.shape).astype(jnp.int32)
    top[...] = largest

    for j in range(1, plane):
        pltpu.make_async_remote_copy(
            src_ref=top, dst_ref=got_plane.at[j - 1], send_sem=plane_send,
            recv_sem=plane_recv, device_id=plane_peer(j), device_id_type=MESH,
        ).start()

    pltpu.make_async_copy(got, got, recv_sem).wait()
    arrived = got[...]
    open_id = arrived[0, 2:3, :]
    age = lax.broadcasted_iota(jnp.int32, arrived.shape, 0) + 1
    same = jnp.broadcast_to(arrived[:, 2:3, :], arrived.shape) == jnp.broadcast_to(
        open_id[None], arrived.shape
    )
    merged = jnp.sum(jnp.where(same & (age <= me), arrived, 0.0), axis=0)
    open_out[0:4, :] = merged
    in_open = jnp.where(
        ids.astype(jnp.float32) == jnp.broadcast_to(open_id, ids.shape), 1.0, 0.0
    )
    reached = jnp.sum(jnp.sum(in_open, axis=0, keepdims=True), axis=1, keepdims=True)
    open_out[4:8, :] = jnp.broadcast_to(reached, (4, TILE))

    pltpu.make_async_copy(got_plane, got_plane, plane_recv).wait()
    for j in range(1, plane):
        largest = jnp.maximum(largest, got_plane[j - 1])
    most_out[...] = largest
    pltpu.make_async_copy(got, got, send_sem).wait()
    pltpu.make_async_copy(got_line, got_line, line_send).wait()
    pltpu.make_async_copy(got_plane, got_plane, plane_send).wait()


def hop_cuts(rooms):
    one, two, three, four = rooms
    ends = ((20, one), (4, 20, two), (4, 8, 12, three), (four,))
    return [list(zip((0,) + cut[:-1], cut)) for cut in ends]


def relay_plan(rooms):
    return [
        (way, hop, a, b)
        for way in (0, 1)
        for hop, cuts in enumerate(hop_cuts(rooms))
        for a, b in cuts
    ]


def exchange_kernel(
    sizes, rooms,
    pack_ref, unpack_ref, sums, cnt, open_ref, out,
    pack, unpack, norm, stage, table_sem, z_send, z_recv, p_send, p_recv, *bufs,
):
    ny, nz, nx, ng = sizes
    plane = ny * nx
    y, z, x, g = place()
    far = nz // 2
    plan = relay_plan(rooms)
    number = {key: n for n, key in enumerate(plan)}
    cuts = hop_cuts(rooms)
    send, recv = bufs[: len(plan)], bufs[len(plan) :]
    barrier = pltpu.get_barrier_semaphore()

    def z_peer(d):
        return (y, lax.rem(z + d, nz), x, g)

    tables = [
        pltpu.make_async_copy(pack_ref, pack, table_sem.at[0]),
        pltpu.make_async_copy(unpack_ref, unpack, table_sem.at[1]),
    ]
    for table in tables:
        table.start()
    for d in (1, nz - 1):
        pl.semaphore_signal(barrier, 1, device_id=z_peer(d), device_id_type=MESH)
    for j in range(1, plane):
        pl.semaphore_signal(
            barrier, 1, device_id_type=MESH,
            device_id=(lax.rem(y + j // nx, ny), z, lax.rem(x + j % nx, nx), g),
        )

    blocks, block_rows, width = norm.shape
    open_sum = jnp.concatenate([open_ref[0:1, :], open_ref[1:2, :]], axis=1)
    open_count = open_ref[3:4, :]
    reached = open_ref[4:5, :].astype(jnp.int32)
    sub = lax.broadcasted_iota(jnp.int32, (block_rows, TILE), 0)

    @pl.loop(0, blocks, unroll=4)
    def _(b):
        at = pl.ds(pl.multiple_of(b * block_rows, block_rows), block_rows)
        joined = sub + b * block_rows < jnp.broadcast_to(reached, (block_rows, TILE))
        count = cnt[at, :] + jnp.where(
            joined, jnp.broadcast_to(open_count, (block_rows, TILE)), 0.0
        )
        scale = 1.0 / jnp.sqrt(count)
        both = jnp.concatenate([joined, joined], axis=1)
        rows = sums[at, :] + jnp.where(
            both, jnp.broadcast_to(open_sum, (block_rows, width)), 0.0
        )
        norm[b] = (rows * jnp.concatenate([scale, scale], axis=1)).astype(jnp.bfloat16)

    for table in tables:
        table.wait()
    for way in (0, 1):
        for a, b in cuts[0]:
            ref = send[number[way, 0, a, b]]

            @pl.loop(0, b - a)
            def _(k):
                ref[k] = norm[pack[1, way * 64 + a + k]]

    pl.semaphore_wait(barrier, 2 + plane - 1)

    def relay(key):
        n = number[key]
        return pltpu.make_async_remote_copy(
            src_ref=send[n], dst_ref=recv[n], send_sem=z_send.at[n], recv_sem=z_recv.at[n],
            device_id=z_peer(nz - 1 if key[0] else 1), device_id_type=MESH,
        )

    def parts(way, hop, count=None):
        return [(recv[number[way, hop, a, b]], a, b) for a, b in cuts[hop][:count]]

    def pick(spot, pieces):
        block = None
        for ref, a, b in pieces:
            one = ref[jnp.clip(spot - 1 - a, 0, b - a - 1)]
            block = one if block is None else jnp.where(spot > a, one, block)
        return block

    def go(hop, piece):
        for way in (0, 1):
            relay((way, hop, *cuts[hop][piece])).start()

    def arrived(hop, piece):
        for way in (0, 1):
            relay((way, hop, *cuts[hop][piece])).wait_recv()

    def repack(hop, piece, count):
        a, b = cuts[hop][piece]
        for way in (0, 1):
            ref = send[number[way, hop, a, b]]
            mine = unpack[nz + (nz - hop if way else hop), 0]
            pieces = parts(way, hop - 1, count)

            @pl.loop(0, b - a)
            def _(k):
                ref[k] = pick(mine + a + k + 1, pieces)

        go(hop, piece)

    def wanted(d, ty, tx, pieces):
        spot = unpack[d, (ty * nz + z) * nx + tx]
        block = pick(spot, pieces)
        return jnp.where(spot > 0, block, jnp.zeros_like(block))

    def wanted_far(ty, tx):
        spot = unpack[far, (ty * nz + z) * nx + tx]
        upper = lax.div(unpack[nz + far, 0] + 1, 2)
        block = jnp.where(
            spot > upper, pick(spot - upper, parts(1, far - 1)), pick(spot, parts(0, far - 1))
        )
        return jnp.where(spot > 0, block, jnp.zeros_like(block))

    def own(ty, tx):
        spot = unpack[0, (ty * nz + z) * nx + tx]
        block = norm[pack[0, z * plane + jnp.maximum(spot, 1) - 1]]
        return jnp.where(spot > 0, block, jnp.zeros_like(block))

    def slot_from(d):
        return (y * nz + lax.rem(z + nz - d, nz)) * nx + x

    def p_copy(d, j, ty, tx):
        return pltpu.make_async_remote_copy(
            src_ref=stage.at[d, j], dst_ref=out.at[slot_from(d)],
            send_sem=p_send, recv_sem=p_recv,
            device_id=(ty, z, tx, g), device_id_type=MESH,
        )

    def deliver(d, block_for):
        def target(j):
            return lax.rem(y + lax.div(j, nx), ny), lax.rem(x + lax.rem(j, nx), nx)

        @pl.loop(1, plane)
        def _(j):
            stage[d, j] = block_for(*target(j))

        @pl.loop(1, plane)
        def _(j):
            p_copy(d, j, *target(j)).start()

        out[slot_from(d)] = block_for(y, x)

    def deliver_from(d, count=None):
        for way in (0, 1):
            step = nz - d if way else d
            pieces = parts(way, d - 1, count)
            deliver(step, lambda ty, tx: wanted(step, ty, tx, pieces))

    def deliver_group(d, group, block_for):
        def target(j):
            ty = lax.rem(y + j, ny)
            return ty, lax.rem(group + ny - ty, nx)

        @pl.loop(0, nx)
        def _(j):
            stage[d, group * nx + j] = block_for(*target(j))

        @pl.loop(0, nx)
        def _(j):
            ty, tx = target(j)

            @pl.when((ty - y) * nx + tx - x != 0)
            def _():
                p_copy(d, group * nx + j, ty, tx).start()

    go(0, 0)
    go(0, 1)
    deliver(0, own)
    arrived(0, 0)
    repack(1, 0, 1)
    deliver_from(1, 1)
    arrived(0, 1)
    repack(1, 1, 2)
    repack(1, 2, 2)
    arrived(1, 0)
    arrived(1, 1)
    repack(2, 0, 2)
    deliver_from(2, 2)
    arrived(1, 2)
    for piece in (1, 2, 3):
        repack(2, piece, 3)
    for group in range(ny):
        arrived(2, group)
        if group == ny - 1:
            repack(3, 0, 4)
        for way in (0, 1):
            step = nz - 3 if way else 3
            pieces = parts(way, 2, group + 1)
            deliver_group(step, group, lambda ty, tx: wanted(step, ty, tx, pieces))
    for way in (0, 1):
        step = nz - 3 if way else 3
        out[slot_from(step)] = wanted(step, y, x, parts(way, 2))
    arrived(3, 0)
    for group in range(ny):
        deliver_group(far, group, wanted_far)
    out[slot_from(far)] = wanted_far(y, x)

    for key in plan:
        relay(key).wait_send()
    landed = out.at[pl.ds(0, nz * (plane - 1))]
    pltpu.make_async_copy(landed, landed, p_send).wait()
    pltpu.make_async_copy(landed, landed, p_recv).wait()


def to_hbm_kernel(src, out, sem):
    parts = sem.shape[0]
    size = src.shape[0] // parts
    copies = [
        pltpu.make_async_copy(
            src.at[pl.ds(n * size, size)], out.at[pl.ds(n * size, size)], sem.at[n]
        )
        for n in range(parts)
    ]
    for copy in copies:
        copy.start()
    for copy in copies:
        copy.wait()


def to_hbm(array):
    return pl.pallas_call(
        to_hbm_kernel,
        out_shape=pltpu.HBM(array.shape, array.dtype),
        in_specs=[pl.BlockSpec(memory_space=pltpu.VMEM)],
        out_specs=pl.BlockSpec(memory_space=pltpu.HBM),
        scratch_shapes=[pltpu.SemaphoreType.DMA((4,))],
        compiler_params=pltpu.CompilerParams(vmem_limit_bytes=1 << 20),
        name="to_hbm",
    )(array)


def body(features, session, owner_map):
    rows_dev, width = features.shape
    blocks = owner_map.shape[1]
    block_rows = rows_dev // blocks
    sizes = tuple(lax.axis_size(name) for name in ROW_GRP)
    ny, nz, nx, ng = sizes
    plane = ny * nx
    slot_cap = max(1, 2 * blocks // (plane * nz))
    slots = plane * nz * slot_cap
    tiles = rows_dev // TILE
    reach = (MOST - 2) // rows_dev + 1
    sums, cnt, open_rows, unpack, pack, most = pl.pallas_call(
        lambda *refs: prelude_kernel(sizes, reach, block_rows, slot_cap, *refs),
        out_shape=(
            jax.ShapeDtypeStruct((rows_dev, width), jnp.float32),
            jax.ShapeDtypeStruct((rows_dev, TILE), jnp.float32),
            jax.ShapeDtypeStruct((8, TILE), jnp.float32),
            jax.ShapeDtypeStruct((2 * nz, slots), jnp.int32),
            jax.ShapeDtypeStruct((2, slots), jnp.int32),
            jax.ShapeDtypeStruct((1, slots), jnp.int32),
        ),
        in_specs=[pl.BlockSpec(memory_space=pltpu.HBM)] * 3,
        out_specs=[pl.BlockSpec(memory_space=pltpu.VMEM)] * 6,
        scratch_shapes=[
            pltpu.VMEM(owner_map.shape, jnp.int32),
            pltpu.VMEM((tiles, TILE), jnp.int32),
            pltpu.VMEM((rows_dev, width), jnp.float32),
            pltpu.VMEM((tiles, TILE), jnp.int32),
            pltpu.VMEM((tiles, TILE), jnp.int32),
            pltpu.VMEM((4, TILE), jnp.float32),
            pltpu.VMEM((reach, 4, TILE), jnp.float32),
            pltpu.VMEM((2, slots), jnp.int32),
            pltpu.VMEM((nz * ng - 1, 2, slots), jnp.int32),
            pltpu.VMEM((1, slots), jnp.int32),
            pltpu.VMEM((plane - 1, 1, slots), jnp.int32),
            pltpu.SemaphoreType.DMA((3,)),
        ]
        + [pltpu.SemaphoreType.DMA] * 6,
        compiler_params=pltpu.CompilerParams(
            collective_id=0, has_side_effects=True, vmem_limit_bytes=24 << 20
        ),
        name="prelude",
    )(
        *(
            pltpu.with_memory_space_constraint(arg, pltpu.HBM)
            for arg in (owner_map, session.reshape(tiles, TILE), features)
        )
    )

    def exchange(room, number):
        block = (block_rows, width)
        return lambda pack, unpack, *rows: to_hbm(pl.pallas_call(
            lambda *refs: exchange_kernel(sizes, room, *refs),
            out_shape=pltpu.VMEM((slots, *block), jnp.bfloat16),
            in_specs=[pl.BlockSpec(memory_space=pltpu.VMEM)] * 5,
            out_specs=pl.BlockSpec(memory_space=pltpu.VMEM),
            scratch_shapes=[
                pltpu.SMEM((2, slots), jnp.int32),
                pltpu.SMEM((2 * nz, slots), jnp.int32),
                pltpu.VMEM((blocks, *block), jnp.bfloat16),
                pltpu.VMEM((nz, plane, *block), jnp.bfloat16),
                pltpu.SemaphoreType.DMA((2,)),
                pltpu.SemaphoreType.DMA((len(relay_plan(room)),)),
                pltpu.SemaphoreType.DMA((len(relay_plan(room)),)),
                pltpu.SemaphoreType.DMA,
                pltpu.SemaphoreType.DMA,
            ]
            + [
                pltpu.VMEM((b - a, *block), jnp.bfloat16)
                for _ in ("send", "recv")
                for _, _, a, b in relay_plan(room)
            ],
            compiler_params=pltpu.CompilerParams(
                collective_id=number, has_side_effects=True, vmem_limit_bytes=32 << 20
            ),
            name=f"exchange_{sum(room)}",
        )(pack, unpack, *rows))

    rooms = ROOMS
    choice = sum(
        jnp.any(most[0, : len(room)] > jnp.array(room)).astype(jnp.int32)
        for room in rooms[:-1]
    )
    return lax.switch(
        choice, [exchange(room, 1 + n) for n, room in enumerate(rooms)],
        pack, unpack, sums, cnt, open_rows,
    )


def solution(mesh):
    split = Mesh(
        mesh.devices.reshape(4, 8, 4, mesh.shape["grp"]), ("row_0", "row_1", "row_2", "grp")
    )
    return jax.shard_map(
        body,
        mesh=split,
        in_specs=(P(ROW_GRP, None), P(ROW_GRP), P(ROW_GRP, None)),
        out_specs=P(ROW_GRP, None, None),
        check_vma=False,
    )
```

```python
import jax
import jax.numpy as jnp
from jax import lax
from jax.experimental import pallas as pl
from jax.experimental.pallas import tpu as pltpu
from jax.sharding import Mesh
from jax.sharding import PartitionSpec as P

ROW = ("row_0", "row_1", "row_2")
ROW_GRP = ("row_0", "row_1", "row_2", "grp")
MOST = 163840
TILE = 128
ROOMS = ((35, 26, 17, 6), (36, 27, 18, 7), (37, 28, 19, 7), (40, 30, 21, 8), (56, 40, 24, 8))
MESH = pl.DeviceIdType.MESH


def coords(d, sizes):
    out = []
    for n in reversed(sizes):
        out.append(lax.rem(d, n))
        d = lax.div(d, n)
    return tuple(reversed(out))


def place():
    return tuple(lax.axis_index(name) for name in ROW_GRP)


def plane_order(y, x, nx):
    return lax.rem(x + y, nx) * nx + y


def prelude_kernel(
    sizes, reach, block_rows, slot_cap,
    owners_hbm, ids_hbm, feat_hbm,
    sums, cnt, open_out, unpack_out, pack_out, choice_out,
    owners_ref, ids_ref, feat, ends, joins, tail, got, mine, got_line, top, got_plane,
    load_sem, send_sem, recv_sem, line_send, line_recv, plane_send, plane_recv,
):
    ny, nz, nx, ng = sizes
    devices = ny * nz * nx * ng
    me = lax.axis_index(ROW_GRP)
    y, z, x, g = place()
    rows_dev, width = feat.shape
    tiles = rows_dev // TILE
    blocks = rows_dev // block_rows
    line = nz * ng
    plane = ny * nx
    loads = [
        pltpu.make_async_copy(src, dst, load_sem.at[n])
        for n, (src, dst) in enumerate(
            ((ids_hbm, ids_ref), (owners_hbm, owners_ref), (feat_hbm, feat))
        )
    ]
    for load in loads:
        load.start()

    def line_peer(j):
        return (y, lax.rem(z + j // ng, nz), x, lax.rem(g + j % ng, ng))

    def plane_peer(j):
        return (lax.rem(y + j // nx, ny), z, lax.rem(x + j % nx, nx), g)

    barrier = pltpu.get_barrier_semaphore()

    @pl.loop(0, reach)
    def _(n):
        peer = lax.rem(me + devices - reach + n, devices)
        pl.semaphore_signal(barrier, 1, device_id=coords(peer, sizes), device_id_type=MESH)

    for j in range(1, line):
        pl.semaphore_signal(barrier, 1, device_id=line_peer(j), device_id_type=MESH)
    for j in range(1, plane):
        pl.semaphore_signal(barrier, 1, device_id=plane_peer(j), device_id_type=MESH)

    loads[0].wait()
    ids = ids_ref[...]
    last = jnp.broadcast_to(ids[tiles - 1 :, TILE - 1 :], (1, TILE))
    in_last = jnp.where(ids == jnp.broadcast_to(last, ids.shape), 1.0, 0.0)
    count = jnp.sum(jnp.sum(in_last, axis=0, keepdims=True), axis=1, keepdims=True)
    first = jnp.broadcast_to(rows_dev - count.astype(jnp.int32), (8, width))
    step = 64
    sub = lax.broadcasted_iota(jnp.int32, (step, width), 0)
    loads[2].wait()

    @pl.loop(0, rows_dev // step, init_carry=jnp.zeros((step, width), jnp.float32), unroll=4)
    def open_rows(t, acc):
        at = pl.ds(pl.multiple_of(t * step, step), step)
        inside = sub + t * step >= jnp.broadcast_to(first[0:1], (step, width))
        return acc + jnp.where(inside, feat[at, :], 0.0)

    total = jnp.sum(open_rows, axis=0, keepdims=True)
    tail[0:1, :] = total[:, :TILE]
    tail[1:2, :] = total[:, TILE:]
    tail[2:3, :] = last.astype(jnp.float32)
    tail[3:4, :] = jnp.broadcast_to(count, (1, TILE))

    loads[1].wait()
    slots = ny * nz * nx * slot_cap
    owners = owners_ref[...]
    across = jnp.broadcast_to(owners, (blocks, blocks))
    down = jnp.broadcast_to(across.T[:, 0:1], (blocks, blocks))
    earlier = lax.broadcasted_iota(jnp.int32, (blocks, blocks), 1) < (
        lax.broadcasted_iota(jnp.int32, (blocks, blocks), 0)
    )
    rank = jnp.sum(jnp.where((across == down) & earlier, 1.0, 0.0), axis=1, keepdims=True)
    target = down[:, 0:1] * slot_cap + rank.astype(jnp.int32)
    hit = jnp.broadcast_to(target, (blocks, slots)) == (
        lax.broadcasted_iota(jnp.int32, (blocks, slots), 1)
    )
    used = jnp.sum(jnp.where(hit, 1.0, 0.0), axis=0, keepdims=True)
    o_from = lax.broadcasted_iota(jnp.int32, (slots, slots), 0)
    o_to = lax.broadcasted_iota(jnp.int32, (slots, slots), 1)

    def plane_of(o):
        return lax.rem(lax.div(o, nx), nz)

    def order_of(o):
        return plane_order(lax.div(o, nx * nz), lax.rem(o, nx), nx)

    ahead = (plane_of(o_from) == plane_of(o_to)) & (order_of(o_from) < order_of(o_to))
    before = jnp.dot(
        jnp.broadcast_to(used, (8, slots)).astype(jnp.bfloat16),
        jnp.where(ahead, 1.0, 0.0).astype(jnp.bfloat16),
        preferred_element_type=jnp.float32,
    )[0:1]
    spot = jnp.where(used > 0.0, before + 1.0, 0.0)
    mine[0:1, :] = spot.astype(jnp.int32)
    home = plane_of(o_to[0:1])
    key = home.astype(jnp.float32) * plane + before

    far = nz // 2
    away = lax.rem(home - z + nz, nz)
    number = [
        jnp.sum(jnp.where(away == d, used, 0.0), axis=1, keepdims=True) for d in range(nz)
    ]
    upper = jnp.floor((number[far] + 1.0) * 0.5)
    listed = jnp.full((1, slots), -1.0, jnp.float32)
    loads_by_hop = []
    for way, shift in ((0, 0.0), (1, 64.0)):
        start = jnp.full((1, 1), shift, jnp.float32)
        starts = []
        for d in range(1, far):
            at = nz - d if way else d
            starts.append(start)
            listed = jnp.where(away == at, before + start, listed)
            start = start + number[at]
        starts.append(start)
        half = (before >= upper) if way else (before < upper)
        skip = upper if way else jnp.zeros_like(upper)
        listed = jnp.where((away == far) & half, before + (start - skip), listed)
        end = start + ((number[far] - upper) if way else upper)
        loads_by_hop.append([end - first for first in starts])
    stats = jnp.zeros((1, slots), jnp.float32)
    hop_lane = lax.broadcasted_iota(jnp.int32, (1, slots), 1)
    for hop in range(far):
        load_here = jnp.maximum(loads_by_hop[0][hop], loads_by_hop[1][hop])
        stats = jnp.where(hop_lane == hop, load_here, stats)
    mine[1:2, :] = stats.astype(jnp.int32)
    list_key = jnp.sum(
        jnp.where(hit, jnp.broadcast_to(listed, (blocks, slots)), 0.0), axis=1, keepdims=True
    )
    block_key = jnp.sum(
        jnp.where(hit, jnp.broadcast_to(key, (blocks, slots)), 0.0), axis=1, keepdims=True
    )
    entry = lax.broadcasted_iota(jnp.int32, (blocks, slots), 1).astype(jnp.float32)
    order = lax.broadcasted_iota(jnp.int32, (blocks, slots), 0)
    for n, one in enumerate((block_key, list_key)):
        pack_out[n : n + 1, :] = jnp.sum(
            jnp.where(jnp.broadcast_to(one, (blocks, slots)) == entry, order, 0),
            axis=0, keepdims=True,
        )

    lane = lax.broadcasted_iota(jnp.int32, ids.shape, 1)
    after = pltpu.roll(ids, TILE - 1, 1)
    end = jnp.where((after != ids) | (lane == TILE - 1), lane, TILE)
    hop = 1
    while hop < TILE:
        nxt = jnp.where(lane + hop < TILE, pltpu.roll(end, TILE - hop, 1), TILE)
        end = jnp.minimum(end, nxt)
        hop *= 2
    ends[...] = end
    prior = jnp.concatenate([jnp.full((1, TILE), -1, jnp.int32), ids[:-1]], axis=0)
    prior = jnp.broadcast_to(prior[:, TILE - 1 :], ids.shape)
    goes_on = jnp.sum(jnp.where(ids == prior, 1.0, 0.0), axis=1, keepdims=True)
    joins[...] = jnp.broadcast_to(goes_on.astype(jnp.int32), ids.shape)

    pl.semaphore_wait(barrier, reach + line - 1 + plane - 1)

    for j in range(1, line):
        pltpu.make_async_remote_copy(
            src_ref=mine, dst_ref=got_line.at[j - 1], send_sem=line_send, recv_sem=line_recv,
            device_id=line_peer(j), device_id_type=MESH,
        ).start()

    @pl.loop(0, reach)
    def _(n):
        k = reach - n
        peer = lax.rem(me + k, devices)
        pltpu.make_async_remote_copy(
            src_ref=tail, dst_ref=got.at[k - 1], send_sem=send_sem, recv_sem=recv_sem,
            device_id=coords(peer, sizes), device_id_type=MESH,
        ).start()

    row = lax.broadcasted_iota(jnp.int32, (TILE, TILE), 0)
    col = lax.broadcasted_iota(jnp.int32, (TILE, TILE), 1)
    causal = col <= row
    ones = jnp.ones((TILE, TILE), jnp.bfloat16)

    @pl.loop(
        0, tiles,
        init_carry=(jnp.zeros((1, width), jnp.float32), jnp.zeros((1, TILE), jnp.float32)),
        unroll=4,
    )
    def _(t, carry):
        open_sum, open_count = carry
        at = pl.ds(pl.multiple_of(t * TILE, TILE), TILE)
        alive = row <= jnp.broadcast_to(ends[pl.ds(t, 1), :], (TILE, TILE))
        mask = jnp.where(alive & causal, 1.0, 0.0).astype(jnp.bfloat16)
        rows = feat[at, :]
        high = rows.astype(jnp.bfloat16)
        rest = rows - high.astype(jnp.float32)
        mid = rest.astype(jnp.bfloat16)
        low = (rest - mid.astype(jnp.float32)).astype(jnp.bfloat16)
        inside = (
            jnp.dot(mask, high, preferred_element_type=jnp.float32)
            + jnp.dot(mask, mid, preferred_element_type=jnp.float32)
            + jnp.dot(mask, low, preferred_element_type=jnp.float32)
        )
        number = jnp.dot(mask, ones, preferred_element_type=jnp.float32)
        joined = row < jnp.broadcast_to(joins[pl.ds(t, 1), :], (TILE, TILE))
        both = jnp.concatenate([joined, joined], axis=1)
        inside = inside + jnp.where(both, jnp.broadcast_to(open_sum, (TILE, width)), 0.0)
        number = number + jnp.where(joined, jnp.broadcast_to(open_count, (TILE, TILE)), 0.0)
        sums[at, :] = inside
        cnt[at, :] = number
        return inside[TILE - 1 :, :], number[TILE - 1 :, :]

    pltpu.make_async_copy(got_line, got_line, line_recv).wait()
    unpack_out[0:1, :] = mine[0:1, :]
    largest = mine[1:2, :]
    for j in range(1, line):
        both = got_line[j - 1]
        largest = jnp.maximum(largest, both[1:2, :])
        if j % ng == 0:
            unpack_out[j // ng : j // ng + 1, :] = both[0:1, :]
    spots = unpack_out[0:nz, :].astype(jnp.float32)
    here = jnp.broadcast_to(plane_of(o_to[0:1]) == z, spots.shape)
    taken = jnp.max(jnp.where(here, spots, 0.0), axis=1, keepdims=True)
    unpack_out[nz : 2 * nz, :] = jnp.broadcast_to(taken, spots.shape).astype(jnp.int32)
    top[...] = largest

    for j in range(1, plane):
        pltpu.make_async_remote_copy(
            src_ref=top, dst_ref=got_plane.at[j - 1], send_sem=plane_send,
            recv_sem=plane_recv, device_id=plane_peer(j), device_id_type=MESH,
        ).start()

    pltpu.make_async_copy(got, got, recv_sem).wait()
    arrived = got[...]
    open_id = arrived[0, 2:3, :]
    age = lax.broadcasted_iota(jnp.int32, arrived.shape, 0) + 1
    same = jnp.broadcast_to(arrived[:, 2:3, :], arrived.shape) == jnp.broadcast_to(
        open_id[None], arrived.shape
    )
    merged = jnp.sum(jnp.where(same & (age <= me), arrived, 0.0), axis=0)
    open_out[0:4, :] = merged
    in_open = jnp.where(
        ids.astype(jnp.float32) == jnp.broadcast_to(open_id, ids.shape), 1.0, 0.0
    )
    reached = jnp.sum(jnp.sum(in_open, axis=0, keepdims=True), axis=1, keepdims=True)
    open_out[4:8, :] = jnp.broadcast_to(reached, (4, TILE))

    pltpu.make_async_copy(got_plane, got_plane, plane_recv).wait()
    for j in range(1, plane):
        largest = jnp.maximum(largest, got_plane[j - 1])
    choice = jnp.zeros((1, 1), jnp.float32)
    largest = largest.astype(jnp.float32)
    for rooms in ROOMS[:-1]:
        room = jnp.zeros((1, slots), jnp.float32)
        for hop, size in enumerate(rooms):
            room = jnp.where(hop_lane == hop, float(size), room)
        over = jnp.max(jnp.where(largest > room, 1.0, 0.0), axis=1, keepdims=True)
        choice = choice + over
    choice_out[...] = jnp.broadcast_to(choice, (1, slots)).astype(jnp.int32)
    pltpu.make_async_copy(got, got, send_sem).wait()
    pltpu.make_async_copy(got_line, got_line, line_send).wait()
    pltpu.make_async_copy(got_plane, got_plane, plane_send).wait()


def hop_cuts(rooms):
    one, two, three, four = rooms
    ends = ((16, 24, one), (8, 12, 20, two), (4, 8, 12, three), (four,))
    return [list(zip((0,) + cut[:-1], cut)) for cut in ends]


def relay_plan(rooms):
    return [
        (way, hop, a, b)
        for way in (0, 1)
        for hop, cuts in enumerate(hop_cuts(rooms))
        for a, b in cuts
    ]


def exchange_kernel(
    sizes, rooms,
    pack_ref, unpack_ref, sums, cnt, open_ref, out,
    pack, unpack, norm, stage, table_sem, z_send, z_recv, p_send, p_recv, *bufs,
):
    ny, nz, nx, ng = sizes
    plane = ny * nx
    y, z, x, g = place()
    far = nz // 2
    plan = relay_plan(rooms)
    number = {key: n for n, key in enumerate(plan)}
    cuts = hop_cuts(rooms)
    send, recv = bufs[: len(plan)], bufs[len(plan) :]
    barrier = pltpu.get_barrier_semaphore()

    def z_peer(d):
        return (y, lax.rem(z + d, nz), x, g)

    tables = [
        pltpu.make_async_copy(pack_ref, pack, table_sem.at[0]),
        pltpu.make_async_copy(unpack_ref, unpack, table_sem.at[1]),
    ]
    for table in tables:
        table.start()
    for d in (1, nz - 1):
        pl.semaphore_signal(barrier, 1, device_id=z_peer(d), device_id_type=MESH)
    for j in range(1, plane):
        pl.semaphore_signal(
            barrier, 1, device_id_type=MESH,
            device_id=(lax.rem(y + j // nx, ny), z, lax.rem(x + j % nx, nx), g),
        )

    blocks, block_rows, width = norm.shape
    open_sum = jnp.concatenate([open_ref[0:1, :], open_ref[1:2, :]], axis=1)
    open_count = open_ref[3:4, :]
    reached = open_ref[4:5, :].astype(jnp.int32)
    sub = lax.broadcasted_iota(jnp.int32, (block_rows, TILE), 0)

    @pl.loop(0, blocks, unroll=4)
    def _(b):
        at = pl.ds(pl.multiple_of(b * block_rows, block_rows), block_rows)
        joined = sub + b * block_rows < jnp.broadcast_to(reached, (block_rows, TILE))
        count = cnt[at, :] + jnp.where(
            joined, jnp.broadcast_to(open_count, (block_rows, TILE)), 0.0
        )
        scale = 1.0 / jnp.sqrt(count)
        both = jnp.concatenate([joined, joined], axis=1)
        rows = sums[at, :] + jnp.where(
            both, jnp.broadcast_to(open_sum, (block_rows, width)), 0.0
        )
        norm[b] = (rows * jnp.concatenate([scale, scale], axis=1)).astype(jnp.bfloat16)

    for table in tables:
        table.wait()
    for way in (0, 1):
        for a, b in cuts[0]:
            ref = send[number[way, 0, a, b]]

            @pl.loop(0, b - a)
            def _(k):
                ref[k] = norm[pack[1, way * 64 + a + k]]

    pl.semaphore_wait(barrier, 2 + plane - 1)

    def relay(key):
        n = number[key]
        return pltpu.make_async_remote_copy(
            src_ref=send[n], dst_ref=recv[n], send_sem=z_send.at[n], recv_sem=z_recv.at[n],
            device_id=z_peer(nz - 1 if key[0] else 1), device_id_type=MESH,
        )

    def parts(way, hop, count=None):
        return [(recv[number[way, hop, a, b]], a, b) for a, b in cuts[hop][:count]]

    def pick(spot, pieces):
        block = None
        for ref, a, b in pieces:
            one = ref[jnp.clip(spot - 1 - a, 0, b - a - 1)]
            block = one if block is None else jnp.where(spot > a, one, block)
        return block

    def go(hop, piece):
        for way in (0, 1):
            relay((way, hop, *cuts[hop][piece])).start()

    def arrived(hop, piece):
        for way in (0, 1):
            relay((way, hop, *cuts[hop][piece])).wait_recv()

    def repack(hop, piece, count):
        a, b = cuts[hop][piece]
        for way in (0, 1):
            ref = send[number[way, hop, a, b]]
            mine = unpack[nz + (nz - hop if way else hop), 0]
            pieces = parts(way, hop - 1, count)

            @pl.loop(0, b - a)
            def _(k):
                ref[k] = pick(mine + a + k + 1, pieces)

        go(hop, piece)

    def wanted(d, ty, tx, pieces):
        spot = unpack[d, (ty * nz + z) * nx + tx]
        block = pick(spot, pieces)
        return jnp.where(spot > 0, block, jnp.zeros_like(block))

    def wanted_far(ty, tx):
        spot = unpack[far, (ty * nz + z) * nx + tx]
        upper = lax.div(unpack[nz + far, 0] + 1, 2)
        block = jnp.where(
            spot > upper, pick(spot - upper, parts(1, far - 1)), pick(spot, parts(0, far - 1))
        )
        return jnp.where(spot > 0, block, jnp.zeros_like(block))

    def own(ty, tx):
        spot = unpack[0, (ty * nz + z) * nx + tx]
        block = norm[pack[0, z * plane + jnp.maximum(spot, 1) - 1]]
        return jnp.where(spot > 0, block, jnp.zeros_like(block))

    def slot_from(d):
        return (y * nz + lax.rem(z + nz - d, nz)) * nx + x

    def p_copy(d, j, ty, tx):
        return pltpu.make_async_remote_copy(
            src_ref=stage.at[d, j], dst_ref=out.at[slot_from(d)],
            send_sem=p_send, recv_sem=p_recv,
            device_id=(ty, z, tx, g), device_id_type=MESH,
        )

    def deliver(d, block_for):
        def target(j):
            return lax.rem(y + lax.div(j, nx), ny), lax.rem(x + lax.rem(j, nx), nx)

        @pl.loop(1, plane)
        def _(j):
            stage[d, j] = block_for(*target(j))

        @pl.loop(1, plane)
        def _(j):
            p_copy(d, j, *target(j)).start()

        out[slot_from(d)] = block_for(y, x)

    def deliver_from(d, count=None):
        for way in (0, 1):
            step = nz - d if way else d
            pieces = parts(way, d - 1, count)
            deliver(step, lambda ty, tx: wanted(step, ty, tx, pieces))

    def deliver_group(d, group, block_for):
        def target(j):
            ty = lax.rem(y + j, ny)
            return ty, lax.rem(group + ny - ty, nx)

        @pl.loop(0, nx)
        def _(j):
            stage[d, group * nx + j] = block_for(*target(j))

        @pl.loop(0, nx)
        def _(j):
            ty, tx = target(j)

            @pl.when((ty - y) * nx + tx - x != 0)
            def _():
                p_copy(d, group * nx + j, ty, tx).start()

    def deliver_groups(d, groups, count):
        for way in (0, 1):
            step = nz - d if way else d
            pieces = parts(way, d - 1, count)
            for group in groups:
                deliver_group(step, group, lambda ty, tx: wanted(step, ty, tx, pieces))

    def keep(d):
        for way in (0, 1):
            step = nz - d if way else d
            out[slot_from(step)] = wanted(step, y, x, parts(way, d - 1))

    for piece in range(3):
        go(0, piece)
    deliver(0, own)
    arrived(0, 0)
    deliver_from(1, 1)
    arrived(0, 1)
    repack(1, 0, 2)
    arrived(0, 2)
    for piece in (1, 2, 3):
        repack(1, piece, 3)
    arrived(1, 0)
    deliver_groups(2, (0, 1), 1)
    arrived(1, 1)
    deliver_groups(2, (2,), 2)
    arrived(1, 2)
    repack(2, 0, 3)
    deliver_groups(2, (3,), 3)
    arrived(1, 3)
    for piece in (1, 2, 3):
        repack(2, piece, 4)
    keep(2)
    for group in range(ny):
        arrived(2, group)
        if group == ny - 1:
            repack(3, 0, 4)
        deliver_groups(3, (group,), group + 1)
    keep(3)
    arrived(3, 0)
    for group in range(ny):
        deliver_group(far, group, wanted_far)
    out[slot_from(far)] = wanted_far(y, x)

    for key in plan:
        relay(key).wait_send()
    landed = out.at[pl.ds(0, nz * (plane - 1))]
    pltpu.make_async_copy(landed, landed, p_send).wait()
    pltpu.make_async_copy(landed, landed, p_recv).wait()


def to_hbm_kernel(src, out, sem):
    parts = sem.shape[0]
    size = src.shape[0] // parts
    copies = [
        pltpu.make_async_copy(
            src.at[pl.ds(n * size, size)], out.at[pl.ds(n * size, size)], sem.at[n]
        )
        for n in range(parts)
    ]
    for copy in copies:
        copy.start()
    for copy in copies:
        copy.wait()


def to_hbm(array):
    return pl.pallas_call(
        to_hbm_kernel,
        out_shape=pltpu.HBM(array.shape, array.dtype),
        in_specs=[pl.BlockSpec(memory_space=pltpu.VMEM)],
        out_specs=pl.BlockSpec(memory_space=pltpu.HBM),
        scratch_shapes=[pltpu.SemaphoreType.DMA((4,))],
        compiler_params=pltpu.CompilerParams(vmem_limit_bytes=1 << 20),
        name="to_hbm",
    )(array)


def body(features, session, owner_map):
    rows_dev, width = features.shape
    blocks = owner_map.shape[1]
    block_rows = rows_dev // blocks
    sizes = tuple(lax.axis_size(name) for name in ROW_GRP)
    ny, nz, nx, ng = sizes
    plane = ny * nx
    slot_cap = max(1, 2 * blocks // (plane * nz))
    slots = plane * nz * slot_cap
    tiles = rows_dev // TILE
    reach = (MOST - 2) // rows_dev + 1
    sums, cnt, open_rows, unpack, pack, choice = pl.pallas_call(
        lambda *refs: prelude_kernel(sizes, reach, block_rows, slot_cap, *refs),
        out_shape=(
            jax.ShapeDtypeStruct((rows_dev, width), jnp.float32),
            jax.ShapeDtypeStruct((rows_dev, TILE), jnp.float32),
            jax.ShapeDtypeStruct((8, TILE), jnp.float32),
            jax.ShapeDtypeStruct((2 * nz, slots), jnp.int32),
            jax.ShapeDtypeStruct((2, slots), jnp.int32),
            jax.ShapeDtypeStruct((1, slots), jnp.int32),
        ),
        in_specs=[pl.BlockSpec(memory_space=pltpu.HBM)] * 3,
        out_specs=[pl.BlockSpec(memory_space=pltpu.VMEM)] * 6,
        scratch_shapes=[
            pltpu.VMEM(owner_map.shape, jnp.int32),
            pltpu.VMEM((tiles, TILE), jnp.int32),
            pltpu.VMEM((rows_dev, width), jnp.float32),
            pltpu.VMEM((tiles, TILE), jnp.int32),
            pltpu.VMEM((tiles, TILE), jnp.int32),
            pltpu.VMEM((4, TILE), jnp.float32),
            pltpu.VMEM((reach, 4, TILE), jnp.float32),
            pltpu.VMEM((2, slots), jnp.int32),
            pltpu.VMEM((nz * ng - 1, 2, slots), jnp.int32),
            pltpu.VMEM((1, slots), jnp.int32),
            pltpu.VMEM((plane - 1, 1, slots), jnp.int32),
            pltpu.SemaphoreType.DMA((3,)),
        ]
        + [pltpu.SemaphoreType.DMA] * 6,
        compiler_params=pltpu.CompilerParams(
            collective_id=0, has_side_effects=True, vmem_limit_bytes=24 << 20
        ),
        name="prelude",
    )(
        *(
            pltpu.with_memory_space_constraint(arg, pltpu.HBM)
            for arg in (owner_map, session.reshape(tiles, TILE), features)
        )
    )

    def exchange(room, number):
        block = (block_rows, width)
        return lambda pack, unpack, *rows: to_hbm(pl.pallas_call(
            lambda *refs: exchange_kernel(sizes, room, *refs),
            out_shape=pltpu.VMEM((slots, *block), jnp.bfloat16),
            in_specs=[pl.BlockSpec(memory_space=pltpu.VMEM)] * 5,
            out_specs=pl.BlockSpec(memory_space=pltpu.VMEM),
            scratch_shapes=[
                pltpu.SMEM((2, slots), jnp.int32),
                pltpu.SMEM((2 * nz, slots), jnp.int32),
                pltpu.VMEM((blocks, *block), jnp.bfloat16),
                pltpu.VMEM((nz, plane, *block), jnp.bfloat16),
                pltpu.SemaphoreType.DMA((2,)),
                pltpu.SemaphoreType.DMA((len(relay_plan(room)),)),
                pltpu.SemaphoreType.DMA((len(relay_plan(room)),)),
                pltpu.SemaphoreType.DMA,
                pltpu.SemaphoreType.DMA,
            ]
            + [
                pltpu.VMEM((b - a, *block), jnp.bfloat16)
                for _ in ("send", "recv")
                for _, _, a, b in relay_plan(room)
            ],
            compiler_params=pltpu.CompilerParams(
                collective_id=number, has_side_effects=True, vmem_limit_bytes=24 << 20
            ),
            name=f"exchange_{sum(room)}",
        )(pack, unpack, *rows))

    rooms = ROOMS
    return lax.switch(
        choice[0, 0], [exchange(room, 1 + n) for n, room in enumerate(rooms)],
        pack, unpack, sums, cnt, open_rows,
    )


def solution(mesh):
    split = Mesh(
        mesh.devices.reshape(4, 8, 4, mesh.shape["grp"]), ("row_0", "row_1", "row_2", "grp")
    )
    return jax.shard_map(
        body,
        mesh=split,
        in_specs=(P(ROW_GRP, None), P(ROW_GRP), P(ROW_GRP, None)),
        out_specs=P(ROW_GRP, None, None),
        check_vma=False,
    )
```

```python
import jax
import jax.numpy as jnp
from jax import lax
from jax.experimental import pallas as pl
from jax.experimental.pallas import tpu as pltpu
from jax.sharding import Mesh
from jax.sharding import PartitionSpec as P

ROW = ("row_0", "row_1", "row_2")
ROW_GRP = ("row_0", "row_1", "row_2", "grp")
MOST = 163840
TILE = 128
ROOMS = (
    (34, 25, 16, 6), (35, 26, 17, 6), (36, 27, 18, 7), (37, 28, 19, 7),
    (38, 29, 20, 7), (40, 30, 21, 8), (56, 40, 24, 8),
)
MESH = pl.DeviceIdType.MESH


def coords(d, sizes):
    out = []
    for n in reversed(sizes):
        out.append(lax.rem(d, n))
        d = lax.div(d, n)
    return tuple(reversed(out))


def place():
    return tuple(lax.axis_index(name) for name in ROW_GRP)


def plane_order(y, x, nx):
    return lax.rem(x + y, nx) * nx + y


def prelude_kernel(
    sizes, reach, block_rows, slot_cap,
    owners_hbm, ids_hbm, feat_hbm,
    sums, cnt, open_out, unpack_out, pack_out, choice_out,
    owners_ref, ids_ref, feat, ends, joins, tail, got, mine, got_line, top, got_plane,
    load_sem, send_sem, recv_sem, line_send, line_recv, plane_send, plane_recv,
):
    ny, nz, nx, ng = sizes
    devices = ny * nz * nx * ng
    me = lax.axis_index(ROW_GRP)
    y, z, x, g = place()
    rows_dev, width = feat.shape
    tiles = rows_dev // TILE
    blocks = rows_dev // block_rows
    line = nz * ng
    plane = ny * nx
    loads = [
        pltpu.make_async_copy(src, dst, load_sem.at[n])
        for n, (src, dst) in enumerate(
            ((ids_hbm, ids_ref), (owners_hbm, owners_ref), (feat_hbm, feat))
        )
    ]
    for load in loads:
        load.start()

    def line_peer(j):
        return (y, lax.rem(z + j // ng, nz), x, lax.rem(g + j % ng, ng))

    def plane_peer(j):
        return (lax.rem(y + j // nx, ny), z, lax.rem(x + j % nx, nx), g)

    barrier = pltpu.get_barrier_semaphore()

    @pl.loop(0, reach)
    def _(n):
        peer = lax.rem(me + devices - reach + n, devices)
        pl.semaphore_signal(barrier, 1, device_id=coords(peer, sizes), device_id_type=MESH)

    for j in range(1, line):
        pl.semaphore_signal(barrier, 1, device_id=line_peer(j), device_id_type=MESH)
    for j in range(1, plane):
        pl.semaphore_signal(barrier, 1, device_id=plane_peer(j), device_id_type=MESH)

    loads[0].wait()
    ids = ids_ref[...]
    last = jnp.broadcast_to(ids[tiles - 1 :, TILE - 1 :], (1, TILE))
    in_last = jnp.where(ids == jnp.broadcast_to(last, ids.shape), 1.0, 0.0)
    count = jnp.sum(jnp.sum(in_last, axis=0, keepdims=True), axis=1, keepdims=True)
    first = jnp.broadcast_to(rows_dev - count.astype(jnp.int32), (8, width))
    step = 64
    sub = lax.broadcasted_iota(jnp.int32, (step, width), 0)
    loads[2].wait()

    @pl.loop(0, rows_dev // step, init_carry=jnp.zeros((step, width), jnp.float32), unroll=4)
    def open_rows(t, acc):
        at = pl.ds(pl.multiple_of(t * step, step), step)
        inside = sub + t * step >= jnp.broadcast_to(first[0:1], (step, width))
        return acc + jnp.where(inside, feat[at, :], 0.0)

    total = jnp.sum(open_rows, axis=0, keepdims=True)
    tail[0:1, :] = total[:, :TILE]
    tail[1:2, :] = total[:, TILE:]
    tail[2:3, :] = last.astype(jnp.float32)
    tail[3:4, :] = jnp.broadcast_to(count, (1, TILE))

    loads[1].wait()
    slots = ny * nz * nx * slot_cap
    owners = owners_ref[...]
    across = jnp.broadcast_to(owners, (blocks, blocks))
    down = jnp.broadcast_to(across.T[:, 0:1], (blocks, blocks))
    earlier = lax.broadcasted_iota(jnp.int32, (blocks, blocks), 1) < (
        lax.broadcasted_iota(jnp.int32, (blocks, blocks), 0)
    )
    rank = jnp.sum(jnp.where((across == down) & earlier, 1.0, 0.0), axis=1, keepdims=True)
    target = down[:, 0:1] * slot_cap + rank.astype(jnp.int32)
    hit = jnp.broadcast_to(target, (blocks, slots)) == (
        lax.broadcasted_iota(jnp.int32, (blocks, slots), 1)
    )
    used = jnp.sum(jnp.where(hit, 1.0, 0.0), axis=0, keepdims=True)
    o_from = lax.broadcasted_iota(jnp.int32, (slots, slots), 0)
    o_to = lax.broadcasted_iota(jnp.int32, (slots, slots), 1)

    def plane_of(o):
        return lax.rem(lax.div(o, nx), nz)

    def order_of(o):
        return plane_order(lax.div(o, nx * nz), lax.rem(o, nx), nx)

    ahead = (plane_of(o_from) == plane_of(o_to)) & (order_of(o_from) < order_of(o_to))
    before = jnp.dot(
        jnp.broadcast_to(used, (8, slots)).astype(jnp.bfloat16),
        jnp.where(ahead, 1.0, 0.0).astype(jnp.bfloat16),
        preferred_element_type=jnp.float32,
    )[0:1]
    spot = jnp.where(used > 0.0, before + 1.0, 0.0)
    mine[0:1, :] = spot.astype(jnp.int32)
    home = plane_of(o_to[0:1])
    key = home.astype(jnp.float32) * plane + before

    far = nz // 2
    away = lax.rem(home - z + nz, nz)
    number = [
        jnp.sum(jnp.where(away == d, used, 0.0), axis=1, keepdims=True) for d in range(nz)
    ]
    upper = jnp.floor((number[far] + 1.0) * 0.5)
    listed = jnp.full((1, slots), -1.0, jnp.float32)
    loads_by_hop = []
    for way, shift in ((0, 0.0), (1, 64.0)):
        start = jnp.full((1, 1), shift, jnp.float32)
        starts = []
        for d in range(1, far):
            at = nz - d if way else d
            starts.append(start)
            listed = jnp.where(away == at, before + start, listed)
            start = start + number[at]
        starts.append(start)
        half = (before >= upper) if way else (before < upper)
        skip = upper if way else jnp.zeros_like(upper)
        listed = jnp.where((away == far) & half, before + (start - skip), listed)
        end = start + ((number[far] - upper) if way else upper)
        loads_by_hop.append([end - first for first in starts])
    stats = jnp.zeros((1, slots), jnp.float32)
    hop_lane = lax.broadcasted_iota(jnp.int32, (1, slots), 1)
    for hop in range(far):
        load_here = jnp.maximum(loads_by_hop[0][hop], loads_by_hop[1][hop])
        stats = jnp.where(hop_lane == hop, load_here, stats)
    mine[1:2, :] = stats.astype(jnp.int32)
    list_key = jnp.sum(
        jnp.where(hit, jnp.broadcast_to(listed, (blocks, slots)), 0.0), axis=1, keepdims=True
    )
    block_key = jnp.sum(
        jnp.where(hit, jnp.broadcast_to(key, (blocks, slots)), 0.0), axis=1, keepdims=True
    )
    entry = lax.broadcasted_iota(jnp.int32, (blocks, slots), 1).astype(jnp.float32)
    order = lax.broadcasted_iota(jnp.int32, (blocks, slots), 0)
    for n, one in enumerate((block_key, list_key)):
        pack_out[n : n + 1, :] = jnp.sum(
            jnp.where(jnp.broadcast_to(one, (blocks, slots)) == entry, order, 0),
            axis=0, keepdims=True,
        )

    lane = lax.broadcasted_iota(jnp.int32, ids.shape, 1)
    after = pltpu.roll(ids, TILE - 1, 1)
    end = jnp.where((after != ids) | (lane == TILE - 1), lane, TILE)
    hop = 1
    while hop < TILE:
        nxt = jnp.where(lane + hop < TILE, pltpu.roll(end, TILE - hop, 1), TILE)
        end = jnp.minimum(end, nxt)
        hop *= 2
    ends[...] = end
    prior = jnp.concatenate([jnp.full((1, TILE), -1, jnp.int32), ids[:-1]], axis=0)
    prior = jnp.broadcast_to(prior[:, TILE - 1 :], ids.shape)
    goes_on = jnp.sum(jnp.where(ids == prior, 1.0, 0.0), axis=1, keepdims=True)
    joins[...] = jnp.broadcast_to(goes_on.astype(jnp.int32), ids.shape)

    pl.semaphore_wait(barrier, reach + line - 1 + plane - 1)

    for j in range(1, line):
        pltpu.make_async_remote_copy(
            src_ref=mine, dst_ref=got_line.at[j - 1], send_sem=line_send, recv_sem=line_recv,
            device_id=line_peer(j), device_id_type=MESH,
        ).start()

    @pl.loop(0, reach)
    def _(n):
        k = reach - n
        peer = lax.rem(me + k, devices)
        pltpu.make_async_remote_copy(
            src_ref=tail, dst_ref=got.at[k - 1], send_sem=send_sem, recv_sem=recv_sem,
            device_id=coords(peer, sizes), device_id_type=MESH,
        ).start()

    row = lax.broadcasted_iota(jnp.int32, (TILE, TILE), 0)
    col = lax.broadcasted_iota(jnp.int32, (TILE, TILE), 1)
    causal = col <= row
    ones = jnp.ones((TILE, TILE), jnp.bfloat16)

    @pl.loop(
        0, tiles,
        init_carry=(jnp.zeros((1, width), jnp.float32), jnp.zeros((1, TILE), jnp.float32)),
        unroll=4,
    )
    def _(t, carry):
        open_sum, open_count = carry
        at = pl.ds(pl.multiple_of(t * TILE, TILE), TILE)
        alive = row <= jnp.broadcast_to(ends[pl.ds(t, 1), :], (TILE, TILE))
        mask = jnp.where(alive & causal, 1.0, 0.0).astype(jnp.bfloat16)
        rows = feat[at, :]
        high = rows.astype(jnp.bfloat16)
        rest = rows - high.astype(jnp.float32)
        mid = rest.astype(jnp.bfloat16)
        low = (rest - mid.astype(jnp.float32)).astype(jnp.bfloat16)
        inside = (
            jnp.dot(mask, high, preferred_element_type=jnp.float32)
            + jnp.dot(mask, mid, preferred_element_type=jnp.float32)
            + jnp.dot(mask, low, preferred_element_type=jnp.float32)
        )
        number = jnp.dot(mask, ones, preferred_element_type=jnp.float32)
        joined = row < jnp.broadcast_to(joins[pl.ds(t, 1), :], (TILE, TILE))
        both = jnp.concatenate([joined, joined], axis=1)
        inside = inside + jnp.where(both, jnp.broadcast_to(open_sum, (TILE, width)), 0.0)
        number = number + jnp.where(joined, jnp.broadcast_to(open_count, (TILE, TILE)), 0.0)
        sums[at, :] = inside
        cnt[at, :] = number
        return inside[TILE - 1 :, :], number[TILE - 1 :, :]

    pltpu.make_async_copy(got_line, got_line, line_recv).wait()
    unpack_out[0:1, :] = mine[0:1, :]
    largest = mine[1:2, :]
    for j in range(1, line):
        both = got_line[j - 1]
        largest = jnp.maximum(largest, both[1:2, :])
        if j % ng == 0:
            unpack_out[j // ng : j // ng + 1, :] = both[0:1, :]
    spots = unpack_out[0:nz, :].astype(jnp.float32)
    here = jnp.broadcast_to(plane_of(o_to[0:1]) == z, spots.shape)
    taken = jnp.max(jnp.where(here, spots, 0.0), axis=1, keepdims=True)
    unpack_out[nz : 2 * nz, :] = jnp.broadcast_to(taken, spots.shape).astype(jnp.int32)
    top[...] = largest

    for j in range(1, plane):
        pltpu.make_async_remote_copy(
            src_ref=top, dst_ref=got_plane.at[j - 1], send_sem=plane_send,
            recv_sem=plane_recv, device_id=plane_peer(j), device_id_type=MESH,
        ).start()

    pltpu.make_async_copy(got, got, recv_sem).wait()
    arrived = got[...]
    open_id = arrived[0, 2:3, :]
    age = lax.broadcasted_iota(jnp.int32, arrived.shape, 0) + 1
    same = jnp.broadcast_to(arrived[:, 2:3, :], arrived.shape) == jnp.broadcast_to(
        open_id[None], arrived.shape
    )
    merged = jnp.sum(jnp.where(same & (age <= me), arrived, 0.0), axis=0)
    open_out[0:4, :] = merged
    in_open = jnp.where(
        ids.astype(jnp.float32) == jnp.broadcast_to(open_id, ids.shape), 1.0, 0.0
    )
    reached = jnp.sum(jnp.sum(in_open, axis=0, keepdims=True), axis=1, keepdims=True)
    open_out[4:8, :] = jnp.broadcast_to(reached, (4, TILE))

    pltpu.make_async_copy(got_plane, got_plane, plane_recv).wait()
    for j in range(1, plane):
        largest = jnp.maximum(largest, got_plane[j - 1])
    choice = jnp.zeros((1, 1), jnp.float32)
    largest = largest.astype(jnp.float32)
    for rooms in ROOMS[:-1]:
        room = jnp.zeros((1, slots), jnp.float32)
        for hop, size in enumerate(rooms):
            room = jnp.where(hop_lane == hop, float(size), room)
        over = jnp.max(jnp.where(largest > room, 1.0, 0.0), axis=1, keepdims=True)
        choice = choice + over
    choice_out[...] = jnp.broadcast_to(choice, (1, slots)).astype(jnp.int32)
    pltpu.make_async_copy(got, got, send_sem).wait()
    pltpu.make_async_copy(got_line, got_line, line_send).wait()
    pltpu.make_async_copy(got_plane, got_plane, plane_send).wait()


def hop_cuts(rooms):
    one, two, three, four = rooms
    ends = ((16, 24, one), (8, 12, 20, two), (4, 8, 12, three), (four,))
    return [list(zip((0,) + cut[:-1], cut)) for cut in ends]


def relay_plan(rooms):
    return [
        (way, hop, a, b)
        for way in (0, 1)
        for hop, cuts in enumerate(hop_cuts(rooms))
        for a, b in cuts
    ]


def exchange_kernel(
    sizes, rooms,
    pack_ref, unpack_ref, sums, cnt, open_ref, out,
    pack, unpack, norm, stage, ring, table_sem, z_send, z_recv, p_send, p_recv, *bufs,
):
    ny, nz, nx, ng = sizes
    plane = ny * nx
    y, z, x, g = place()
    far = nz // 2
    plan = relay_plan(rooms)
    number = {key: n for n, key in enumerate(plan)}
    cuts = hop_cuts(rooms)
    send, recv = bufs[: len(plan)], bufs[len(plan) :]
    barrier = pltpu.get_barrier_semaphore()

    def z_peer(d):
        return (y, lax.rem(z + d, nz), x, g)

    tables = [
        pltpu.make_async_copy(pack_ref, pack, table_sem.at[0]),
        pltpu.make_async_copy(unpack_ref, unpack, table_sem.at[1]),
    ]
    for table in tables:
        table.start()
    x_ring = [(y, z, lax.rem(x + j, nx), g) for j in range(1, nx)]
    y_ring = [(lax.rem(y + j, ny), z, x, g) for j in range(1, ny)]
    near = [z_peer(1), z_peer(nz - 1)] + x_ring + y_ring
    for peer in near:
        pl.semaphore_signal(barrier, 1, device_id=peer, device_id_type=MESH)

    blocks, block_rows, width = norm.shape
    open_sum = jnp.concatenate([open_ref[0:1, :], open_ref[1:2, :]], axis=1)
    open_count = open_ref[3:4, :]
    reached = open_ref[4:5, :].astype(jnp.int32)
    sub = lax.broadcasted_iota(jnp.int32, (block_rows, TILE), 0)

    @pl.loop(0, blocks, unroll=4)
    def _(b):
        at = pl.ds(pl.multiple_of(b * block_rows, block_rows), block_rows)
        joined = sub + b * block_rows < jnp.broadcast_to(reached, (block_rows, TILE))
        count = cnt[at, :] + jnp.where(
            joined, jnp.broadcast_to(open_count, (block_rows, TILE)), 0.0
        )
        scale = 1.0 / jnp.sqrt(count)
        both = jnp.concatenate([joined, joined], axis=1)
        rows = sums[at, :] + jnp.where(
            both, jnp.broadcast_to(open_sum, (block_rows, width)), 0.0
        )
        norm[b] = (rows * jnp.concatenate([scale, scale], axis=1)).astype(jnp.bfloat16)

    for table in tables:
        table.wait()
    for way in (0, 1):
        for a, b in cuts[0]:
            ref = send[number[way, 0, a, b]]

            @pl.loop(0, b - a)
            def _(k):
                ref[k] = norm[pack[1, way * 64 + a + k]]

    pl.semaphore_wait(barrier, len(near))

    def relay(key):
        n = number[key]
        return pltpu.make_async_remote_copy(
            src_ref=send[n], dst_ref=recv[n], send_sem=z_send.at[n], recv_sem=z_recv.at[n],
            device_id=z_peer(nz - 1 if key[0] else 1), device_id_type=MESH,
        )

    def parts(way, hop, count=None):
        return [(recv[number[way, hop, a, b]], a, b) for a, b in cuts[hop][:count]]

    def pick(spot, pieces):
        block = None
        for ref, a, b in pieces:
            one = ref[jnp.clip(spot - 1 - a, 0, b - a - 1)]
            block = one if block is None else jnp.where(spot > a, one, block)
        return block

    def go(hop, piece):
        for way in (0, 1):
            relay((way, hop, *cuts[hop][piece])).start()

    def arrived(hop, piece):
        for way in (0, 1):
            relay((way, hop, *cuts[hop][piece])).wait_recv()

    def repack(hop, piece, count):
        a, b = cuts[hop][piece]
        for way in (0, 1):
            ref = send[number[way, hop, a, b]]
            mine = unpack[nz + (nz - hop if way else hop), 0]
            pieces = parts(way, hop - 1, count)

            @pl.loop(0, b - a)
            def _(k):
                ref[k] = pick(mine + a + k + 1, pieces)

        go(hop, piece)

    def wanted(d, ty, tx, pieces):
        spot = unpack[d, (ty * nz + z) * nx + tx]
        block = pick(spot, pieces)
        return jnp.where(spot > 0, block, jnp.zeros_like(block))

    def wanted_far(ty, tx):
        spot = unpack[far, (ty * nz + z) * nx + tx]
        upper = lax.div(unpack[nz + far, 0] + 1, 2)
        block = jnp.where(
            spot > upper, pick(spot - upper, parts(1, far - 1)), pick(spot, parts(0, far - 1))
        )
        return jnp.where(spot > 0, block, jnp.zeros_like(block))

    def own(ty, tx):
        spot = unpack[0, (ty * nz + z) * nx + tx]
        block = norm[pack[0, z * plane + jnp.maximum(spot, 1) - 1]]
        return jnp.where(spot > 0, block, jnp.zeros_like(block))

    def slot_from(d):
        return (y * nz + lax.rem(z + nz - d, nz)) * nx + x

    def p_copy(d, j, ty, tx):
        return pltpu.make_async_remote_copy(
            src_ref=stage.at[d, j], dst_ref=out.at[slot_from(d)],
            send_sem=p_send, recv_sem=p_recv,
            device_id=(ty, z, tx, g), device_id_type=MESH,
        )

    def deliver(d, block_for):
        def target(j):
            return lax.rem(y + lax.div(j, nx), ny), lax.rem(x + lax.rem(j, nx), nx)

        @pl.loop(1, plane)
        def _(j):
            stage[d, j] = block_for(*target(j))

        @pl.loop(1, plane)
        def _(j):
            p_copy(d, j, *target(j)).start()

        out[slot_from(d)] = block_for(y, x)

    def deliver_from(d, count=None):
        for way in (0, 1):
            step = nz - d if way else d
            pieces = parts(way, d - 1, count)
            deliver(step, lambda ty, tx: wanted(step, ty, tx, pieces))

    def deliver_group(d, group, block_for):
        def target(j):
            ty = lax.rem(y + j, ny)
            return ty, lax.rem(group + ny - ty, nx)

        @pl.loop(0, nx)
        def _(j):
            stage[d, group * nx + j] = block_for(*target(j))

        @pl.loop(0, nx)
        def _(j):
            ty, tx = target(j)

            @pl.when((ty - y) * nx + tx - x != 0)
            def _():
                p_copy(d, group * nx + j, ty, tx).start()

    def deliver_groups(d, groups, count):
        for way in (0, 1):
            step = nz - d if way else d
            pieces = parts(way, d - 1, count)
            for group in groups:
                deliver_group(step, group, lambda ty, tx: wanted(step, ty, tx, pieces))

    def keep(d):
        for way in (0, 1):
            step = nz - d if way else d
            out[slot_from(step)] = wanted(step, y, x, parts(way, d - 1))

    for piece in range(3):
        go(0, piece)
    for peer in x_ring:
        pl.semaphore_signal(ring, 1, device_id=peer, device_id_type=MESH)
    pl.semaphore_wait(ring, len(x_ring))
    deliver(0, own)
    arrived(0, 0)
    deliver_from(1, 1)
    arrived(0, 1)
    repack(1, 0, 2)
    arrived(0, 2)
    for piece in (1, 2, 3):
        repack(1, piece, 3)
    arrived(1, 0)
    deliver_groups(2, (0, 1), 1)
    arrived(1, 1)
    deliver_groups(2, (2,), 2)
    arrived(1, 2)
    repack(2, 0, 3)
    deliver_groups(2, (3,), 3)
    arrived(1, 3)
    for piece in (1, 2, 3):
        repack(2, piece, 4)
    keep(2)
    for group in range(ny):
        arrived(2, group)
        if group == ny - 1:
            repack(3, 0, 4)
        deliver_groups(3, (group,), group + 1)
    keep(3)
    arrived(3, 0)
    for group in range(ny):
        deliver_group(far, group, wanted_far)
    out[slot_from(far)] = wanted_far(y, x)

    for key in plan:
        relay(key).wait_send()
    landed = out.at[pl.ds(0, nz * (plane - 1))]
    pltpu.make_async_copy(landed, landed, p_send).wait()
    pltpu.make_async_copy(landed, landed, p_recv).wait()


def to_hbm_kernel(src, out, sem):
    parts = sem.shape[0]
    size = src.shape[0] // parts
    copies = [
        pltpu.make_async_copy(
            src.at[pl.ds(n * size, size)], out.at[pl.ds(n * size, size)], sem.at[n]
        )
        for n in range(parts)
    ]
    for copy in copies:
        copy.start()
    for copy in copies:
        copy.wait()


def to_hbm(array):
    return pl.pallas_call(
        to_hbm_kernel,
        out_shape=pltpu.HBM(array.shape, array.dtype),
        in_specs=[pl.BlockSpec(memory_space=pltpu.VMEM)],
        out_specs=pl.BlockSpec(memory_space=pltpu.HBM),
        scratch_shapes=[pltpu.SemaphoreType.DMA((4,))],
        compiler_params=pltpu.CompilerParams(vmem_limit_bytes=1 << 20),
        name="to_hbm",
    )(array)


def body(features, session, owner_map):
    rows_dev, width = features.shape
    blocks = owner_map.shape[1]
    block_rows = rows_dev // blocks
    sizes = tuple(lax.axis_size(name) for name in ROW_GRP)
    ny, nz, nx, ng = sizes
    plane = ny * nx
    slot_cap = max(1, 2 * blocks // (plane * nz))
    slots = plane * nz * slot_cap
    tiles = rows_dev // TILE
    reach = (MOST - 2) // rows_dev + 1
    sums, cnt, open_rows, unpack, pack, choice = pl.pallas_call(
        lambda *refs: prelude_kernel(sizes, reach, block_rows, slot_cap, *refs),
        out_shape=(
            jax.ShapeDtypeStruct((rows_dev, width), jnp.float32),
            jax.ShapeDtypeStruct((rows_dev, TILE), jnp.float32),
            jax.ShapeDtypeStruct((8, TILE), jnp.float32),
            jax.ShapeDtypeStruct((2 * nz, slots), jnp.int32),
            jax.ShapeDtypeStruct((2, slots), jnp.int32),
            jax.ShapeDtypeStruct((1, slots), jnp.int32),
        ),
        in_specs=[pl.BlockSpec(memory_space=pltpu.HBM)] * 3,
        out_specs=[pl.BlockSpec(memory_space=pltpu.VMEM)] * 6,
        scratch_shapes=[
            pltpu.VMEM(owner_map.shape, jnp.int32),
            pltpu.VMEM((tiles, TILE), jnp.int32),
            pltpu.VMEM((rows_dev, width), jnp.float32),
            pltpu.VMEM((tiles, TILE), jnp.int32),
            pltpu.VMEM((tiles, TILE), jnp.int32),
            pltpu.VMEM((4, TILE), jnp.float32),
            pltpu.VMEM((reach, 4, TILE), jnp.float32),
            pltpu.VMEM((2, slots), jnp.int32),
            pltpu.VMEM((nz * ng - 1, 2, slots), jnp.int32),
            pltpu.VMEM((1, slots), jnp.int32),
            pltpu.VMEM((plane - 1, 1, slots), jnp.int32),
            pltpu.SemaphoreType.DMA((3,)),
        ]
        + [pltpu.SemaphoreType.DMA] * 6,
        compiler_params=pltpu.CompilerParams(
            collective_id=0, has_side_effects=True, vmem_limit_bytes=24 << 20
        ),
        name="prelude",
    )(
        *(
            pltpu.with_memory_space_constraint(arg, pltpu.HBM)
            for arg in (owner_map, session.reshape(tiles, TILE), features)
        )
    )

    def exchange(room, number):
        block = (block_rows, width)
        return lambda pack, unpack, *rows: to_hbm(pl.pallas_call(
            lambda *refs: exchange_kernel(sizes, room, *refs),
            out_shape=pltpu.VMEM((slots, *block), jnp.bfloat16),
            in_specs=[pl.BlockSpec(memory_space=pltpu.VMEM)] * 5,
            out_specs=pl.BlockSpec(memory_space=pltpu.VMEM),
            scratch_shapes=[
                pltpu.SMEM((2, slots), jnp.int32),
                pltpu.SMEM((2 * nz, slots), jnp.int32),
                pltpu.VMEM((blocks, *block), jnp.bfloat16),
                pltpu.VMEM((nz, plane, *block), jnp.bfloat16),
                pltpu.SemaphoreType.REGULAR,
                pltpu.SemaphoreType.DMA((2,)),
                pltpu.SemaphoreType.DMA((len(relay_plan(room)),)),
                pltpu.SemaphoreType.DMA((len(relay_plan(room)),)),
                pltpu.SemaphoreType.DMA,
                pltpu.SemaphoreType.DMA,
            ]
            + [
                pltpu.VMEM((b - a, *block), jnp.bfloat16)
                for _ in ("send", "recv")
                for _, _, a, b in relay_plan(room)
            ],
            compiler_params=pltpu.CompilerParams(
                collective_id=number, has_side_effects=True, vmem_limit_bytes=24 << 20
            ),
            name=f"exchange_{sum(room)}",
        )(pack, unpack, *rows))

    rooms = ROOMS
    return lax.switch(
        choice[0, 0], [exchange(room, 1 + n) for n, room in enumerate(rooms)],
        pack, unpack, sums, cnt, open_rows,
    )


def solution(mesh):
    split = Mesh(
        mesh.devices.reshape(4, 8, 4, mesh.shape["grp"]), ("row_0", "row_1", "row_2", "grp")
    )
    return jax.shard_map(
        body,
        mesh=split,
        in_specs=(P(ROW_GRP, None), P(ROW_GRP), P(ROW_GRP, None)),
        out_specs=P(ROW_GRP, None, None),
        check_vma=False,
    )
```

```python
import jax
import jax.numpy as jnp
from jax import lax
from jax.experimental import pallas as pl
from jax.experimental.pallas import tpu as pltpu
from jax.sharding import Mesh
from jax.sharding import PartitionSpec as P

ROW = ("row_0", "row_1", "row_2")
ROW_GRP = ("row_0", "row_1", "row_2", "grp")
MOST = 163840
TILE = 128
ROOMS = (
    (34, 25, 16, 6), (35, 26, 17, 6), (36, 27, 18, 7), (37, 28, 19, 7),
    (38, 29, 20, 7), (40, 30, 21, 8), (56, 40, 24, 8),
)
MESH = pl.DeviceIdType.MESH


def coords(d, sizes):
    out = []
    for n in reversed(sizes):
        out.append(lax.rem(d, n))
        d = lax.div(d, n)
    return tuple(reversed(out))


def place():
    return tuple(lax.axis_index(name) for name in ROW_GRP)


def plane_order(dy, dx, nx):
    return lax.rem(dy - dx + nx, nx) * nx + dx


def prelude_kernel(
    sizes, reach, block_rows, slot_cap,
    owners_hbm, ids_hbm, feat_hbm,
    sums, cnt, open_out, unpack_out, pack_out, choice_out,
    owners_ref, ids_ref, feat, ends, joins, tail, got, mine, got_line, top, got_plane,
    load_sem, send_sem, recv_sem, line_send, line_recv, plane_send, plane_recv,
):
    ny, nz, nx, ng = sizes
    devices = ny * nz * nx * ng
    me = lax.axis_index(ROW_GRP)
    y, z, x, g = place()
    rows_dev, width = feat.shape
    tiles = rows_dev // TILE
    blocks = rows_dev // block_rows
    line = nz * ng
    plane = ny * nx
    loads = [
        pltpu.make_async_copy(src, dst, load_sem.at[n])
        for n, (src, dst) in enumerate(
            ((ids_hbm, ids_ref), (owners_hbm, owners_ref), (feat_hbm, feat))
        )
    ]
    for load in loads:
        load.start()

    def line_peer(j):
        return (y, lax.rem(z + j // ng, nz), x, lax.rem(g + j % ng, ng))

    def plane_peer(j):
        return (lax.rem(y + j // nx, ny), z, lax.rem(x + j % nx, nx), g)

    barrier = pltpu.get_barrier_semaphore()

    @pl.loop(0, reach)
    def _(n):
        peer = lax.rem(me + devices - reach + n, devices)
        pl.semaphore_signal(barrier, 1, device_id=coords(peer, sizes), device_id_type=MESH)

    for j in range(1, line):
        pl.semaphore_signal(barrier, 1, device_id=line_peer(j), device_id_type=MESH)
    for j in range(1, plane):
        pl.semaphore_signal(barrier, 1, device_id=plane_peer(j), device_id_type=MESH)

    loads[0].wait()
    ids = ids_ref[...]
    last = jnp.broadcast_to(ids[tiles - 1 :, TILE - 1 :], (1, TILE))
    in_last = jnp.where(ids == jnp.broadcast_to(last, ids.shape), 1.0, 0.0)
    count = jnp.sum(jnp.sum(in_last, axis=0, keepdims=True), axis=1, keepdims=True)
    first = jnp.broadcast_to(rows_dev - count.astype(jnp.int32), (8, width))
    step = 64
    sub = lax.broadcasted_iota(jnp.int32, (step, width), 0)
    loads[2].wait()

    @pl.loop(0, rows_dev // step, init_carry=jnp.zeros((step, width), jnp.float32), unroll=4)
    def open_rows(t, acc):
        at = pl.ds(pl.multiple_of(t * step, step), step)
        inside = sub + t * step >= jnp.broadcast_to(first[0:1], (step, width))
        return acc + jnp.where(inside, feat[at, :], 0.0)

    total = jnp.sum(open_rows, axis=0, keepdims=True)
    tail[0:1, :] = total[:, :TILE]
    tail[1:2, :] = total[:, TILE:]
    tail[2:3, :] = last.astype(jnp.float32)
    tail[3:4, :] = jnp.broadcast_to(count, (1, TILE))

    loads[1].wait()
    slots = ny * nz * nx * slot_cap
    owners = owners_ref[...]
    across = jnp.broadcast_to(owners, (blocks, blocks))
    down = jnp.broadcast_to(across.T[:, 0:1], (blocks, blocks))
    earlier = lax.broadcasted_iota(jnp.int32, (blocks, blocks), 1) < (
        lax.broadcasted_iota(jnp.int32, (blocks, blocks), 0)
    )
    rank = jnp.sum(jnp.where((across == down) & earlier, 1.0, 0.0), axis=1, keepdims=True)
    target = down[:, 0:1] * slot_cap + rank.astype(jnp.int32)
    hit = jnp.broadcast_to(target, (blocks, slots)) == (
        lax.broadcasted_iota(jnp.int32, (blocks, slots), 1)
    )
    used = jnp.sum(jnp.where(hit, 1.0, 0.0), axis=0, keepdims=True)
    o_from = lax.broadcasted_iota(jnp.int32, (slots, slots), 0)
    o_to = lax.broadcasted_iota(jnp.int32, (slots, slots), 1)

    def plane_of(o):
        return lax.rem(lax.div(o, nx), nz)

    def order_of(o):
        dy = lax.rem(lax.div(o, nx * nz) - y + ny, ny)
        dx = lax.rem(lax.rem(o, nx) - x + nx, nx)
        return plane_order(dy, dx, nx)

    ahead = (plane_of(o_from) == plane_of(o_to)) & (order_of(o_from) < order_of(o_to))
    before = jnp.dot(
        jnp.broadcast_to(used, (8, slots)).astype(jnp.bfloat16),
        jnp.where(ahead, 1.0, 0.0).astype(jnp.bfloat16),
        preferred_element_type=jnp.float32,
    )[0:1]
    spot = jnp.where(used > 0.0, before + 1.0, 0.0)
    mine[0:1, :] = spot.astype(jnp.int32)
    home = plane_of(o_to[0:1])
    key = home.astype(jnp.float32) * plane + before

    far = nz // 2
    away = lax.rem(home - z + nz, nz)
    number = [
        jnp.sum(jnp.where(away == d, used, 0.0), axis=1, keepdims=True) for d in range(nz)
    ]
    upper = jnp.floor((number[far] + 1.0) * 0.5)
    listed = jnp.full((1, slots), -1.0, jnp.float32)
    loads_by_hop = []
    for way, shift in ((0, 0.0), (1, 64.0)):
        start = jnp.full((1, 1), shift, jnp.float32)
        starts = []
        for d in range(1, far):
            at = nz - d if way else d
            starts.append(start)
            listed = jnp.where(away == at, before + start, listed)
            start = start + number[at]
        starts.append(start)
        half = (before >= upper) if way else (before < upper)
        skip = upper if way else jnp.zeros_like(upper)
        listed = jnp.where((away == far) & half, before + (start - skip), listed)
        end = start + ((number[far] - upper) if way else upper)
        loads_by_hop.append([end - first for first in starts])
    stats = jnp.zeros((1, slots), jnp.float32)
    hop_lane = lax.broadcasted_iota(jnp.int32, (1, slots), 1)
    for hop in range(far):
        load_here = jnp.maximum(loads_by_hop[0][hop], loads_by_hop[1][hop])
        stats = jnp.where(hop_lane == hop, load_here, stats)
    mine[1:2, :] = stats.astype(jnp.int32)
    list_key = jnp.sum(
        jnp.where(hit, jnp.broadcast_to(listed, (blocks, slots)), 0.0), axis=1, keepdims=True
    )
    block_key = jnp.sum(
        jnp.where(hit, jnp.broadcast_to(key, (blocks, slots)), 0.0), axis=1, keepdims=True
    )
    entry = lax.broadcasted_iota(jnp.int32, (blocks, slots), 1).astype(jnp.float32)
    order = lax.broadcasted_iota(jnp.int32, (blocks, slots), 0)
    for n, one in enumerate((block_key, list_key)):
        pack_out[n : n + 1, :] = jnp.sum(
            jnp.where(jnp.broadcast_to(one, (blocks, slots)) == entry, order, 0),
            axis=0, keepdims=True,
        )

    lane = lax.broadcasted_iota(jnp.int32, ids.shape, 1)
    after = pltpu.roll(ids, TILE - 1, 1)
    end = jnp.where((after != ids) | (lane == TILE - 1), lane, TILE)
    hop = 1
    while hop < TILE:
        nxt = jnp.where(lane + hop < TILE, pltpu.roll(end, TILE - hop, 1), TILE)
        end = jnp.minimum(end, nxt)
        hop *= 2
    ends[...] = end
    prior = jnp.concatenate([jnp.full((1, TILE), -1, jnp.int32), ids[:-1]], axis=0)
    prior = jnp.broadcast_to(prior[:, TILE - 1 :], ids.shape)
    goes_on = jnp.sum(jnp.where(ids == prior, 1.0, 0.0), axis=1, keepdims=True)
    joins[...] = jnp.broadcast_to(goes_on.astype(jnp.int32), ids.shape)

    pl.semaphore_wait(barrier, reach + line - 1 + plane - 1)

    for j in range(1, line):
        pltpu.make_async_remote_copy(
            src_ref=mine, dst_ref=got_line.at[j - 1], send_sem=line_send, recv_sem=line_recv,
            device_id=line_peer(j), device_id_type=MESH,
        ).start()

    @pl.loop(0, reach)
    def _(n):
        k = reach - n
        peer = lax.rem(me + k, devices)
        pltpu.make_async_remote_copy(
            src_ref=tail, dst_ref=got.at[k - 1], send_sem=send_sem, recv_sem=recv_sem,
            device_id=coords(peer, sizes), device_id_type=MESH,
        ).start()

    row = lax.broadcasted_iota(jnp.int32, (TILE, TILE), 0)
    col = lax.broadcasted_iota(jnp.int32, (TILE, TILE), 1)
    causal = col <= row
    ones = jnp.ones((TILE, TILE), jnp.bfloat16)

    @pl.loop(
        0, tiles,
        init_carry=(jnp.zeros((1, width), jnp.float32), jnp.zeros((1, TILE), jnp.float32)),
        unroll=4,
    )
    def _(t, carry):
        open_sum, open_count = carry
        at = pl.ds(pl.multiple_of(t * TILE, TILE), TILE)
        alive = row <= jnp.broadcast_to(ends[pl.ds(t, 1), :], (TILE, TILE))
        mask = jnp.where(alive & causal, 1.0, 0.0).astype(jnp.bfloat16)
        rows = feat[at, :]
        high = rows.astype(jnp.bfloat16)
        rest = rows - high.astype(jnp.float32)
        mid = rest.astype(jnp.bfloat16)
        low = (rest - mid.astype(jnp.float32)).astype(jnp.bfloat16)
        inside = (
            jnp.dot(mask, high, preferred_element_type=jnp.float32)
            + jnp.dot(mask, mid, preferred_element_type=jnp.float32)
            + jnp.dot(mask, low, preferred_element_type=jnp.float32)
        )
        number = jnp.dot(mask, ones, preferred_element_type=jnp.float32)
        joined = row < jnp.broadcast_to(joins[pl.ds(t, 1), :], (TILE, TILE))
        both = jnp.concatenate([joined, joined], axis=1)
        inside = inside + jnp.where(both, jnp.broadcast_to(open_sum, (TILE, width)), 0.0)
        number = number + jnp.where(joined, jnp.broadcast_to(open_count, (TILE, TILE)), 0.0)
        sums[at, :] = inside
        cnt[at, :] = number
        return inside[TILE - 1 :, :], number[TILE - 1 :, :]

    pltpu.make_async_copy(got_line, got_line, line_recv).wait()
    unpack_out[0:1, :] = mine[0:1, :]
    largest = mine[1:2, :]
    for j in range(1, line):
        both = got_line[j - 1]
        largest = jnp.maximum(largest, both[1:2, :])
        if j % ng == 0:
            unpack_out[j // ng : j // ng + 1, :] = both[0:1, :]
    spots = unpack_out[0:nz, :].astype(jnp.float32)
    here = jnp.broadcast_to(plane_of(o_to[0:1]) == z, spots.shape)
    taken = jnp.max(jnp.where(here, spots, 0.0), axis=1, keepdims=True)
    unpack_out[nz : 2 * nz, :] = jnp.broadcast_to(taken, spots.shape).astype(jnp.int32)
    top[...] = largest

    for j in range(1, plane):
        pltpu.make_async_remote_copy(
            src_ref=top, dst_ref=got_plane.at[j - 1], send_sem=plane_send,
            recv_sem=plane_recv, device_id=plane_peer(j), device_id_type=MESH,
        ).start()

    pltpu.make_async_copy(got, got, recv_sem).wait()
    arrived = got[...]
    open_id = arrived[0, 2:3, :]
    age = lax.broadcasted_iota(jnp.int32, arrived.shape, 0) + 1
    same = jnp.broadcast_to(arrived[:, 2:3, :], arrived.shape) == jnp.broadcast_to(
        open_id[None], arrived.shape
    )
    merged = jnp.sum(jnp.where(same & (age <= me), arrived, 0.0), axis=0)
    open_out[0:4, :] = merged
    in_open = jnp.where(
        ids.astype(jnp.float32) == jnp.broadcast_to(open_id, ids.shape), 1.0, 0.0
    )
    reached = jnp.sum(jnp.sum(in_open, axis=0, keepdims=True), axis=1, keepdims=True)
    open_out[4:8, :] = jnp.broadcast_to(reached, (4, TILE))

    pltpu.make_async_copy(got_plane, got_plane, plane_recv).wait()
    for j in range(1, plane):
        largest = jnp.maximum(largest, got_plane[j - 1])
    choice = jnp.zeros((1, 1), jnp.float32)
    largest = largest.astype(jnp.float32)
    for rooms in ROOMS[:-1]:
        room = jnp.zeros((1, slots), jnp.float32)
        for hop, size in enumerate(rooms):
            room = jnp.where(hop_lane == hop, float(size), room)
        over = jnp.max(jnp.where(largest > room, 1.0, 0.0), axis=1, keepdims=True)
        choice = choice + over
    choice_out[...] = jnp.broadcast_to(choice, (1, slots)).astype(jnp.int32)
    pltpu.make_async_copy(got, got, send_sem).wait()
    pltpu.make_async_copy(got_line, got_line, line_send).wait()
    pltpu.make_async_copy(got_plane, got_plane, plane_send).wait()


def hop_cuts(rooms):
    one, two, three, four = rooms
    ends = ((16, 24, one), (8, 12, 20, two), (4, 8, 12, three), (four,))
    return [list(zip((0,) + cut[:-1], cut)) for cut in ends]


def relay_plan(rooms):
    return [
        (way, hop, a, b)
        for way in (0, 1)
        for hop, cuts in enumerate(hop_cuts(rooms))
        for a, b in cuts
    ]


def exchange_kernel(
    sizes, rooms,
    pack_ref, unpack_ref, sums, cnt, open_ref, out,
    pack, unpack, norm, stage, ring, table_sem, z_send, z_recv, p_send, p_recv, *bufs,
):
    ny, nz, nx, ng = sizes
    plane = ny * nx
    y, z, x, g = place()
    far = nz // 2
    plan = relay_plan(rooms)
    number = {key: n for n, key in enumerate(plan)}
    cuts = hop_cuts(rooms)
    send, recv = bufs[: len(plan)], bufs[len(plan) :]
    barrier = pltpu.get_barrier_semaphore()

    def z_peer(d):
        return (y, lax.rem(z + d, nz), x, g)

    tables = [
        pltpu.make_async_copy(pack_ref, pack, table_sem.at[0]),
        pltpu.make_async_copy(unpack_ref, unpack, table_sem.at[1]),
    ]
    for table in tables:
        table.start()
    x_ring = [(y, z, lax.rem(x + j, nx), g) for j in range(1, nx)]
    y_ring = [(lax.rem(y + j, ny), z, x, g) for j in range(1, ny)]
    near = [z_peer(1), z_peer(nz - 1)] + x_ring + y_ring
    for peer in near:
        pl.semaphore_signal(barrier, 1, device_id=peer, device_id_type=MESH)

    blocks, block_rows, width = norm.shape
    open_sum = jnp.concatenate([open_ref[0:1, :], open_ref[1:2, :]], axis=1)
    open_count = open_ref[3:4, :]
    reached = open_ref[4:5, :].astype(jnp.int32)
    sub = lax.broadcasted_iota(jnp.int32, (block_rows, TILE), 0)

    @pl.loop(0, blocks, unroll=4)
    def _(b):
        at = pl.ds(pl.multiple_of(b * block_rows, block_rows), block_rows)
        joined = sub + b * block_rows < jnp.broadcast_to(reached, (block_rows, TILE))
        count = cnt[at, :] + jnp.where(
            joined, jnp.broadcast_to(open_count, (block_rows, TILE)), 0.0
        )
        scale = 1.0 / jnp.sqrt(count)
        both = jnp.concatenate([joined, joined], axis=1)
        rows = sums[at, :] + jnp.where(
            both, jnp.broadcast_to(open_sum, (block_rows, width)), 0.0
        )
        norm[b] = (rows * jnp.concatenate([scale, scale], axis=1)).astype(jnp.bfloat16)

    for table in tables:
        table.wait()
    for way in (0, 1):
        for a, b in cuts[0]:
            ref = send[number[way, 0, a, b]]

            @pl.loop(0, b - a)
            def _(k):
                ref[k] = norm[pack[1, way * 64 + a + k]]

    pl.semaphore_wait(barrier, len(near))

    def relay(key):
        n = number[key]
        return pltpu.make_async_remote_copy(
            src_ref=send[n], dst_ref=recv[n], send_sem=z_send.at[n], recv_sem=z_recv.at[n],
            device_id=z_peer(nz - 1 if key[0] else 1), device_id_type=MESH,
        )

    def parts(way, hop, count=None):
        return [(recv[number[way, hop, a, b]], a, b) for a, b in cuts[hop][:count]]

    def pick(spot, pieces):
        block = None
        for ref, a, b in pieces:
            one = ref[jnp.clip(spot - 1 - a, 0, b - a - 1)]
            block = one if block is None else jnp.where(spot > a, one, block)
        return block

    def go(hop, piece):
        for way in (0, 1):
            relay((way, hop, *cuts[hop][piece])).start()

    def arrived(hop, piece):
        for way in (0, 1):
            relay((way, hop, *cuts[hop][piece])).wait_recv()

    def repack(hop, piece, count):
        a, b = cuts[hop][piece]
        for way in (0, 1):
            ref = send[number[way, hop, a, b]]
            mine = unpack[nz + (nz - hop if way else hop), 0]
            pieces = parts(way, hop - 1, count)

            @pl.loop(0, b - a)
            def _(k):
                ref[k] = pick(mine + a + k + 1, pieces)

        go(hop, piece)

    def wanted(d, ty, tx, pieces):
        spot = unpack[d, (ty * nz + z) * nx + tx]
        block = pick(spot, pieces)
        return jnp.where(spot > 0, block, jnp.zeros_like(block))

    def wanted_far(ty, tx):
        spot = unpack[far, (ty * nz + z) * nx + tx]
        upper = lax.div(unpack[nz + far, 0] + 1, 2)
        block = jnp.where(
            spot > upper, pick(spot - upper, parts(1, far - 1)), pick(spot, parts(0, far - 1))
        )
        return jnp.where(spot > 0, block, jnp.zeros_like(block))

    def own(ty, tx):
        spot = unpack[0, (ty * nz + z) * nx + tx]
        block = norm[pack[0, z * plane + jnp.maximum(spot, 1) - 1]]
        return jnp.where(spot > 0, block, jnp.zeros_like(block))

    def slot_from(d):
        return (y * nz + lax.rem(z + nz - d, nz)) * nx + x

    def p_copy(d, j, ty, tx):
        return pltpu.make_async_remote_copy(
            src_ref=stage.at[d, j], dst_ref=out.at[slot_from(d)],
            send_sem=p_send, recv_sem=p_recv,
            device_id=(ty, z, tx, g), device_id_type=MESH,
        )

    def deliver(d, block_for):
        def target(j):
            return lax.rem(y + lax.div(j, nx), ny), lax.rem(x + lax.rem(j, nx), nx)

        @pl.loop(1, plane)
        def _(j):
            stage[d, j] = block_for(*target(j))

        @pl.loop(1, plane)
        def _(j):
            p_copy(d, j, *target(j)).start()

        out[slot_from(d)] = block_for(y, x)

    def deliver_from(d, count=None):
        for way in (0, 1):
            step = nz - d if way else d
            pieces = parts(way, d - 1, count)
            deliver(step, lambda ty, tx: wanted(step, ty, tx, pieces))

    def deliver_group(d, group, block_for):
        def target(j):
            return lax.rem(y + group + j, ny), lax.rem(x + j, nx)

        first = 1 if group == 0 else 0

        @pl.loop(first, nx)
        def _(j):
            stage[d, group * nx + j] = block_for(*target(j))

        @pl.loop(first, nx)
        def _(j):
            p_copy(d, group * nx + j, *target(j)).start()

    def deliver_groups(d, groups, count):
        for way in (0, 1):
            step = nz - d if way else d
            pieces = parts(way, d - 1, count)
            for group in groups:
                deliver_group(step, group, lambda ty, tx: wanted(step, ty, tx, pieces))

    def keep(d):
        for way in (0, 1):
            step = nz - d if way else d
            out[slot_from(step)] = wanted(step, y, x, parts(way, d - 1))

    for piece in range(3):
        go(0, piece)
    for peer in x_ring:
        pl.semaphore_signal(ring, 1, device_id=peer, device_id_type=MESH)
    pl.semaphore_wait(ring, len(x_ring))
    deliver(0, own)
    arrived(0, 0)
    deliver_from(1, 1)
    arrived(0, 1)
    repack(1, 0, 2)
    arrived(0, 2)
    for piece in (1, 2, 3):
        repack(1, piece, 3)
    arrived(1, 0)
    deliver_groups(2, (0, 1), 1)
    arrived(1, 1)
    deliver_groups(2, (2,), 2)
    arrived(1, 2)
    repack(2, 0, 3)
    deliver_groups(2, (3,), 3)
    arrived(1, 3)
    for piece in (1, 2, 3):
        repack(2, piece, 4)
    keep(2)
    for group in range(ny):
        arrived(2, group)
        if group == ny - 1:
            repack(3, 0, 4)
        deliver_groups(3, (group,), group + 1)
    keep(3)
    arrived(3, 0)
    for group in range(ny):
        deliver_group(far, group, wanted_far)
    out[slot_from(far)] = wanted_far(y, x)

    for key in plan:
        relay(key).wait_send()
    landed = out.at[pl.ds(0, nz * (plane - 1))]
    pltpu.make_async_copy(landed, landed, p_send).wait()
    pltpu.make_async_copy(landed, landed, p_recv).wait()


def to_hbm_kernel(src, out, sem):
    parts = sem.shape[0]
    size = src.shape[0] // parts
    copies = [
        pltpu.make_async_copy(
            src.at[pl.ds(n * size, size)], out.at[pl.ds(n * size, size)], sem.at[n]
        )
        for n in range(parts)
    ]
    for copy in copies:
        copy.start()
    for copy in copies:
        copy.wait()


def to_hbm(array):
    return pl.pallas_call(
        to_hbm_kernel,
        out_shape=pltpu.HBM(array.shape, array.dtype),
        in_specs=[pl.BlockSpec(memory_space=pltpu.VMEM)],
        out_specs=pl.BlockSpec(memory_space=pltpu.HBM),
        scratch_shapes=[pltpu.SemaphoreType.DMA((4,))],
        compiler_params=pltpu.CompilerParams(vmem_limit_bytes=1 << 20),
        name="to_hbm",
    )(array)


def body(features, session, owner_map):
    rows_dev, width = features.shape
    blocks = owner_map.shape[1]
    block_rows = rows_dev // blocks
    sizes = tuple(lax.axis_size(name) for name in ROW_GRP)
    ny, nz, nx, ng = sizes
    plane = ny * nx
    slot_cap = max(1, 2 * blocks // (plane * nz))
    slots = plane * nz * slot_cap
    tiles = rows_dev // TILE
    reach = (MOST - 2) // rows_dev + 1
    sums, cnt, open_rows, unpack, pack, choice = pl.pallas_call(
        lambda *refs: prelude_kernel(sizes, reach, block_rows, slot_cap, *refs),
        out_shape=(
            jax.ShapeDtypeStruct((rows_dev, width), jnp.float32),
            jax.ShapeDtypeStruct((rows_dev, TILE), jnp.float32),
            jax.ShapeDtypeStruct((8, TILE), jnp.float32),
            jax.ShapeDtypeStruct((2 * nz, slots), jnp.int32),
            jax.ShapeDtypeStruct((2, slots), jnp.int32),
            jax.ShapeDtypeStruct((1, slots), jnp.int32),
        ),
        in_specs=[pl.BlockSpec(memory_space=pltpu.HBM)] * 3,
        out_specs=[pl.BlockSpec(memory_space=pltpu.VMEM)] * 6,
        scratch_shapes=[
            pltpu.VMEM(owner_map.shape, jnp.int32),
            pltpu.VMEM((tiles, TILE), jnp.int32),
            pltpu.VMEM((rows_dev, width), jnp.float32),
            pltpu.VMEM((tiles, TILE), jnp.int32),
            pltpu.VMEM((tiles, TILE), jnp.int32),
            pltpu.VMEM((4, TILE), jnp.float32),
            pltpu.VMEM((reach, 4, TILE), jnp.float32),
            pltpu.VMEM((2, slots), jnp.int32),
            pltpu.VMEM((nz * ng - 1, 2, slots), jnp.int32),
            pltpu.VMEM((1, slots), jnp.int32),
            pltpu.VMEM((plane - 1, 1, slots), jnp.int32),
            pltpu.SemaphoreType.DMA((3,)),
        ]
        + [pltpu.SemaphoreType.DMA] * 6,
        compiler_params=pltpu.CompilerParams(
            collective_id=0, has_side_effects=True, vmem_limit_bytes=24 << 20
        ),
        name="prelude",
    )(
        *(
            pltpu.with_memory_space_constraint(arg, pltpu.HBM)
            for arg in (owner_map, session.reshape(tiles, TILE), features)
        )
    )

    def exchange(room, number):
        block = (block_rows, width)
        return lambda pack, unpack, *rows: to_hbm(pl.pallas_call(
            lambda *refs: exchange_kernel(sizes, room, *refs),
            out_shape=pltpu.VMEM((slots, *block), jnp.bfloat16),
            in_specs=[pl.BlockSpec(memory_space=pltpu.VMEM)] * 5,
            out_specs=pl.BlockSpec(memory_space=pltpu.VMEM),
            scratch_shapes=[
                pltpu.SMEM((2, slots), jnp.int32),
                pltpu.SMEM((2 * nz, slots), jnp.int32),
                pltpu.VMEM((blocks, *block), jnp.bfloat16),
                pltpu.VMEM((nz, plane, *block), jnp.bfloat16),
                pltpu.SemaphoreType.REGULAR,
                pltpu.SemaphoreType.DMA((2,)),
                pltpu.SemaphoreType.DMA((len(relay_plan(room)),)),
                pltpu.SemaphoreType.DMA((len(relay_plan(room)),)),
                pltpu.SemaphoreType.DMA,
                pltpu.SemaphoreType.DMA,
            ]
            + [
                pltpu.VMEM((b - a, *block), jnp.bfloat16)
                for _ in ("send", "recv")
                for _, _, a, b in relay_plan(room)
            ],
            compiler_params=pltpu.CompilerParams(
                collective_id=number, has_side_effects=True, vmem_limit_bytes=24 << 20
            ),
            name=f"exchange_{sum(room)}",
        )(pack, unpack, *rows))

    rooms = ROOMS
    return lax.switch(
        choice[0, 0], [exchange(room, 1 + n) for n, room in enumerate(rooms)],
        pack, unpack, sums, cnt, open_rows,
    )


def solution(mesh):
    split = Mesh(
        mesh.devices.reshape(4, 8, 4, mesh.shape["grp"]), ("row_0", "row_1", "row_2", "grp")
    )
    return jax.shard_map(
        body,
        mesh=split,
        in_specs=(P(ROW_GRP, None), P(ROW_GRP), P(ROW_GRP, None)),
        out_specs=P(ROW_GRP, None, None),
        check_vma=False,
    )
```

```python
import jax
import jax.numpy as jnp
from jax import lax
from jax.experimental import pallas as pl
from jax.experimental.pallas import tpu as pltpu
from jax.sharding import Mesh
from jax.sharding import PartitionSpec as P

ROW = ("row_0", "row_1", "row_2")
ROW_GRP = ("row_0", "row_1", "row_2", "grp")
MOST = 163840
TILE = 128
ROOMS = (
    (34, 25, 16, 6), (35, 26, 17, 6), (35, 27, 17, 7), (36, 27, 18, 7), (37, 28, 19, 7),
    (38, 29, 20, 7), (40, 30, 21, 8), (56, 40, 24, 8),
)
MESH = pl.DeviceIdType.MESH


def coords(d, sizes):
    out = []
    for n in reversed(sizes):
        out.append(lax.rem(d, n))
        d = lax.div(d, n)
    return tuple(reversed(out))


def place():
    return tuple(lax.axis_index(name) for name in ROW_GRP)


def plane_order(dy, dx, nx):
    return lax.rem(dy - dx + nx, nx) * nx + dx


def prelude_kernel(
    sizes, reach, block_rows, slot_cap,
    owners_hbm, ids_hbm, feat_hbm,
    sums, cnt, open_out, unpack_out, pack_out, choice_out,
    owners_ref, ids_ref, feat, ends, joins, tail, got, mine, got_line, top, got_plane,
    load_sem, send_sem, recv_sem, line_send, line_recv, plane_send, plane_recv,
):
    ny, nz, nx, ng = sizes
    devices = ny * nz * nx * ng
    me = lax.axis_index(ROW_GRP)
    y, z, x, g = place()
    rows_dev, width = feat.shape
    tiles = rows_dev // TILE
    blocks = rows_dev // block_rows
    line = nz * ng
    plane = ny * nx
    loads = [
        pltpu.make_async_copy(src, dst, load_sem.at[n])
        for n, (src, dst) in enumerate(
            ((ids_hbm, ids_ref), (owners_hbm, owners_ref), (feat_hbm, feat))
        )
    ]
    for load in loads:
        load.start()

    def line_peer(j):
        return (y, lax.rem(z + j // ng, nz), x, lax.rem(g + j % ng, ng))

    def plane_peer(j):
        return (lax.rem(y + j // nx, ny), z, lax.rem(x + j % nx, nx), g)

    barrier = pltpu.get_barrier_semaphore()

    @pl.loop(0, reach)
    def _(n):
        peer = lax.rem(me + devices - reach + n, devices)
        pl.semaphore_signal(barrier, 1, device_id=coords(peer, sizes), device_id_type=MESH)

    for j in range(1, line):
        pl.semaphore_signal(barrier, 1, device_id=line_peer(j), device_id_type=MESH)
    for j in range(1, plane):
        pl.semaphore_signal(barrier, 1, device_id=plane_peer(j), device_id_type=MESH)

    loads[0].wait()
    ids = ids_ref[...]
    last = jnp.broadcast_to(ids[tiles - 1 :, TILE - 1 :], (1, TILE))
    in_last = jnp.where(ids == jnp.broadcast_to(last, ids.shape), 1.0, 0.0)
    count = jnp.sum(jnp.sum(in_last, axis=0, keepdims=True), axis=1, keepdims=True)
    first = jnp.broadcast_to(rows_dev - count.astype(jnp.int32), (8, width))
    step = 64
    sub = lax.broadcasted_iota(jnp.int32, (step, width), 0)
    loads[2].wait()

    @pl.loop(0, rows_dev // step, init_carry=jnp.zeros((step, width), jnp.float32), unroll=4)
    def open_rows(t, acc):
        at = pl.ds(pl.multiple_of(t * step, step), step)
        inside = sub + t * step >= jnp.broadcast_to(first[0:1], (step, width))
        return acc + jnp.where(inside, feat[at, :], 0.0)

    total = jnp.sum(open_rows, axis=0, keepdims=True)
    tail[0:1, :] = total[:, :TILE]
    tail[1:2, :] = total[:, TILE:]
    tail[2:3, :] = last.astype(jnp.float32)
    tail[3:4, :] = jnp.broadcast_to(count, (1, TILE))

    loads[1].wait()
    slots = ny * nz * nx * slot_cap
    owners = owners_ref[...]
    across = jnp.broadcast_to(owners, (blocks, blocks))
    down = jnp.broadcast_to(across.T[:, 0:1], (blocks, blocks))
    earlier = lax.broadcasted_iota(jnp.int32, (blocks, blocks), 1) < (
        lax.broadcasted_iota(jnp.int32, (blocks, blocks), 0)
    )
    rank = jnp.sum(jnp.where((across == down) & earlier, 1.0, 0.0), axis=1, keepdims=True)
    target = down[:, 0:1] * slot_cap + rank.astype(jnp.int32)
    hit = jnp.broadcast_to(target, (blocks, slots)) == (
        lax.broadcasted_iota(jnp.int32, (blocks, slots), 1)
    )
    used = jnp.sum(jnp.where(hit, 1.0, 0.0), axis=0, keepdims=True)
    o_from = lax.broadcasted_iota(jnp.int32, (slots, slots), 0)
    o_to = lax.broadcasted_iota(jnp.int32, (slots, slots), 1)

    def plane_of(o):
        return lax.rem(lax.div(o, nx), nz)

    def order_of(o):
        dy = lax.rem(lax.div(o, nx * nz) - y + ny, ny)
        dx = lax.rem(lax.rem(o, nx) - x + nx, nx)
        return plane_order(dy, dx, nx)

    ahead = (plane_of(o_from) == plane_of(o_to)) & (order_of(o_from) < order_of(o_to))
    before = jnp.dot(
        jnp.broadcast_to(used, (8, slots)).astype(jnp.bfloat16),
        jnp.where(ahead, 1.0, 0.0).astype(jnp.bfloat16),
        preferred_element_type=jnp.float32,
    )[0:1]
    spot = jnp.where(used > 0.0, before + 1.0, 0.0)
    mine[0:1, :] = spot.astype(jnp.int32)
    home = plane_of(o_to[0:1])
    key = home.astype(jnp.float32) * plane + before

    far = nz // 2
    away = lax.rem(home - z + nz, nz)
    number = [
        jnp.sum(jnp.where(away == d, used, 0.0), axis=1, keepdims=True) for d in range(nz)
    ]
    upper = jnp.floor((number[far] + 1.0) * 0.5)
    listed = jnp.full((1, slots), -1.0, jnp.float32)
    loads_by_hop = []
    for way, shift in ((0, 0.0), (1, 64.0)):
        start = jnp.full((1, 1), shift, jnp.float32)
        starts = []
        for d in range(1, far):
            at = nz - d if way else d
            starts.append(start)
            listed = jnp.where(away == at, before + start, listed)
            start = start + number[at]
        starts.append(start)
        half = (before >= upper) if way else (before < upper)
        skip = upper if way else jnp.zeros_like(upper)
        listed = jnp.where((away == far) & half, before + (start - skip), listed)
        end = start + ((number[far] - upper) if way else upper)
        loads_by_hop.append([end - first for first in starts])
    stats = jnp.zeros((1, slots), jnp.float32)
    hop_lane = lax.broadcasted_iota(jnp.int32, (1, slots), 1)
    for hop in range(far):
        load_here = jnp.maximum(loads_by_hop[0][hop], loads_by_hop[1][hop])
        stats = jnp.where(hop_lane == hop, load_here, stats)
    mine[1:2, :] = stats.astype(jnp.int32)
    list_key = jnp.sum(
        jnp.where(hit, jnp.broadcast_to(listed, (blocks, slots)), 0.0), axis=1, keepdims=True
    )
    block_key = jnp.sum(
        jnp.where(hit, jnp.broadcast_to(key, (blocks, slots)), 0.0), axis=1, keepdims=True
    )
    entry = lax.broadcasted_iota(jnp.int32, (blocks, slots), 1).astype(jnp.float32)
    order = lax.broadcasted_iota(jnp.int32, (blocks, slots), 0)
    for n, one in enumerate((block_key, list_key)):
        pack_out[n : n + 1, :] = jnp.sum(
            jnp.where(jnp.broadcast_to(one, (blocks, slots)) == entry, order, 0),
            axis=0, keepdims=True,
        )

    lane = lax.broadcasted_iota(jnp.int32, ids.shape, 1)
    after = pltpu.roll(ids, TILE - 1, 1)
    end = jnp.where((after != ids) | (lane == TILE - 1), lane, TILE)
    hop = 1
    while hop < TILE:
        nxt = jnp.where(lane + hop < TILE, pltpu.roll(end, TILE - hop, 1), TILE)
        end = jnp.minimum(end, nxt)
        hop *= 2
    ends[...] = end
    prior = jnp.concatenate([jnp.full((1, TILE), -1, jnp.int32), ids[:-1]], axis=0)
    prior = jnp.broadcast_to(prior[:, TILE - 1 :], ids.shape)
    goes_on = jnp.sum(jnp.where(ids == prior, 1.0, 0.0), axis=1, keepdims=True)
    joins[...] = jnp.broadcast_to(goes_on.astype(jnp.int32), ids.shape)

    pl.semaphore_wait(barrier, reach + line - 1 + plane - 1)

    for j in range(1, line):
        pltpu.make_async_remote_copy(
            src_ref=mine, dst_ref=got_line.at[j - 1], send_sem=line_send, recv_sem=line_recv,
            device_id=line_peer(j), device_id_type=MESH,
        ).start()

    @pl.loop(0, reach)
    def _(n):
        k = reach - n
        peer = lax.rem(me + k, devices)
        pltpu.make_async_remote_copy(
            src_ref=tail, dst_ref=got.at[k - 1], send_sem=send_sem, recv_sem=recv_sem,
            device_id=coords(peer, sizes), device_id_type=MESH,
        ).start()

    row = lax.broadcasted_iota(jnp.int32, (TILE, TILE), 0)
    col = lax.broadcasted_iota(jnp.int32, (TILE, TILE), 1)
    causal = col <= row
    ones = jnp.ones((TILE, TILE), jnp.bfloat16)

    @pl.loop(
        0, tiles,
        init_carry=(jnp.zeros((1, width), jnp.float32), jnp.zeros((1, TILE), jnp.float32)),
        unroll=4,
    )
    def _(t, carry):
        open_sum, open_count = carry
        at = pl.ds(pl.multiple_of(t * TILE, TILE), TILE)
        alive = row <= jnp.broadcast_to(ends[pl.ds(t, 1), :], (TILE, TILE))
        mask = jnp.where(alive & causal, 1.0, 0.0).astype(jnp.bfloat16)
        rows = feat[at, :]
        high = rows.astype(jnp.bfloat16)
        rest = rows - high.astype(jnp.float32)
        mid = rest.astype(jnp.bfloat16)
        low = (rest - mid.astype(jnp.float32)).astype(jnp.bfloat16)
        inside = (
            jnp.dot(mask, high, preferred_element_type=jnp.float32)
            + jnp.dot(mask, mid, preferred_element_type=jnp.float32)
            + jnp.dot(mask, low, preferred_element_type=jnp.float32)
        )
        number = jnp.dot(mask, ones, preferred_element_type=jnp.float32)
        joined = row < jnp.broadcast_to(joins[pl.ds(t, 1), :], (TILE, TILE))
        both = jnp.concatenate([joined, joined], axis=1)
        inside = inside + jnp.where(both, jnp.broadcast_to(open_sum, (TILE, width)), 0.0)
        number = number + jnp.where(joined, jnp.broadcast_to(open_count, (TILE, TILE)), 0.0)
        sums[at, :] = inside
        cnt[at, :] = number
        return inside[TILE - 1 :, :], number[TILE - 1 :, :]

    pltpu.make_async_copy(got_line, got_line, line_recv).wait()
    unpack_out[0:1, :] = mine[0:1, :]
    largest = mine[1:2, :]
    for j in range(1, line):
        both = got_line[j - 1]
        largest = jnp.maximum(largest, both[1:2, :])
        if j % ng == 0:
            unpack_out[j // ng : j // ng + 1, :] = both[0:1, :]
    spots = unpack_out[0:nz, :].astype(jnp.float32)
    here = jnp.broadcast_to(plane_of(o_to[0:1]) == z, spots.shape)
    taken = jnp.max(jnp.where(here, spots, 0.0), axis=1, keepdims=True)
    unpack_out[nz : 2 * nz, :] = jnp.broadcast_to(taken, spots.shape).astype(jnp.int32)
    top[...] = largest

    for j in range(1, plane):
        pltpu.make_async_remote_copy(
            src_ref=top, dst_ref=got_plane.at[j - 1], send_sem=plane_send,
            recv_sem=plane_recv, device_id=plane_peer(j), device_id_type=MESH,
        ).start()

    pltpu.make_async_copy(got, got, recv_sem).wait()
    arrived = got[...]
    open_id = arrived[0, 2:3, :]
    age = lax.broadcasted_iota(jnp.int32, arrived.shape, 0) + 1
    same = jnp.broadcast_to(arrived[:, 2:3, :], arrived.shape) == jnp.broadcast_to(
        open_id[None], arrived.shape
    )
    merged = jnp.sum(jnp.where(same & (age <= me), arrived, 0.0), axis=0)
    open_out[0:4, :] = merged
    in_open = jnp.where(
        ids.astype(jnp.float32) == jnp.broadcast_to(open_id, ids.shape), 1.0, 0.0
    )
    reached = jnp.sum(jnp.sum(in_open, axis=0, keepdims=True), axis=1, keepdims=True)
    open_out[4:8, :] = jnp.broadcast_to(reached, (4, TILE))

    pltpu.make_async_copy(got_plane, got_plane, plane_recv).wait()
    for j in range(1, plane):
        largest = jnp.maximum(largest, got_plane[j - 1])
    choice = jnp.zeros((1, 1), jnp.float32)
    largest = largest.astype(jnp.float32)
    for rooms in ROOMS[:-1]:
        room = jnp.zeros((1, slots), jnp.float32)
        for hop, size in enumerate(rooms):
            room = jnp.where(hop_lane == hop, float(size), room)
        over = jnp.max(jnp.where(largest > room, 1.0, 0.0), axis=1, keepdims=True)
        choice = choice + over
    choice_out[...] = jnp.broadcast_to(choice, (1, slots)).astype(jnp.int32)
    pltpu.make_async_copy(got, got, send_sem).wait()
    pltpu.make_async_copy(got_line, got_line, line_send).wait()
    pltpu.make_async_copy(got_plane, got_plane, plane_send).wait()


def hop_cuts(rooms):
    one, two, three, four = rooms
    ends = ((16, 24, one), (8, 12, 20, two), (4, 8, 12, three), (4, four))
    return [list(zip((0,) + cut[:-1], cut)) for cut in ends]


def relay_plan(rooms):
    return [
        (way, hop, a, b)
        for way in (0, 1)
        for hop, cuts in enumerate(hop_cuts(rooms))
        for a, b in cuts
    ]


def exchange_kernel(
    sizes, rooms,
    pack_ref, unpack_ref, sums, cnt, open_ref, out,
    pack, unpack, norm, stage, ring, table_sem, z_send, z_recv, p_send, p_recv, *bufs,
):
    ny, nz, nx, ng = sizes
    plane = ny * nx
    y, z, x, g = place()
    far = nz // 2
    plan = relay_plan(rooms)
    number = {key: n for n, key in enumerate(plan)}
    cuts = hop_cuts(rooms)
    send, recv = bufs[: len(plan)], bufs[len(plan) :]
    barrier = pltpu.get_barrier_semaphore()

    def z_peer(d):
        return (y, lax.rem(z + d, nz), x, g)

    tables = [
        pltpu.make_async_copy(pack_ref, pack, table_sem.at[0]),
        pltpu.make_async_copy(unpack_ref, unpack, table_sem.at[1]),
    ]
    for table in tables:
        table.start()
    x_ring = [(y, z, lax.rem(x + j, nx), g) for j in range(1, nx)]
    y_ring = [(lax.rem(y + j, ny), z, x, g) for j in range(1, ny)]
    near = [z_peer(1), z_peer(nz - 1)] + x_ring + y_ring
    for peer in near:
        pl.semaphore_signal(barrier, 1, device_id=peer, device_id_type=MESH)

    blocks, block_rows, width = norm.shape
    open_sum = jnp.concatenate([open_ref[0:1, :], open_ref[1:2, :]], axis=1)
    open_count = open_ref[3:4, :]
    reached = open_ref[4:5, :].astype(jnp.int32)
    sub = lax.broadcasted_iota(jnp.int32, (block_rows, TILE), 0)

    @pl.loop(0, blocks, unroll=4)
    def _(b):
        at = pl.ds(pl.multiple_of(b * block_rows, block_rows), block_rows)
        joined = sub + b * block_rows < jnp.broadcast_to(reached, (block_rows, TILE))
        count = cnt[at, :] + jnp.where(
            joined, jnp.broadcast_to(open_count, (block_rows, TILE)), 0.0
        )
        scale = 1.0 / jnp.sqrt(count)
        both = jnp.concatenate([joined, joined], axis=1)
        rows = sums[at, :] + jnp.where(
            both, jnp.broadcast_to(open_sum, (block_rows, width)), 0.0
        )
        norm[b] = (rows * jnp.concatenate([scale, scale], axis=1)).astype(jnp.bfloat16)

    for table in tables:
        table.wait()
    pl.semaphore_wait(barrier, len(near))

    def relay(key):
        n = number[key]
        return pltpu.make_async_remote_copy(
            src_ref=send[n], dst_ref=recv[n], send_sem=z_send.at[n], recv_sem=z_recv.at[n],
            device_id=z_peer(nz - 1 if key[0] else 1), device_id_type=MESH,
        )

    def parts(way, hop, count=None):
        return [(recv[number[way, hop, a, b]], a, b) for a, b in cuts[hop][:count]]

    def pick(spot, pieces):
        block = None
        for ref, a, b in pieces:
            one = ref[jnp.clip(spot - 1 - a, 0, b - a - 1)]
            block = one if block is None else jnp.where(spot > a, one, block)
        return block

    def go(hop, piece):
        for way in (0, 1):
            relay((way, hop, *cuts[hop][piece])).start()

    def arrived(hop, piece):
        for way in (0, 1):
            relay((way, hop, *cuts[hop][piece])).wait_recv()

    def repack(hop, piece, count):
        a, b = cuts[hop][piece]
        for way in (0, 1):
            ref = send[number[way, hop, a, b]]
            mine = unpack[nz + (nz - hop if way else hop), 0]
            pieces = parts(way, hop - 1, count)

            @pl.loop(0, b - a)
            def _(k):
                ref[k] = pick(mine + a + k + 1, pieces)

        go(hop, piece)

    def wanted(d, ty, tx, pieces):
        spot = unpack[d, (ty * nz + z) * nx + tx]
        block = pick(spot, pieces)
        return jnp.where(spot > 0, block, jnp.zeros_like(block))

    def wanted_far(ty, tx, count=None):
        spot = unpack[far, (ty * nz + z) * nx + tx]
        upper = lax.div(unpack[nz + far, 0] + 1, 2)
        block = jnp.where(
            spot > upper,
            pick(spot - upper, parts(1, far - 1, count)),
            pick(spot, parts(0, far - 1, count)),
        )
        return jnp.where(spot > 0, block, jnp.zeros_like(block))

    def own(ty, tx):
        spot = unpack[0, (ty * nz + z) * nx + tx]
        block = norm[pack[0, z * plane + jnp.maximum(spot, 1) - 1]]
        return jnp.where(spot > 0, block, jnp.zeros_like(block))

    def slot_from(d):
        return (y * nz + lax.rem(z + nz - d, nz)) * nx + x

    def p_copy(d, j, ty, tx):
        return pltpu.make_async_remote_copy(
            src_ref=stage.at[d, j], dst_ref=out.at[slot_from(d)],
            send_sem=p_send, recv_sem=p_recv,
            device_id=(ty, z, tx, g), device_id_type=MESH,
        )

    def deliver(d, block_for):
        def target(j):
            return lax.rem(y + lax.div(j, nx), ny), lax.rem(x + lax.rem(j, nx), nx)

        @pl.loop(1, plane)
        def _(j):
            stage[d, j] = block_for(*target(j))

        @pl.loop(1, plane)
        def _(j):
            p_copy(d, j, *target(j)).start()

        out[slot_from(d)] = block_for(y, x)

    def deliver_from(d, count=None):
        for way in (0, 1):
            step = nz - d if way else d
            pieces = parts(way, d - 1, count)
            deliver(step, lambda ty, tx: wanted(step, ty, tx, pieces))

    def deliver_group(d, group, block_for):
        def target(j):
            return lax.rem(y + group + j, ny), lax.rem(x + j, nx)

        first = 1 if group == 0 else 0

        @pl.loop(first, nx)
        def _(j):
            stage[d, group * nx + j] = block_for(*target(j))

        @pl.loop(first, nx)
        def _(j):
            p_copy(d, group * nx + j, *target(j)).start()

    def deliver_groups(d, groups, count):
        for way in (0, 1):
            step = nz - d if way else d
            pieces = parts(way, d - 1, count)
            for group in groups:
                deliver_group(step, group, lambda ty, tx: wanted(step, ty, tx, pieces))

    def keep(d):
        for way in (0, 1):
            step = nz - d if way else d
            out[slot_from(step)] = wanted(step, y, x, parts(way, d - 1))

    for piece, (a, b) in enumerate(cuts[0]):
        for way in (0, 1):
            ref = send[number[way, 0, a, b]]

            @pl.loop(0, b - a)
            def _(k):
                ref[k] = norm[pack[1, way * 64 + a + k]]

        go(0, piece)
    for peer in x_ring:
        pl.semaphore_signal(ring, 1, device_id=peer, device_id_type=MESH)
    pl.semaphore_wait(ring, len(x_ring))
    deliver(0, own)
    arrived(0, 0)
    deliver_from(1, 1)
    arrived(0, 1)
    repack(1, 0, 2)
    arrived(0, 2)
    for piece in (1, 2, 3):
        repack(1, piece, 3)
    arrived(1, 0)
    deliver_groups(2, (0, 1), 1)
    arrived(1, 1)
    deliver_groups(2, (2,), 2)
    arrived(1, 2)
    repack(2, 0, 3)
    deliver_groups(2, (3,), 3)
    arrived(1, 3)
    for piece in (1, 2, 3):
        repack(2, piece, 4)
    keep(2)
    for group in range(ny):
        arrived(2, group)
        if group == ny - 1:
            repack(3, 0, 4)
            repack(3, 1, 4)
        deliver_groups(3, (group,), group + 1)
    keep(3)
    arrived(3, 0)
    deliver_group(far, 0, lambda ty, tx: wanted_far(ty, tx, 1))
    arrived(3, 1)
    for group in range(1, ny):
        deliver_group(far, group, wanted_far)
    out[slot_from(far)] = wanted_far(y, x)

    for key in plan:
        relay(key).wait_send()
    landed = out.at[pl.ds(0, nz * (plane - 1))]
    pltpu.make_async_copy(landed, landed, p_send).wait()
    pltpu.make_async_copy(landed, landed, p_recv).wait()


def to_hbm_kernel(src, out, sem):
    parts = sem.shape[0]
    size = src.shape[0] // parts
    copies = [
        pltpu.make_async_copy(
            src.at[pl.ds(n * size, size)], out.at[pl.ds(n * size, size)], sem.at[n]
        )
        for n in range(parts)
    ]
    for copy in copies:
        copy.start()
    for copy in copies:
        copy.wait()


def to_hbm(array):
    return pl.pallas_call(
        to_hbm_kernel,
        out_shape=pltpu.HBM(array.shape, array.dtype),
        in_specs=[pl.BlockSpec(memory_space=pltpu.VMEM)],
        out_specs=pl.BlockSpec(memory_space=pltpu.HBM),
        scratch_shapes=[pltpu.SemaphoreType.DMA((4,))],
        compiler_params=pltpu.CompilerParams(vmem_limit_bytes=1 << 20),
        name="to_hbm",
    )(array)


def body(features, session, owner_map):
    rows_dev, width = features.shape
    blocks = owner_map.shape[1]
    block_rows = rows_dev // blocks
    sizes = tuple(lax.axis_size(name) for name in ROW_GRP)
    ny, nz, nx, ng = sizes
    plane = ny * nx
    slot_cap = max(1, 2 * blocks // (plane * nz))
    slots = plane * nz * slot_cap
    tiles = rows_dev // TILE
    reach = (MOST - 2) // rows_dev + 1
    sums, cnt, open_rows, unpack, pack, choice = pl.pallas_call(
        lambda *refs: prelude_kernel(sizes, reach, block_rows, slot_cap, *refs),
        out_shape=(
            jax.ShapeDtypeStruct((rows_dev, width), jnp.float32),
            jax.ShapeDtypeStruct((rows_dev, TILE), jnp.float32),
            jax.ShapeDtypeStruct((8, TILE), jnp.float32),
            jax.ShapeDtypeStruct((2 * nz, slots), jnp.int32),
            jax.ShapeDtypeStruct((2, slots), jnp.int32),
            jax.ShapeDtypeStruct((1, slots), jnp.int32),
        ),
        in_specs=[pl.BlockSpec(memory_space=pltpu.HBM)] * 3,
        out_specs=[pl.BlockSpec(memory_space=pltpu.VMEM)] * 6,
        scratch_shapes=[
            pltpu.VMEM(owner_map.shape, jnp.int32),
            pltpu.VMEM((tiles, TILE), jnp.int32),
            pltpu.VMEM((rows_dev, width), jnp.float32),
            pltpu.VMEM((tiles, TILE), jnp.int32),
            pltpu.VMEM((tiles, TILE), jnp.int32),
            pltpu.VMEM((4, TILE), jnp.float32),
            pltpu.VMEM((reach, 4, TILE), jnp.float32),
            pltpu.VMEM((2, slots), jnp.int32),
            pltpu.VMEM((nz * ng - 1, 2, slots), jnp.int32),
            pltpu.VMEM((1, slots), jnp.int32),
            pltpu.VMEM((plane - 1, 1, slots), jnp.int32),
            pltpu.SemaphoreType.DMA((3,)),
        ]
        + [pltpu.SemaphoreType.DMA] * 6,
        compiler_params=pltpu.CompilerParams(
            collective_id=0, has_side_effects=True, vmem_limit_bytes=24 << 20
        ),
        name="prelude",
    )(
        *(
            pltpu.with_memory_space_constraint(arg, pltpu.HBM)
            for arg in (owner_map, session.reshape(tiles, TILE), features)
        )
    )

    def exchange(room, number):
        block = (block_rows, width)
        return lambda pack, unpack, *rows: to_hbm(pl.pallas_call(
            lambda *refs: exchange_kernel(sizes, room, *refs),
            out_shape=pltpu.VMEM((slots, *block), jnp.bfloat16),
            in_specs=[pl.BlockSpec(memory_space=pltpu.VMEM)] * 5,
            out_specs=pl.BlockSpec(memory_space=pltpu.VMEM),
            scratch_shapes=[
                pltpu.SMEM((2, slots), jnp.int32),
                pltpu.SMEM((2 * nz, slots), jnp.int32),
                pltpu.VMEM((blocks, *block), jnp.bfloat16),
                pltpu.VMEM((nz, plane, *block), jnp.bfloat16),
                pltpu.SemaphoreType.REGULAR,
                pltpu.SemaphoreType.DMA((2,)),
                pltpu.SemaphoreType.DMA((len(relay_plan(room)),)),
                pltpu.SemaphoreType.DMA((len(relay_plan(room)),)),
                pltpu.SemaphoreType.DMA,
                pltpu.SemaphoreType.DMA,
            ]
            + [
                pltpu.VMEM((b - a, *block), jnp.bfloat16)
                for _ in ("send", "recv")
                for _, _, a, b in relay_plan(room)
            ],
            compiler_params=pltpu.CompilerParams(
                collective_id=number, has_side_effects=True, vmem_limit_bytes=24 << 20
            ),
            name=f"exchange_{sum(room)}",
        )(pack, unpack, *rows))

    rooms = ROOMS
    return lax.switch(
        choice[0, 0], [exchange(room, 1 + n) for n, room in enumerate(rooms)],
        pack, unpack, sums, cnt, open_rows,
    )


def solution(mesh):
    split = Mesh(
        mesh.devices.reshape(4, 8, 4, mesh.shape["grp"]), ("row_0", "row_1", "row_2", "grp")
    )
    return jax.shard_map(
        body,
        mesh=split,
        in_specs=(P(ROW_GRP, None), P(ROW_GRP), P(ROW_GRP, None)),
        out_specs=P(ROW_GRP, None, None),
        check_vma=False,
    )
```
